32 devices in a mesh: dp: 2 (over x), tp: 4 (over z), sp: 4 (over y, core).
Axes of the slice: x: 2, y: 2, z: 4, core: 2. Of those that a mesh axis runs over, the one named last changes fastest.
Arguments:
- hidden: bfloat16 [128, 8192], P('dp'), parts along dimension 0
- norm_gain: float32 [8192], replicated
- w_query: bfloat16 [8192, 8192], P(None, 'tp')
- w_key: bfloat16 [8192, 1024], P(None, 'tp')
- w_value: bfloat16 [8192, 1024], P(None, 'tp')
- w_out: bfloat16 [8192, 8192], P('tp')
- k_cache: bfloat16 [128, 1024, 8, 128], P('dp', 'sp', 'tp'), parts along dimension 0
- v_cache: bfloat16 [128, 1024, 8, 128], P('dp', 'sp', 'tp'), parts along dimension 0
- positions: int32 [128], P('dp'), parts along dimension 0
Outputs:
- output 1: bfloat16 [128, 8192], P('dp'), parts along dimension 0
- output 2: bfloat16 [128, 1024, 8, 128], P('dp', 'sp', 'tp'), parts along dimension 0
- output 3: bfloat16 [128, 1024, 8, 128], P('dp', 'sp', 'tp'), parts along dimension 0
There are 2 independent parts. The reference program is written for one: setup_inputs(seed, part) draws one part's arguments, and reference() takes and returns one part's arrays. A program takes and returns all parts, laid end to end along the dimension named above; an argument that names none is the same for every part.
All inputs are finite; a program needn't handle non-finite values.
Results may differ from the reference program's by a relative error of at most 0.00432738.
Values sent between devices are 32-bit elements.
A program may use at most 1 GiB of HBM per device.

```python
import jax
import jax.numpy as jnp
from jax import lax

D = 8192
HEADS = 64
KV_HEADS = 8
HEAD = 128
BATCH = 64
SEQ = 1024
ROPE_BASE = 1000000
EPS = 1e-5
GROUP = HEADS // KV_HEADS


def rotary(tensor, positions):
    half_dim = tensor.shape[-1] // 2
    inv_freq = 1.0 / (ROPE_BASE ** (jnp.arange(half_dim, dtype=jnp.float32) * 2.0 / tensor.shape[-1]))
    angles = positions.astype(jnp.float32)[:, None, None] * inv_freq[None, None, :]
    cosine = jnp.cos(angles)
    sine_val = jnp.sin(angles)
    first_half = tensor[..., :half_dim]
    second_half = tensor[..., half_dim:]
    return jnp.concatenate([first_half * cosine - second_half * sine_val, first_half * sine_val + second_half * cosine], axis=-1)


def smooth_field(base_key, amplitude, noise_scale):
    key_coef, key_noise = jax.random.split(base_key)
    num_freq = 4
    seq_frac = jnp.arange(SEQ, dtype=jnp.float32) / SEQ
    freq_list = jnp.arange(1, num_freq + 1, dtype=jnp.float32)
    phases = 2.0 * jnp.pi * seq_frac[:, None] * freq_list[None, :]
    basis_mat = jnp.concatenate([jnp.cos(phases), jnp.sin(phases)], axis=1)
    coef_mat = jax.random.normal(key_coef, (BATCH, 2 * num_freq, KV_HEADS * HEAD), jnp.float32) * (amplitude / num_freq ** 0.5)
    smooth_part = jnp.einsum("sf,bfc->bsc", basis_mat, coef_mat)
    noise_part = jax.random.normal(key_noise, (BATCH, SEQ, KV_HEADS * HEAD), jnp.float32)
    return (smooth_part + noise_scale * noise_part).reshape(BATCH, SEQ, KV_HEADS, HEAD)


def draw_positions(base_key):
    key_len, key_pick = jax.random.split(base_key)
    pos_draw = jax.random.randint(key_len, (BATCH,), SEQ // 4, SEQ, jnp.int32)
    longest = jax.random.randint(key_pick, (), 0, BATCH, jnp.int32)
    return jnp.where(jnp.arange(BATCH) == longest, SEQ - 1, pos_draw).astype(jnp.int32)


def setup_inputs(seed: int = 0, part: int = 0) -> dict:
    key_list = jax.random.split(jax.random.key(seed), 9)
    q_width = HEADS * HEAD
    kv_width = KV_HEADS * HEAD
    norm_gain = 1.0 + 0.3 * jax.random.normal(key_list[0], (D,), jnp.float32)
    w_query32 = jax.random.normal(key_list[1], (D, q_width), jnp.float32) * D ** -0.5
    head_zero = w_query32.reshape(D, KV_HEADS, GROUP, HEAD)[:, :, 0, :].reshape(D, kv_width)
    w_key32 = 0.75 * head_zero + 0.66 * jax.random.normal(key_list[2], (D, kv_width), jnp.float32) * D ** -0.5
    w_value32 = jax.random.normal(key_list[3], (D, kv_width), jnp.float32) * D ** -0.5
    w_out32 = jax.random.normal(key_list[4], (q_width, D), jnp.float32) * q_width ** -0.5
    hidden = jax.random.normal(jax.random.fold_in(key_list[5], part), (BATCH, D), jnp.float32)
    k_cache = smooth_field(jax.random.fold_in(key_list[6], part), 1.2, 0.5)
    v_cache = smooth_field(jax.random.fold_in(key_list[7], part), 1.5, 0.5)
    positions = draw_positions(jax.random.fold_in(key_list[8], part))
    return {
        "hidden": hidden.astype(jnp.bfloat16),
        "norm_gain": norm_gain,
        "w_query": w_query32.astype(jnp.bfloat16),
        "w_key": w_key32.astype(jnp.bfloat16),
        "w_value": w_value32.astype(jnp.bfloat16),
        "w_out": w_out32.astype(jnp.bfloat16),
        "k_cache": k_cache.astype(jnp.bfloat16),
        "v_cache": v_cache.astype(jnp.bfloat16),
        "positions": positions,
    }


def reference(hidden, norm_gain, w_query, w_key, w_value, w_out, k_cache, v_cache, positions):
    resid_f32 = hidden.astype(jnp.float32)
    normed = (resid_f32 * lax.rsqrt(jnp.mean(resid_f32 * resid_f32, axis=-1, keepdims=True) + EPS) * norm_gain).astype(jnp.bfloat16)
    q_proj = jnp.dot(normed, w_query, preferred_element_type=jnp.float32).reshape(BATCH, HEADS, HEAD)
    k_proj = jnp.dot(normed, w_key, preferred_element_type=jnp.float32).reshape(BATCH, KV_HEADS, HEAD)
    v_new = jnp.dot(normed, w_value, preferred_element_type=jnp.float32).astype(jnp.bfloat16).reshape(BATCH, KV_HEADS, HEAD)
    q_rot = rotary(q_proj, positions).astype(jnp.bfloat16).reshape(BATCH, KV_HEADS, GROUP, HEAD)
    k_new = rotary(k_proj, positions).astype(jnp.bfloat16)
    slot_mask = (jnp.arange(SEQ)[None, :] == positions[:, None])[:, :, None, None]
    k_updated = jnp.where(slot_mask, k_new[:, None], k_cache)
    v_updated = jnp.where(slot_mask, v_new[:, None], v_cache)
    score_scale = HEAD ** -0.5

    def one_sequence(seq_args):
        q_seq, k_seq, v_seq, last_pos = seq_args
        scores = jnp.einsum("kgd,skd->kgs", q_seq.astype(jnp.float32), k_seq.astype(jnp.float32)) * score_scale
        scores = jnp.where(jnp.arange(SEQ) <= last_pos, scores, -jnp.inf)
        attn_prob = jax.nn.softmax(scores, axis=-1)
        return jnp.einsum("kgs,skd->kgd", attn_prob, v_seq.astype(jnp.float32))

    attn_out = lax.map(one_sequence, (q_rot, k_updated, v_updated, positions))
    attn_out = attn_out.astype(jnp.bfloat16).reshape(BATCH, HEADS * HEAD)
    proj_out = jnp.dot(attn_out, w_out, preferred_element_type=jnp.float32)
    return (resid_f32 + proj_out).astype(jnp.bfloat16), k_updated, v_updated
```

```python
import functools

import jax
import jax.numpy as jnp
from jax import lax
from jax.experimental import pallas as pl
from jax.experimental.pallas import tpu as pltpu
from jax.sharding import PartitionSpec as P

ROPE_BASE = 1000000.0
EPS = 1e-5
NEG_BIG = float(jnp.finfo(jnp.float32).min)
MESH = pl.DeviceIdType.MESH
F32 = jnp.float32
BF16 = jnp.bfloat16
VMEM_LIMIT = 60 * 1024 * 1024
NC = 8
NS = 4
LAG = 3


def remote(src, dst, send, recv, device):
    return pltpu.make_async_remote_copy(
        src_ref=src, dst_ref=dst, send_sem=send, recv_sem=recv, device_id=device, device_id_type=MESH
    )


def round_bf16(x):
    return x.astype(BF16).astype(F32)


def qkv_kernel(
    hid, gain, cosf, sinf, wq, wk, wv, q_out, kv_out,
    hbuf, gbuf, rbuf, wqb, wkvb, q_own, q_land, kv_own, kv_land, hsem, wsem, ssem, rsem,
):
    me = lax.axis_index("sp")
    core = lax.rem(me, 2)
    partner = {"sp": me + 1 - 2 * core}
    batch, d_model = hid.shape
    tiles, _, cols = wqb.shape
    half = tiles * cols
    hcopy = pltpu.make_async_copy(hid, hbuf, hsem.at[0])
    gcopy = pltpu.make_async_copy(gain, gbuf, hsem.at[1])
    hcopy.start()
    gcopy.start()
    head_cols = pl.ds(pl.multiple_of(core * 128, 128), 128)
    kcopy = pltpu.make_async_copy(wk.at[:, head_cols], wkvb.at[:, pl.ds(0, 128)], hsem.at[2])
    vcopy = pltpu.make_async_copy(wv.at[:, head_cols], wkvb.at[:, pl.ds(128, 128)], hsem.at[3])
    kcopy.start()
    vcopy.start()

    def wcopy(t):
        return pltpu.make_async_copy(
            wq.at[:, pl.ds(pl.multiple_of(core * half + t * cols, cols), cols)], wqb.at[t], wsem.at[t]
        )

    for t in range(tiles):
        wcopy(t).start()
    barrier = pltpu.get_barrier_semaphore()
    pl.semaphore_signal(barrier, inc=1, device_id=partner, device_id_type=MESH)

    hcopy.wait()
    gcopy.wait()

    def norm_rows(i, carry):
        rows = pl.ds(pl.multiple_of(i * 16, 16), 16)
        x = hbuf[rows, :].astype(F32)
        scale = lax.rsqrt(jnp.sum(x * x, axis=-1, keepdims=True) * (1.0 / d_model) + EPS)
        rbuf[rows, :] = (x * scale * gbuf[...]).astype(BF16)
        return carry

    lax.fori_loop(0, batch // 16, norm_rows, 0)

    def rotate(x):
        return round_bf16(x * cosf[...] + pltpu.roll(x, 64, 1) * sinf[...])

    kcopy.wait()
    vcopy.wait()
    kv = jnp.dot(rbuf[...], wkvb[...], preferred_element_type=F32)
    kv_own[0] = rotate(kv[:, :128])
    kv_own[1] = round_bf16(kv[:, 128:])
    pl.semaphore_wait(barrier, 1)
    kv_send = remote(kv_own, kv_land, ssem.at[tiles], rsem.at[tiles], partner)
    kv_send.start()

    def q_send(t):
        rows = pl.ds(pl.multiple_of(t * 2 * batch, 2 * batch), 2 * batch)
        return remote(q_own.at[rows], q_land.at[rows], ssem.at[t], rsem.at[t], partner)

    def q_tile(t, carry):
        wcopy(t).wait()
        q = jnp.dot(rbuf[...], wqb[t], preferred_element_type=F32)
        for h in range(2):
            q_own[pl.ds(pl.multiple_of((t * 2 + h) * batch, batch), batch), :] = rotate(q[:, h * 128:(h + 1) * 128])
        q_send(t).start()
        return carry

    lax.fori_loop(0, tiles, q_tile, 0)
    rows_half = q_own.shape[0]
    q_out[pl.ds(pl.multiple_of(core * rows_half, rows_half), rows_half), :] = q_own[...]
    kv_out[core] = kv_own[...]
    kv_send.wait()
    kv_out[1 - core] = kv_land[...]
    for t in range(tiles):
        q_send(t).wait()
    q_out[pl.ds(pl.multiple_of((1 - core) * rows_half, rows_half), rows_half), :] = q_land[...]


def attention_kernel(
    pos, q_ref, kv_ref, kc, vc, ko, vo, acc_ref, stat_ref, kbuf, vbuf, mbuf, lbuf, isem, osem,
):
    batch, rows, hd = kbuf.shape
    heads = acc_ref.shape[0] // batch
    groups = batch // 8
    me = lax.axis_index("sp")
    first = me * (rows // 2)

    def seqs(g):
        return pl.ds(pl.multiple_of(g * 8, 8), 8)

    def fetch(which, g):
        src, dst = ((kc, kbuf), (vc, vbuf))[which]
        return pltpu.make_async_copy(src.at[seqs(g)], dst.at[seqs(g)], isem.at[which, g])

    def store(which, g):
        src, dst = ((kbuf, ko), (vbuf, vo))[which]
        return pltpu.make_async_copy(src.at[seqs(g)], dst.at[seqs(g)], osem.at[which, g])

    for g in range(groups):
        fetch(0, g).start()
        fetch(1, g).start()

    row_iota = lax.broadcasted_iota(jnp.int32, (16, hd), 0)
    col_iota = lax.broadcasted_iota(jnp.int32, (heads, rows), 1)
    head_iota = lax.broadcasted_iota(jnp.int32, (heads, rows), 0)
    col_head = lax.rem(col_iota, 2)
    col_pos = jnp.where(col_head == head_iota // (heads // 2), first + col_iota // 2, 1 << 20)

    def group(g, carry):
        fetch(0, g).wait()
        fetch(1, g).wait()
        for i in range(8):
            b = g * 8 + i
            slot = 2 * (pos[b] - first)
            inside = jnp.logical_and(slot >= 0, slot < rows)
            base = pl.multiple_of((jnp.clip(slot, 0, rows - 1) // 16) * 16, 16)
            target = jnp.where(inside, slot - base, -100)
            for buf, which in ((kbuf, 0), (vbuf, 1)):
                old = buf[b, pl.ds(base, 16), :].astype(F32)
                new0 = kv_ref[0, which, pl.ds(b, 1), :]
                new1 = kv_ref[1, which, pl.ds(b, 1), :]
                new = jnp.where(row_iota == target, new0, jnp.where(row_iota == target + 1, new1, old))
                buf[b, pl.ds(base, 16), :] = new.astype(BF16)
        scores = []
        for i in range(8):
            b = g * 8 + i
            q = q_ref[pl.ds(b, heads, stride=batch), :].astype(BF16)
            s = lax.dot_general(q, kbuf[b], (((1,), (1,)), ((), ())), preferred_element_type=F32) * (hd ** -0.5)
            scores.append(jnp.where(col_pos <= pos[b], s, NEG_BIG))
        for i in range(8):
            b = g * 8 + i
            s = scores[i]
            top = jnp.max(s, axis=-1, keepdims=True)
            weights = jnp.where(col_pos <= pos[b], jnp.exp(s - top), 0.0)
            total = jnp.sum(weights, axis=-1, keepdims=True)
            where = pl.ds(b, heads, stride=batch)
            acc_ref[where, :] = jnp.dot(weights.astype(BF16), vbuf[b], preferred_element_type=F32)
            mbuf[where, :] = jnp.broadcast_to(top, (heads, hd))
            lbuf[where, :] = jnp.broadcast_to(total, (heads, hd))
        store(0, g).start()
        store(1, g).start()
        return carry

    lax.fori_loop(0, groups, group, 0)
    lane = lax.broadcasted_iota(jnp.int32, (batch, hd), 1)
    packed = jnp.zeros((batch, hd), F32)
    for h in range(heads):
        packed = jnp.where(lane == h, mbuf[h * batch:(h + 1) * batch, :], packed)
        packed = jnp.where(lane == heads + h, lbuf[h * batch:(h + 1) * batch, :], packed)
    stat_ref[...] = packed
    for g in range(groups):
        store(0, g).wait()
        store(1, g).wait()


def output_kernel(
    acc, stat, hid, wo, out,
    hbuf, wob, obf, acc_p, acc_c, acc_y, o_own, o_land, st_p, st_c, st_y, part, land_a, land_b, tot,
    lsem, stsem, dsem, fsem,
):
    z = lax.axis_index("tp")
    me = lax.axis_index("sp")
    core = lax.rem(me, 2)
    mate = me + 1 - 2 * core
    across = lax.rem(me + 2, 4)
    diagonal = across + 1 - 2 * core
    partner = {"sp": mate}
    ynbr = {"sp": across}
    outer = jnp.logical_or(z == 0, z == 3)
    inner = jnp.logical_not(outer)
    z_in = jnp.where(z == 0, 1, jnp.where(z == 1, 2, jnp.where(z == 2, 1, 2)))
    z_out = jnp.where(z == 1, 0, 3)
    heads, batch, hd = acc.shape
    mine = heads // 2
    cols = wob.shape[2]
    per_dev = NC * cols
    rows_s = batch // NS

    hcopy = pltpu.make_async_copy(hid, hbuf, lsem.at[NC])

    def wcopy(j):
        return pltpu.make_async_copy(
            wo.at[:, pl.ds(pl.multiple_of(me * per_dev + j * cols, cols), cols)], wob.at[j], lsem.at[j]
        )

    barrier = pltpu.get_barrier_semaphore()
    pl.semaphore_signal(barrier, inc=1, device_id=partner, device_id_type=MESH)
    pl.semaphore_signal(barrier, inc=1, device_id=ynbr, device_id_type=MESH)

    @pl.when(z > 0)
    def _():
        pl.semaphore_signal(barrier, inc=1, device_id={"tp": z - 1}, device_id_type=MESH)

    @pl.when(z < 3)
    def _():
        pl.semaphore_signal(barrier, inc=1, device_id={"tp": z + 1}, device_id_type=MESH)

    for j in range(NC):
        wcopy(j).start()
    hcopy.start()

    @pl.when(outer)
    def _():
        pl.semaphore_wait(barrier, 3)

    @pl.when(inner)
    def _():
        pl.semaphore_wait(barrier, 4)

    def part_rows(s):
        return pl.ds(s * rows_s, rows_s)

    st_send = remote(stat, st_p, stsem.at[0], stsem.at[1], partner)
    st_send.start()
    p_send = []
    for s in range(NS):
        copy = remote(
            acc.at[pl.ds((1 - core) * mine, mine), part_rows(s)], acc_p.at[:, part_rows(s)],
            dsem.at[0, s], dsem.at[1, s], partner,
        )
        copy.start()
        p_send.append(copy)

    lane = lax.broadcasted_iota(jnp.int32, (batch, hd), 1)

    def merge(a, b):
        top = jnp.maximum(a, b)
        ea = jnp.exp(a - top)
        eb = jnp.exp(b - top)
        la = pltpu.roll(a, hd - heads, 1)
        lb = pltpu.roll(b, hd - heads, 1)
        return top, ea, eb, la * ea + lb * eb

    def own_heads(x):
        return jnp.where(core == 0, x, pltpu.roll(x, hd - mine, 1))

    st_send.wait_recv()
    top, ea, eb, total = merge(own_heads(stat[...]), own_heads(st_p[...]))
    st_c[...] = jnp.where(lane < heads, top, pltpu.roll(total, heads, 1))
    sty_send = remote(st_c, st_y, stsem.at[2], stsem.at[3], ynbr)
    sty_send.start()
    y_send = []
    for s in range(NS):
        p_send[s].wait_recv()
        sl = slice(s * rows_s, (s + 1) * rows_s)
        for h in range(mine):
            acc_c[h, sl, :] = acc[core * mine + h, sl, :] * ea[sl, h:h + 1] + acc_p[h, sl, :] * eb[sl, h:h + 1]
        copy = remote(acc_c.at[:, part_rows(s)], acc_y.at[:, part_rows(s)], dsem.at[2, s], dsem.at[3, s], ynbr)
        copy.start()
        y_send.append(copy)
    sty_send.wait_recv()
    _, ea, eb, total = merge(st_c[...], st_y[...])
    o_send = []
    for s in range(NS):
        y_send[s].wait_recv()
        sl = slice(s * rows_s, (s + 1) * rows_s)
        for h in range(mine):
            o = acc_c[h, sl, :] * ea[sl, h:h + 1] + acc_y[h, sl, :] * eb[sl, h:h + 1]
            o = round_bf16(o / total[sl, h:h + 1])
            o_own[h, sl, :] = o
            obf[sl, pl.ds(pl.multiple_of((core * mine + h) * hd, hd), hd)] = o.astype(BF16)
        copy = remote(o_own.at[:, part_rows(s)], o_land.at[:, part_rows(s)], dsem.at[4, s], dsem.at[5, s], partner)
        copy.start()
        o_send.append(copy)
    for s in range(NS):
        o_send[s].wait_recv()
        sl = slice(s * rows_s, (s + 1) * rows_s)
        for h in range(mine):
            obf[sl, pl.ds(pl.multiple_of(((1 - core) * mine + h) * hd, hd), hd)] = o_land[h, sl, :].astype(BF16)

    def send_a(j):
        return remote(part.at[j], land_a.at[j], fsem.at[0, j], fsem.at[1, j], {"tp": z_in})

    def send_b(j):
        return remote(part.at[j], land_b.at[j], fsem.at[2, j], fsem.at[3, j], {"tp": z_in})

    def send_c(j):
        return remote(tot.at[me, j], tot.at[me, j], fsem.at[4, j], fsem.at[5, j], {"tp": z_out})

    def send_d(j):
        return remote(tot.at[me, j], tot.at[me, j], fsem.at[6, j], fsem.at[7, j], ynbr)

    def send_e(j):
        return remote(tot.at[me, j], tot.at[me, j], fsem.at[8, j], fsem.at[9, j], partner)

    def send_f(j):
        return remote(tot.at[across, j], tot.at[across, j], fsem.at[10, j], fsem.at[11, j], partner)

    def project(j, carry):
        wcopy(j).wait()
        part[j] = jnp.dot(obf[...], wob[j], preferred_element_type=F32)

        @pl.when(outer)
        def _():
            send_a(j).start()

        return carry

    lax.fori_loop(0, NC, project, 0)
    hcopy.wait()

    def emit(quarter, j):
        where = pl.ds(pl.multiple_of(quarter * per_dev + j * cols, cols), cols)
        out[:, where] = (hbuf[:, where].astype(F32) + tot[quarter, j]).astype(BF16)

    def share(j):
        send_d(j).start()
        send_e(j).start()
        emit(me, j)

    def collect(j):
        send_d(j).wait_recv()
        send_f(j).start()
        emit(across, j)
        send_e(j).wait_recv()
        emit(mate, j)

    def last(j):
        send_f(j).wait_recv()
        emit(diagonal, j)

    @pl.when(outer)
    def _():
        for j in range(NC + LAG):
            if j < NC:
                send_c(j).wait_recv()
                share(j)
            if j >= LAG:
                collect(j - LAG)
        for j in range(NC):
            last(j)
        for j in range(NC):
            send_a(j).wait_send()

    @pl.when(inner)
    def _():
        for j in range(NC + 2 * LAG):
            if j < NC:
                send_a(j).wait_recv()
                part[j] = part[j] + land_a[j]
                send_b(j).start()
            if LAG <= j < NC + LAG:
                k = j - LAG
                send_b(k).wait_recv()
                tot[me, k] = part[k] + land_b[k]
                send_c(k).start()
                share(k)
            if j >= 2 * LAG:
                collect(j - 2 * LAG)
        for j in range(NC):
            last(j)
        for j in range(NC):
            send_b(j).wait_send()
            send_c(j).wait_send()

    st_send.wait_send()
    sty_send.wait_send()
    for s in range(NS):
        p_send[s].wait_send()
        y_send[s].wait_send()
        o_send[s].wait_send()
    for j in range(NC):
        send_d(j).wait_send()
        send_e(j).wait_send()
        send_f(j).wait_send()


def solution(mesh):
    vmem = pl.BlockSpec(memory_space=pltpu.VMEM)
    smem = pl.BlockSpec(memory_space=pltpu.SMEM)
    hbm = pl.BlockSpec(memory_space=pl.ANY)
    dma = pltpu.SemaphoreType.DMA

    def local_step(hidden, norm_gain, w_query, w_key, w_value, w_out, k_cache, v_cache, positions):
        batch, seq_local, kv_local, hd = k_cache.shape
        d_model, q_cols = w_query.shape
        heads = q_cols // hd
        rows = seq_local * kv_local
        half_dim = hd // 2
        inv_freq = 1.0 / (ROPE_BASE ** (jnp.arange(half_dim, dtype=F32) * 2.0 / hd))
        angles = positions.astype(F32)[:, None] * inv_freq[None, :]
        cosine, sine = jnp.cos(angles), jnp.sin(angles)
        cosf = jnp.concatenate([cosine, cosine], axis=-1)
        sinf = jnp.concatenate([-sine, sine], axis=-1)

        tiles = 4
        tcols = q_cols // 2 // tiles
        half_rows = heads // 2 * batch
        q, kv = pl.pallas_call(
            qkv_kernel,
            out_shape=(
                jax.ShapeDtypeStruct((heads * batch, hd), F32),
                jax.ShapeDtypeStruct((2, 2, batch, hd), F32),
            ),
            in_specs=[hbm, hbm, vmem, vmem, hbm, hbm, hbm],
            out_specs=(vmem, vmem),
            scratch_shapes=[
                pltpu.VMEM((batch, d_model), BF16),
                pltpu.VMEM((1, d_model), F32),
                pltpu.VMEM((batch, d_model), BF16),
                pltpu.VMEM((tiles, d_model, tcols), BF16),
                pltpu.VMEM((d_model, 2 * hd), BF16),
                pltpu.VMEM((half_rows, hd), F32),
                pltpu.VMEM((half_rows, hd), F32),
                pltpu.VMEM((2, batch, hd), F32),
                pltpu.VMEM((2, batch, hd), F32),
                dma((4,)),
                dma((tiles,)),
                dma((tiles + 1,)),
                dma((tiles + 1,)),
            ],
            compiler_params=pltpu.CompilerParams(
                collective_id=0, has_side_effects=True, vmem_limit_bytes=VMEM_LIMIT
            ),
            name="qkv",
        )(hidden, norm_gain.reshape(1, d_model), cosf, sinf, w_query, w_key, w_value)

        cache3 = jax.ShapeDtypeStruct((batch, rows, hd), BF16)
        k_upd, v_upd, acc, stat = pl.pallas_call(
            attention_kernel,
            out_shape=(
                cache3, cache3,
                jax.ShapeDtypeStruct((heads * batch, hd), F32),
                jax.ShapeDtypeStruct((batch, hd), F32),
            ),
            in_specs=[smem, vmem, vmem, hbm, hbm],
            out_specs=(hbm, hbm, vmem, vmem),
            scratch_shapes=[
                pltpu.VMEM((batch, rows, hd), BF16),
                pltpu.VMEM((batch, rows, hd), BF16),
                pltpu.VMEM((heads * batch, hd), F32),
                pltpu.VMEM((heads * batch, hd), F32),
                dma((2, batch // 8)),
                dma((2, batch // 8)),
            ],
            compiler_params=pltpu.CompilerParams(vmem_limit_bytes=VMEM_LIMIT),
            name="attention",
        )(positions, q, kv, k_cache.reshape(batch, rows, hd), v_cache.reshape(batch, rows, hd))

        mine = heads // 2
        ocols = d_model // 4 // NC
        buf = pltpu.VMEM((mine, batch, hd), F32)
        st = pltpu.VMEM((batch, hd), F32)
        chunk = pltpu.VMEM((NC, batch, ocols), F32)
        out = pl.pallas_call(
            output_kernel,
            out_shape=jax.ShapeDtypeStruct((batch, d_model), BF16),
            in_specs=[vmem, vmem, hbm, hbm],
            out_specs=vmem,
            scratch_shapes=[
                pltpu.VMEM((batch, d_model), BF16),
                pltpu.VMEM((NC, q_cols, ocols), BF16),
                pltpu.VMEM((batch, q_cols), BF16),
                buf, buf, buf, buf, buf, st, st, st, chunk, chunk, chunk,
                pltpu.VMEM((4, NC, batch, ocols), F32),
                dma((NC + 1,)),
                dma((4,)),
                dma((6, NS)),
                dma((12, NC)),
            ],
            compiler_params=pltpu.CompilerParams(
                collective_id=1, has_side_effects=True, vmem_limit_bytes=VMEM_LIMIT
            ),
            name="output",
        )(acc.reshape(heads, batch, hd), stat, hidden, w_out)
        return out, k_upd.reshape(k_cache.shape), v_upd.reshape(v_cache.shape)

    cache_spec = P("dp", "sp", "tp", None)
    specs_in = (P("dp", None), P(None), P(None, "tp"), P(None, "tp"), P(None, "tp"), P("tp", None), cache_spec, cache_spec, P("dp"))
    specs_out = (P("dp", None), cache_spec, cache_spec)
    return jax.shard_map(local_step, mesh=mesh, in_specs=specs_in, out_specs=specs_out, check_vma=False)
```

```python
import math

import jax
import jax.numpy as jnp
from jax import lax
from jax.experimental import pallas as pl
from jax.experimental.pallas import tpu as pltpu
from jax.sharding import PartitionSpec as P

ROPE_BASE = 1000000.0
EPS = 1e-5
NEG_BIG = float(jnp.finfo(jnp.float32).min)
MESH = pl.DeviceIdType.MESH
F32 = jnp.float32
BF16 = jnp.bfloat16
NC = 16
WIDE = 2
NS = 4
LAG = 4


def remote(src, dst, send, recv, device):
    return pltpu.make_async_remote_copy(
        src_ref=src, dst_ref=dst, send_sem=send, recv_sem=recv, device_id=device, device_id_type=MESH
    )


def round_bf16(x):
    return x.astype(BF16).astype(F32)


def qkv_kernel(
    pos, hid, gain, wq, wk, wv, kc, vc, q_out, kv_out, kc_out, vc_out,
    pos_s, hbuf, gbuf, rbuf, wqb, wkvb, pieces, psem, hsem, wsem, csem, xsem,
):
    me = lax.axis_index("sp")
    core = lax.rem(me, 2)
    mate = me + 1 - 2 * core
    across = lax.rem(me + 2, 4)
    partner = {"sp": mate}
    ynbr = {"sp": across}
    batch, d_model = hid.shape
    tiles, _, cols = wqb.shape
    quarter = tiles * cols
    hcopy = pltpu.make_async_copy(hid, hbuf, hsem.at[0])
    gcopy = pltpu.make_async_copy(gain, gbuf, hsem.at[1])
    pcopy = pltpu.make_async_copy(pos, pos_s, psem.at[0])
    hcopy.start()
    gcopy.start()
    pcopy.start()
    head_cols = pl.ds(pl.multiple_of(core * 128, 128), 128)
    keys = me < 2

    @pl.when(keys)
    def _():
        pltpu.make_async_copy(wk.at[:, head_cols], wkvb, hsem.at[2]).start()

    @pl.when(jnp.logical_not(keys))
    def _():
        pltpu.make_async_copy(wv.at[:, head_cols], wkvb, hsem.at[2]).start()

    def wcopy(t):
        return pltpu.make_async_copy(
            wq.at[:, pl.ds(pl.multiple_of(me * quarter + t * cols, cols), cols)], wqb.at[t], wsem.at[t]
        )

    for t in range(tiles):
        wcopy(t).start()
    barrier = pltpu.get_barrier_semaphore()
    pl.semaphore_signal(barrier, inc=1, device_id=partner, device_id_type=MESH)
    pl.semaphore_signal(barrier, inc=1, device_id=ynbr, device_id_type=MESH)

    def cache_copy(which, g):
        src, dst = ((kc, kc_out), (vc, vc_out))[which]
        rows = pl.ds(g * (batch // 4), batch // 4)
        return pltpu.make_async_copy(src.at[rows], dst.at[rows], csem.at[which, g])

    pcopy.wait()
    lane = lax.broadcasted_iota(jnp.int32, (batch, 128), 1)
    row = lax.broadcasted_iota(jnp.int32, (batch, 128), 0)
    position = jnp.zeros((batch, 128), jnp.int32)
    for b in range(batch):
        position = jnp.where(row == b, pos_s[b], position)
    index = jnp.where(lane < 64, lane, lane - 64).astype(F32)
    angle = position.astype(F32) * jnp.exp(index * (-2.0 / 128 * math.log(ROPE_BASE)))
    cosf = jnp.cos(angle)
    sinf = jnp.where(lane < 64, -1.0, 1.0) * jnp.sin(angle)

    hcopy.wait()
    gcopy.wait()

    def norm_rows(i, carry):
        rows = pl.ds(pl.multiple_of(i * 16, 16), 16)
        x = hbuf[rows, :].astype(F32)
        scale = lax.rsqrt(jnp.sum(x * x, axis=-1, keepdims=True) * (1.0 / d_model) + EPS)
        rbuf[rows, :] = (x * scale * gbuf[...]).astype(BF16)
        return carry

    lax.fori_loop(0, batch // 16, norm_rows, 0)

    def rotate(x):
        return x * cosf + pltpu.roll(x, 64, 1) * sinf

    def span(p):
        return pl.ds(4, 1) if p == 0 else pl.ds(2 * (p - 1), 2)

    def exchange(kind, owner, p, device):
        part = pieces.at[owner, span(p)]
        return remote(part, part, xsem.at[2 * kind, p], xsem.at[2 * kind + 1, p], device)

    def publish(p):
        exchange(0, me, p, ynbr).start()
        exchange(1, me, p, partner).start()

    pltpu.make_async_copy(wk.at[:, head_cols], wkvb, hsem.at[2]).wait()
    kv = jnp.dot(rbuf[...], wkvb[...], preferred_element_type=F32)
    pieces[me, 4] = round_bf16(jnp.where(keys, rotate(kv), kv))
    pl.semaphore_wait(barrier, 2)
    publish(0)
    for t in range(tiles):
        wcopy(t).wait()
        if t == tiles - 1:
            for g in range(4):
                cache_copy(0, g).start()
                cache_copy(1, g).start()
        q = jnp.dot(rbuf[...], wqb[t], preferred_element_type=F32)
        for h in range(2):
            pieces[me, 2 * t + h] = round_bf16(rotate(q[:, h * 128:(h + 1) * 128]))
        publish(t + 1)
    for p in range(tiles + 1):
        exchange(0, me, p, ynbr).wait_recv()
        exchange(2, across, p, partner).start()
    for p in range(tiles + 1):
        exchange(1, me, p, partner).wait_recv()
        exchange(2, across, p, partner).wait_recv()
    for owner in range(4):
        for h in range(4):
            q_out[pl.ds((owner * 4 + h) * batch, batch), :] = pieces[owner, h]
        kv_out[owner % 2, owner // 2] = pieces[owner, 4]
    for p in range(tiles + 1):
        exchange(0, me, p, ynbr).wait_send()
        exchange(1, me, p, partner).wait_send()
        exchange(2, across, p, partner).wait_send()
    for g in range(4):
        cache_copy(0, g).wait()
        cache_copy(1, g).wait()


def attention_kernel(
    pos, q_ref, kv_ref, kc, vc, ko, vo, acc_ref, stat_ref, kbuf, vbuf, mbuf, lbuf, osem,
):
    batch, rows, hd = kbuf.shape
    heads = acc_ref.shape[0] // batch
    groups = batch // 8
    me = lax.axis_index("sp")
    first = me * (rows // 2)

    def seqs(g):
        return pl.ds(pl.multiple_of(g * 8, 8), 8)

    def store(which, g):
        src, dst = ((kbuf, ko), (vbuf, vo))[which]
        return pltpu.make_async_copy(src.at[seqs(g)], dst.at[seqs(g)], osem.at[which, g])

    row_iota = lax.broadcasted_iota(jnp.int32, (16, hd), 0)
    col_iota = lax.broadcasted_iota(jnp.int32, (heads, rows), 1)
    head_iota = lax.broadcasted_iota(jnp.int32, (heads, rows), 0)
    col_head = lax.rem(col_iota, 2)
    col_pos = jnp.where(col_head == head_iota // (heads // 2), first + col_iota // 2, 1 << 20)

    def group(g, carry):
        for i in range(8):
            b = g * 8 + i
            slot = 2 * (pos[b] - first)
            inside = jnp.logical_and(slot >= 0, slot < rows)
            base = pl.multiple_of((jnp.clip(slot, 0, rows - 1) // 16) * 16, 16)
            target = jnp.where(inside, slot - base, -100)
            for buf, which in ((kbuf, 0), (vbuf, 1)):
                old = buf[b, pl.ds(base, 16), :].astype(F32)
                new0 = kv_ref[0, which, pl.ds(b, 1), :]
                new1 = kv_ref[1, which, pl.ds(b, 1), :]
                new = jnp.where(row_iota == target, new0, jnp.where(row_iota == target + 1, new1, old))
                buf[b, pl.ds(base, 16), :] = new.astype(BF16)
        scores = []
        for i in range(8):
            b = g * 8 + i
            q = q_ref[pl.ds(b, heads, stride=batch), :].astype(BF16)
            s = lax.dot_general(q, kbuf[b], (((1,), (1,)), ((), ())), preferred_element_type=F32) * (hd ** -0.5)
            scores.append(jnp.where(col_pos <= pos[b], s, NEG_BIG))
        for i in range(8):
            b = g * 8 + i
            s = scores[i]
            top = jnp.max(s, axis=-1, keepdims=True)
            weights = jnp.where(col_pos <= pos[b], jnp.exp(s - top), 0.0)
            total = jnp.sum(weights, axis=-1, keepdims=True)
            where = pl.ds(b, heads, stride=batch)
            acc_ref[where, :] = jnp.dot(weights.astype(BF16), vbuf[b], preferred_element_type=F32)
            mbuf[where, :] = jnp.broadcast_to(top, (heads, hd))
            lbuf[where, :] = jnp.broadcast_to(total, (heads, hd))
        store(0, g).start()
        store(1, g).start()
        return carry

    lax.fori_loop(0, groups, group, 0)
    lane = lax.broadcasted_iota(jnp.int32, (batch, hd), 1)
    packed = jnp.zeros((batch, hd), F32)
    for h in range(heads):
        packed = jnp.where(lane == h, mbuf[h * batch:(h + 1) * batch, :], packed)
        packed = jnp.where(lane == heads + h, lbuf[h * batch:(h + 1) * batch, :], packed)
    stat_ref[...] = packed
    for g in range(groups):
        store(0, g).wait()
        store(1, g).wait()


def output_kernel(
    acc, stat, hid, wo, out,
    hbuf, wob, obf, acc_p, acc_c, acc_y, o_own, o_land, st_p, st_c, st_y, part, land_a, land_b, tot,
    lsem, stsem, dsem, fsem,
):
    z = lax.axis_index("tp")
    me = lax.axis_index("sp")
    core = lax.rem(me, 2)
    mate = me + 1 - 2 * core
    across = lax.rem(me + 2, 4)
    diagonal = across + 1 - 2 * core
    partner = {"sp": mate}
    ynbr = {"sp": across}
    outer = jnp.logical_or(z == 0, z == 3)
    inner = jnp.logical_not(outer)
    z_in = jnp.where(z == 0, 1, jnp.where(z == 1, 2, jnp.where(z == 2, 1, 2)))
    z_out = jnp.where(z == 1, 0, 3)
    heads, batch, hd = acc.shape
    mine = heads // 2
    tile = wob.shape[2]
    cols = tile // WIDE
    per_dev = NC * cols
    rows_s = batch // NS

    hcopy = pltpu.make_async_copy(hid, hbuf, lsem.at[NC // WIDE])

    def wcopy(j):
        return pltpu.make_async_copy(
            wo.at[:, pl.ds(pl.multiple_of(me * per_dev + j * tile, tile), tile)], wob.at[j], lsem.at[j]
        )

    barrier = pltpu.get_barrier_semaphore()
    pl.semaphore_signal(barrier, inc=1, device_id=partner, device_id_type=MESH)
    pl.semaphore_signal(barrier, inc=1, device_id=ynbr, device_id_type=MESH)

    @pl.when(z > 0)
    def _():
        pl.semaphore_signal(barrier, inc=1, device_id={"tp": z - 1}, device_id_type=MESH)

    @pl.when(z < 3)
    def _():
        pl.semaphore_signal(barrier, inc=1, device_id={"tp": z + 1}, device_id_type=MESH)

    for j in range(NC // WIDE):
        wcopy(j).start()
    hcopy.start()

    @pl.when(outer)
    def _():
        pl.semaphore_wait(barrier, 3)

    @pl.when(inner)
    def _():
        pl.semaphore_wait(barrier, 4)

    def part_rows(s):
        return pl.ds(s * rows_s, rows_s)

    st_send = remote(stat, st_p, stsem.at[0], stsem.at[1], partner)
    st_send.start()
    p_send = []
    for s in range(NS):
        copy = remote(
            acc.at[pl.ds((1 - core) * mine, mine), part_rows(s)], acc_p.at[:, part_rows(s)],
            dsem.at[0, s], dsem.at[1, s], partner,
        )
        copy.start()
        p_send.append(copy)

    lane = lax.broadcasted_iota(jnp.int32, (batch, hd), 1)

    def merge(a, b):
        top = jnp.maximum(a, b)
        ea = jnp.exp(a - top)
        eb = jnp.exp(b - top)
        la = pltpu.roll(a, hd - heads, 1)
        lb = pltpu.roll(b, hd - heads, 1)
        return top, ea, eb, la * ea + lb * eb

    def own_heads(x):
        return jnp.where(core == 0, x, pltpu.roll(x, hd - mine, 1))

    st_send.wait_recv()
    top, ea, eb, total = merge(own_heads(stat[...]), own_heads(st_p[...]))
    st_c[...] = jnp.where(lane < heads, top, pltpu.roll(total, heads, 1))
    sty_send = remote(st_c, st_y, stsem.at[2], stsem.at[3], ynbr)
    sty_send.start()
    y_send = []
    for s in range(NS):
        p_send[s].wait_recv()
        sl = slice(s * rows_s, (s + 1) * rows_s)
        for h in range(mine):
            acc_c[h, sl, :] = acc[core * mine + h, sl, :] * ea[sl, h:h + 1] + acc_p[h, sl, :] * eb[sl, h:h + 1]
        copy = remote(acc_c.at[:, part_rows(s)], acc_y.at[:, part_rows(s)], dsem.at[2, s], dsem.at[3, s], ynbr)
        copy.start()
        y_send.append(copy)
    sty_send.wait_recv()
    _, ea, eb, total = merge(st_c[...], st_y[...])
    o_send = []
    for s in range(NS):
        y_send[s].wait_recv()
        sl = slice(s * rows_s, (s + 1) * rows_s)
        for h in range(mine):
            o = acc_c[h, sl, :] * ea[sl, h:h + 1] + acc_y[h, sl, :] * eb[sl, h:h + 1]
            o = round_bf16(o / total[sl, h:h + 1])
            o_own[h, sl, :] = o
            obf[sl, pl.ds(pl.multiple_of((core * mine + h) * hd, hd), hd)] = o.astype(BF16)
        copy = remote(o_own.at[:, part_rows(s)], o_land.at[:, part_rows(s)], dsem.at[4, s], dsem.at[5, s], partner)
        copy.start()
        o_send.append(copy)
    for s in range(NS):
        o_send[s].wait_recv()
        sl = slice(s * rows_s, (s + 1) * rows_s)
        for h in range(mine):
            obf[sl, pl.ds(pl.multiple_of(((1 - core) * mine + h) * hd, hd), hd)] = o_land[h, sl, :].astype(BF16)

    def send_a(j):
        return remote(part.at[j], land_a.at[j], fsem.at[0, j], fsem.at[1, j], {"tp": z_in})

    def send_b(j):
        return remote(part.at[j], land_b.at[j], fsem.at[2, j], fsem.at[3, j], {"tp": z_in})

    def send_c(j):
        return remote(tot.at[me, j], tot.at[me, j], fsem.at[4, j], fsem.at[5, j], {"tp": z_out})

    def send_d(j):
        return remote(tot.at[me, j], tot.at[me, j], fsem.at[6, j], fsem.at[7, j], ynbr)

    def send_e(j):
        return remote(tot.at[me, j], tot.at[me, j], fsem.at[8, j], fsem.at[9, j], partner)

    def send_f(j):
        return remote(tot.at[across, j], tot.at[across, j], fsem.at[10, j], fsem.at[11, j], partner)

    def project(j, carry):
        wcopy(j).wait()
        product = jnp.dot(obf[...], wob[j], preferred_element_type=F32)
        for w in range(WIDE):
            part[j * WIDE + w] = product[:, w * cols:(w + 1) * cols]

        @pl.when(outer)
        def _():
            for w in range(WIDE):
                send_a(j * WIDE + w).start()

        return carry

    lax.fori_loop(0, NC // WIDE, project, 0)
    hcopy.wait()

    def emit(quarter, j):
        where = pl.ds(pl.multiple_of(quarter * per_dev + j * cols, cols), cols)
        out[:, where] = (hbuf[:, where].astype(F32) + tot[quarter, j]).astype(BF16)

    def share(j):
        send_d(j).start()
        send_e(j).start()
        emit(me, j)

    def collect(j):
        send_d(j).wait_recv()
        send_f(j).start()
        emit(across, j)
        send_e(j).wait_recv()
        emit(mate, j)

    def last(j):
        send_f(j).wait_recv()
        emit(diagonal, j)

    @pl.when(outer)
    def _():
        for j in range(NC + LAG):
            if j < NC:
                send_c(j).wait_recv()
                share(j)
            if j >= LAG:
                collect(j - LAG)
        for j in range(NC):
            last(j)
        for j in range(NC):
            send_a(j).wait_send()

    @pl.when(inner)
    def _():
        for j in range(NC + 2 * LAG):
            if j < NC:
                send_a(j).wait_recv()
                part[j] = part[j] + land_a[j]
                send_b(j).start()
            if LAG <= j < NC + LAG:
                k = j - LAG
                send_b(k).wait_recv()
                tot[me, k] = part[k] + land_b[k]
                send_c(k).start()
                share(k)
            if j >= 2 * LAG:
                collect(j - 2 * LAG)
        for j in range(NC):
            last(j)
        for j in range(NC):
            send_b(j).wait_send()
            send_c(j).wait_send()

    st_send.wait_send()
    sty_send.wait_send()
    for s in range(NS):
        p_send[s].wait_send()
        y_send[s].wait_send()
        o_send[s].wait_send()
    for j in range(NC):
        send_d(j).wait_send()
        send_e(j).wait_send()
        send_f(j).wait_send()


def solution(mesh):
    vmem = pl.BlockSpec(memory_space=pltpu.VMEM)
    smem = pl.BlockSpec(memory_space=pltpu.SMEM)
    hbm = pl.BlockSpec(memory_space=pltpu.HBM)
    dma = pltpu.SemaphoreType.DMA

    def keep(x):
        return pltpu.with_memory_space_constraint(x, pltpu.VMEM)

    def stay(x):
        return pltpu.with_memory_space_constraint(x, pltpu.HBM)

    def params(mib, collective=None):
        if collective is None:
            return pltpu.CompilerParams(vmem_limit_bytes=mib * 2**20)
        return pltpu.CompilerParams(vmem_limit_bytes=mib * 2**20, collective_id=collective, has_side_effects=True)

    def local_step(hidden, norm_gain, w_query, w_key, w_value, w_out, k_cache, v_cache, positions):
        batch, seq_local, kv_local, hd = k_cache.shape
        d_model, q_cols = w_query.shape
        heads = q_cols // hd
        rows = seq_local * kv_local
        tiles = 2
        tcols = q_cols // 4 // tiles
        cache = (batch, rows, hd)
        acc_type = pltpu.VMEM((heads * batch, hd), F32)
        q, kv, k_in, v_in = pl.pallas_call(
            qkv_kernel,
            out_shape=(acc_type, pltpu.VMEM((2, 2, batch, hd), F32), pltpu.VMEM(cache, BF16), pltpu.VMEM(cache, BF16)),
            in_specs=[hbm] * 8,
            out_specs=(vmem,) * 4,
            scratch_shapes=[
                pltpu.SMEM((batch,), jnp.int32),
                pltpu.VMEM((batch, d_model), BF16),
                pltpu.VMEM((1, d_model), F32),
                pltpu.VMEM((batch, d_model), BF16),
                pltpu.VMEM((tiles, d_model, tcols), BF16),
                pltpu.VMEM((d_model, hd), BF16),
                pltpu.VMEM((4, 5, batch, hd), F32),
                dma((1,)),
                dma((3,)),
                dma((tiles,)),
                dma((2, 4)),
                dma((6, tiles + 1)),
            ],
            compiler_params=params(24, 0),
            name="qkv",
        )(
            stay(positions), stay(hidden), stay(norm_gain.reshape(1, d_model)), stay(w_query), stay(w_key), stay(w_value),
            stay(k_cache.reshape(cache)), stay(v_cache.reshape(cache)),
        )

        k_upd, v_upd, acc, stat, _, _ = pl.pallas_call(
            attention_kernel,
            out_shape=(
                jax.ShapeDtypeStruct(cache, BF16), jax.ShapeDtypeStruct(cache, BF16),
                acc_type, pltpu.VMEM((batch, hd), F32),
                pltpu.VMEM(cache, BF16), pltpu.VMEM(cache, BF16),
            ),
            in_specs=[smem, vmem, vmem, vmem, vmem],
            out_specs=(hbm, hbm, vmem, vmem, vmem, vmem),
            input_output_aliases={3: 4, 4: 5},
            scratch_shapes=[
                pltpu.VMEM((heads * batch, hd), F32),
                pltpu.VMEM((heads * batch, hd), F32),
                dma((2, batch // 8)),
            ],
            compiler_params=params(10),
            name="attention",
        )(positions, keep(q), keep(kv), keep(k_in), keep(v_in))

        mine = heads // 2
        ocols = d_model // 4 // NC
        buf = pltpu.VMEM((mine, batch, hd), F32)
        st = pltpu.VMEM((batch, hd), F32)
        chunk = pltpu.VMEM((NC, batch, ocols), F32)
        out = pl.pallas_call(
            output_kernel,
            out_shape=pltpu.VMEM((batch, d_model), BF16),
            in_specs=[vmem, vmem, hbm, hbm],
            out_specs=vmem,
            scratch_shapes=[
                pltpu.VMEM((batch, d_model), BF16),
                pltpu.VMEM((NC // WIDE, q_cols, ocols * WIDE), BF16),
                pltpu.VMEM((batch, q_cols), BF16),
                buf, buf, buf, buf, buf, st, st, st, chunk, chunk, chunk,
                pltpu.VMEM((4, NC, batch, ocols), F32),
                dma((NC // WIDE + 1,)),
                dma((4,)),
                dma((6, NS)),
                dma((12, NC)),
            ],
            compiler_params=params(24, 1),
            name="output",
        )(keep(acc.reshape(heads, batch, hd)), keep(stat), stay(hidden), stay(w_out))
        return out, k_upd.reshape(k_cache.shape), v_upd.reshape(v_cache.shape)

    cache_spec = P("dp", "sp", "tp", None)
    specs_in = (P("dp", None), P(None), P(None, "tp"), P(None, "tp"), P(None, "tp"), P("tp", None), cache_spec, cache_spec, P("dp"))
    specs_out = (P("dp", None), cache_spec, cache_spec)
    return jax.shard_map(local_step, mesh=mesh, in_specs=specs_in, out_specs=specs_out, check_vma=False)
```

```python
import math

import jax
import jax.numpy as jnp
from jax import lax
from jax.experimental import pallas as pl
from jax.experimental.pallas import tpu as pltpu
from jax.sharding import PartitionSpec as P

ROPE_BASE = 1000000.0
EPS = 1e-5
NEG_BIG = float(jnp.finfo(jnp.float32).min)
MESH = pl.DeviceIdType.MESH
F32 = jnp.float32
BF16 = jnp.bfloat16
TILES = 16
FIRST = 6
MOST = max(FIRST, TILES - FIRST)
HALVES = 2
NS = 4
LAG = 4


def remote(src, dst, send, recv, device):
    return pltpu.make_async_remote_copy(
        src_ref=src, dst_ref=dst, send_sem=send, recv_sem=recv, device_id=device, device_id_type=MESH
    )


def round_bf16(x):
    return x.astype(BF16).astype(F32)


def qkv_kernel(
    pos, hid, gain, wq, wk, wv, kc, vc, q_out, kv_out, kc_out, vc_out,
    pos_s, hbuf, gbuf, rbuf, wqb, wkvb, pieces, psem, hsem, wsem, csem, xsem,
):
    me = lax.axis_index("sp")
    core = lax.rem(me, 2)
    mate = me + 1 - 2 * core
    across = lax.rem(me + 2, 4)
    partner = {"sp": mate}
    ynbr = {"sp": across}
    batch, d_model = hid.shape
    tiles, _, cols = wqb.shape
    quarter = tiles * cols
    hcopy = pltpu.make_async_copy(hid, hbuf, hsem.at[0])
    gcopy = pltpu.make_async_copy(gain, gbuf, hsem.at[1])
    pcopy = pltpu.make_async_copy(pos, pos_s, psem.at[0])
    hcopy.start()
    gcopy.start()
    pcopy.start()
    head_cols = pl.ds(pl.multiple_of(core * 128, 128), 128)
    keys = me < 2

    @pl.when(keys)
    def _():
        pltpu.make_async_copy(wk.at[:, head_cols], wkvb, hsem.at[2]).start()

    @pl.when(jnp.logical_not(keys))
    def _():
        pltpu.make_async_copy(wv.at[:, head_cols], wkvb, hsem.at[2]).start()

    def wcopy(t):
        return pltpu.make_async_copy(
            wq.at[:, pl.ds(pl.multiple_of(me * quarter + t * cols, cols), cols)], wqb.at[t], wsem.at[t]
        )

    for t in range(tiles):
        wcopy(t).start()
    barrier = pltpu.get_barrier_semaphore()
    pl.semaphore_signal(barrier, inc=1, device_id=partner, device_id_type=MESH)
    pl.semaphore_signal(barrier, inc=1, device_id=ynbr, device_id_type=MESH)

    def cache_copy(which, g):
        src, dst = ((kc, kc_out), (vc, vc_out))[which]
        rows = pl.ds(g * (batch // 4), batch // 4)
        return pltpu.make_async_copy(src.at[rows], dst.at[rows], csem.at[which, g])

    pcopy.wait()
    lane = lax.broadcasted_iota(jnp.int32, (batch, 128), 1)
    row = lax.broadcasted_iota(jnp.int32, (batch, 128), 0)
    position = jnp.zeros((batch, 128), jnp.int32)
    for b in range(batch):
        position = jnp.where(row == b, pos_s[b], position)
    index = jnp.where(lane < 64, lane, lane - 64).astype(F32)
    angle = position.astype(F32) * jnp.exp(index * (-2.0 / 128 * math.log(ROPE_BASE)))
    cosf = jnp.cos(angle)
    sinf = jnp.where(lane < 64, -1.0, 1.0) * jnp.sin(angle)

    hcopy.wait()
    gcopy.wait()

    def norm_rows(i, carry):
        rows = pl.ds(pl.multiple_of(i * 16, 16), 16)
        x = hbuf[rows, :].astype(F32)
        scale = lax.rsqrt(jnp.sum(x * x, axis=-1, keepdims=True) * (1.0 / d_model) + EPS)
        rbuf[rows, :] = (x * scale * gbuf[...]).astype(BF16)
        return carry

    lax.fori_loop(0, batch // 16, norm_rows, 0)

    def rotate(x):
        return x * cosf + pltpu.roll(x, 64, 1) * sinf

    def span(p):
        return pl.ds(4, 1) if p == 0 else pl.ds(2 * (p - 1), 2)

    def exchange(kind, owner, p, device):
        part = pieces.at[owner, span(p)]
        return remote(part, part, xsem.at[2 * kind, p], xsem.at[2 * kind + 1, p], device)

    def publish(p):
        exchange(0, me, p, ynbr).start()
        exchange(1, me, p, partner).start()

    pltpu.make_async_copy(wk.at[:, head_cols], wkvb, hsem.at[2]).wait()
    kv = jnp.dot(rbuf[...], wkvb[...], preferred_element_type=F32)
    pieces[me, 4] = round_bf16(jnp.where(keys, rotate(kv), kv))
    pl.semaphore_wait(barrier, 2)
    publish(0)
    for t in range(tiles):
        wcopy(t).wait()
        if t == tiles - 1:
            for g in range(4):
                cache_copy(0, g).start()
                cache_copy(1, g).start()
        q = jnp.dot(rbuf[...], wqb[t], preferred_element_type=F32)
        for h in range(2):
            pieces[me, 2 * t + h] = round_bf16(rotate(q[:, h * 128:(h + 1) * 128]))
        publish(t + 1)
    for p in range(tiles + 1):
        exchange(0, me, p, ynbr).wait_recv()
        exchange(2, across, p, partner).start()
    for p in range(tiles + 1):
        exchange(1, me, p, partner).wait_recv()
        exchange(2, across, p, partner).wait_recv()
    for owner in range(4):
        for h in range(4):
            q_out[pl.ds((owner * 4 + h) * batch, batch), :] = pieces[owner, h]
        kv_out[owner % 2, owner // 2] = pieces[owner, 4]
    for p in range(tiles + 1):
        exchange(0, me, p, ynbr).wait_send()
        exchange(1, me, p, partner).wait_send()
        exchange(2, across, p, partner).wait_send()
    for g in range(4):
        cache_copy(0, g).wait()
        cache_copy(1, g).wait()


def attention_kernel(
    pos, q_ref, kv_ref, kc, vc, ko, vo, acc_ref, stat_ref, kbuf, vbuf, mbuf, lbuf, osem,
):
    batch, rows, hd = kbuf.shape
    heads = acc_ref.shape[0] // batch
    groups = batch // 8
    me = lax.axis_index("sp")
    first = me * (rows // 2)

    def seqs(g):
        return pl.ds(pl.multiple_of(g * 8, 8), 8)

    def store(which, g):
        src, dst = ((kbuf, ko), (vbuf, vo))[which]
        return pltpu.make_async_copy(src.at[seqs(g)], dst.at[seqs(g)], osem.at[which, g])

    row_iota = lax.broadcasted_iota(jnp.int32, (16, hd), 0)
    col_iota = lax.broadcasted_iota(jnp.int32, (heads, rows), 1)
    head_iota = lax.broadcasted_iota(jnp.int32, (heads, rows), 0)
    col_head = lax.rem(col_iota, 2)
    col_pos = jnp.where(col_head == head_iota // (heads // 2), first + col_iota // 2, 1 << 20)

    def group(g, carry):
        for i in range(8):
            b = g * 8 + i
            slot = 2 * (pos[b] - first)
            inside = jnp.logical_and(slot >= 0, slot < rows)
            base = pl.multiple_of((jnp.clip(slot, 0, rows - 1) // 16) * 16, 16)
            target = jnp.where(inside, slot - base, -100)
            for buf, which in ((kbuf, 0), (vbuf, 1)):
                old = buf[b, pl.ds(base, 16), :].astype(F32)
                new0 = kv_ref[0, which, pl.ds(b, 1), :]
                new1 = kv_ref[1, which, pl.ds(b, 1), :]
                new = jnp.where(row_iota == target, new0, jnp.where(row_iota == target + 1, new1, old))
                buf[b, pl.ds(base, 16), :] = new.astype(BF16)
        scores = []
        for i in range(8):
            b = g * 8 + i
            q = q_ref[pl.ds(b, heads, stride=batch), :].astype(BF16)
            s = lax.dot_general(q, kbuf[b], (((1,), (1,)), ((), ())), preferred_element_type=F32) * (hd ** -0.5)
            scores.append(jnp.where(col_pos <= pos[b], s, NEG_BIG))
        for i in range(8):
            b = g * 8 + i
            s = scores[i]
            top = jnp.max(s, axis=-1, keepdims=True)
            weights = jnp.where(col_pos <= pos[b], jnp.exp(s - top), 0.0)
            total = jnp.sum(weights, axis=-1, keepdims=True)
            where = pl.ds(b, heads, stride=batch)
            acc_ref[where, :] = jnp.dot(weights.astype(BF16), vbuf[b], preferred_element_type=F32)
            mbuf[where, :] = jnp.broadcast_to(top, (heads, hd))
            lbuf[where, :] = jnp.broadcast_to(total, (heads, hd))
        store(0, g).start()
        store(1, g).start()
        return carry

    lax.fori_loop(0, groups, group, 0)
    lane = lax.broadcasted_iota(jnp.int32, (batch, hd), 1)
    packed = jnp.zeros((batch, hd), F32)
    for h in range(heads):
        packed = jnp.where(lane == h, mbuf[h * batch:(h + 1) * batch, :], packed)
        packed = jnp.where(lane == heads + h, lbuf[h * batch:(h + 1) * batch, :], packed)
    stat_ref[...] = packed
    for g in range(groups):
        store(0, g).wait()
        store(1, g).wait()


def output_kernel(
    acc, stat, hid, wo, out,
    hbuf, wob, obf, acc_p, acc_c, acc_y, o_own, o_land, st_p, st_c, st_y, part, land_a, land_b, tot,
    lsem, stsem, dsem, fsem,
):
    z = lax.axis_index("tp")
    me = lax.axis_index("sp")
    core = lax.rem(me, 2)
    mate = me + 1 - 2 * core
    across = lax.rem(me + 2, 4)
    diagonal = across + 1 - 2 * core
    partner = {"sp": mate}
    ynbr = {"sp": across}
    outer = jnp.logical_or(z == 0, z == 3)
    inner = jnp.logical_not(outer)
    z_in = jnp.where(z == 0, 1, jnp.where(z == 1, 2, jnp.where(z == 2, 1, 2)))
    z_out = jnp.where(z == 1, 0, 3)
    heads, batch, hd = acc.shape
    mine = heads // 2
    tile = wob.shape[2]
    rows_s = batch // NS
    rows_h = batch // HALVES
    mine_n = jnp.where(core == 0, FIRST, TILES - FIRST)
    mate_n = TILES - mine_n

    hcopy = pltpu.make_async_copy(hid, hbuf, lsem.at[MOST])

    def columns(quarter, t):
        first = (quarter // 2) * TILES + lax.rem(quarter, 2) * FIRST
        return pl.ds(pl.multiple_of((first + t) * tile, tile), tile)

    def wcopy(t):
        return pltpu.make_async_copy(wo.at[:, columns(me, t)], wob.at[t], lsem.at[t])

    def repeat(low, high, body):
        def step(i, carry):
            body(i)
            return carry

        lax.fori_loop(low, high, step, 0)

    barrier = pltpu.get_barrier_semaphore()
    pl.semaphore_signal(barrier, inc=1, device_id=partner, device_id_type=MESH)
    pl.semaphore_signal(barrier, inc=1, device_id=ynbr, device_id_type=MESH)

    @pl.when(z > 0)
    def _():
        pl.semaphore_signal(barrier, inc=1, device_id={"tp": z - 1}, device_id_type=MESH)

    @pl.when(z < 3)
    def _():
        pl.semaphore_signal(barrier, inc=1, device_id={"tp": z + 1}, device_id_type=MESH)

    repeat(0, mine_n, lambda t: wcopy(t).start())
    hcopy.start()

    @pl.when(outer)
    def _():
        pl.semaphore_wait(barrier, 3)

    @pl.when(inner)
    def _():
        pl.semaphore_wait(barrier, 4)

    def part_rows(s):
        return pl.ds(s * rows_s, rows_s)

    st_send = remote(stat, st_p, stsem.at[0], stsem.at[1], partner)
    st_send.start()
    p_send = []
    for s in range(NS):
        copy = remote(
            acc.at[pl.ds((1 - core) * mine, mine), part_rows(s)], acc_p.at[:, part_rows(s)],
            dsem.at[0, s], dsem.at[1, s], partner,
        )
        copy.start()
        p_send.append(copy)

    lane = lax.broadcasted_iota(jnp.int32, (batch, hd), 1)

    def merge(a, b):
        top = jnp.maximum(a, b)
        ea = jnp.exp(a - top)
        eb = jnp.exp(b - top)
        la = pltpu.roll(a, hd - heads, 1)
        lb = pltpu.roll(b, hd - heads, 1)
        return top, ea, eb, la * ea + lb * eb

    def own_heads(x):
        return jnp.where(core == 0, x, pltpu.roll(x, hd - mine, 1))

    st_send.wait_recv()
    top, ea, eb, total = merge(own_heads(stat[...]), own_heads(st_p[...]))
    st_c[...] = jnp.where(lane < heads, top, pltpu.roll(total, heads, 1))
    sty_send = remote(st_c, st_y, stsem.at[2], stsem.at[3], ynbr)
    sty_send.start()
    y_send = []
    for s in range(NS):
        p_send[s].wait_recv()
        sl = slice(s * rows_s, (s + 1) * rows_s)
        for h in range(mine):
            acc_c[h, sl, :] = acc[core * mine + h, sl, :] * ea[sl, h:h + 1] + acc_p[h, sl, :] * eb[sl, h:h + 1]
        copy = remote(acc_c.at[:, part_rows(s)], acc_y.at[:, part_rows(s)], dsem.at[2, s], dsem.at[3, s], ynbr)
        copy.start()
        y_send.append(copy)
    sty_send.wait_recv()
    _, ea, eb, total = merge(st_c[...], st_y[...])
    o_send = []

    def send_a(j):
        return remote(part.at[j], land_a.at[j], fsem.at[0, j], fsem.at[1, j], {"tp": z_in})

    def send_b(j):
        return remote(part.at[j], land_b.at[j], fsem.at[2, j], fsem.at[3, j], {"tp": z_in})

    def send_c(j):
        return remote(tot.at[me, j], tot.at[me, j], fsem.at[4, j], fsem.at[5, j], {"tp": z_out})

    def send_d(j):
        return remote(tot.at[me, j], tot.at[me, j], fsem.at[6, j], fsem.at[7, j], ynbr)

    def send_e(j):
        return remote(tot.at[me, j], tot.at[me, j], fsem.at[8, j], fsem.at[9, j], partner)

    def send_f(j):
        return remote(tot.at[across, j], tot.at[across, j], fsem.at[10, j], fsem.at[11, j], partner)

    for half in range(HALVES):
        chunks = range(half * NS // HALVES, (half + 1) * NS // HALVES)
        for s in chunks:
            y_send[s].wait_recv()
            sl = slice(s * rows_s, (s + 1) * rows_s)
            for h in range(mine):
                o = acc_c[h, sl, :] * ea[sl, h:h + 1] + acc_y[h, sl, :] * eb[sl, h:h + 1]
                o = round_bf16(o / total[sl, h:h + 1])
                o_own[h, sl, :] = o
                obf[sl, pl.ds(pl.multiple_of((core * mine + h) * hd, hd), hd)] = o.astype(BF16)
            copy = remote(o_own.at[:, part_rows(s)], o_land.at[:, part_rows(s)], dsem.at[4, s], dsem.at[5, s], partner)
            copy.start()
            o_send.append(copy)
        for s in chunks:
            o_send[s].wait_recv()
            sl = slice(s * rows_s, (s + 1) * rows_s)
            for h in range(mine):
                obf[sl, pl.ds(pl.multiple_of(((1 - core) * mine + h) * hd, hd), hd)] = o_land[h, sl, :].astype(BF16)

        def project(t, half=half):
            if half == 0:
                wcopy(t).wait()
            j = half * mine_n + t
            part[j] = jnp.dot(obf[half * rows_h:(half + 1) * rows_h, :], wob[t], preferred_element_type=F32)

            @pl.when(outer)
            def _():
                send_a(j).start()

        repeat(0, mine_n, project)
    hcopy.wait()

    def emit(quarter, count, j):
        half = j // count
        rows = pl.ds(pl.multiple_of(half * rows_h, rows_h), rows_h)
        where = columns(quarter, j - half * count)
        out[rows, where] = (hbuf[rows, where].astype(F32) + tot[quarter, j]).astype(BF16)

    def share(j):
        send_d(j).start()
        send_e(j).start()
        emit(me, mine_n, j)

    def collect_y(j):
        send_d(j).wait_recv()
        send_f(j).start()
        emit(across, mine_n, j)

    def collect_core(j):
        send_e(j).wait_recv()
        emit(mate, mate_n, j)

    def last(j):
        send_f(j).wait_recv()
        emit(diagonal, mate_n, j)

    mine_c = HALVES * mine_n
    mate_c = HALVES * mate_n

    def collect(k):
        @pl.when(k >= 0)
        def _():
            collect_y(k)

        @pl.when(jnp.logical_and(k >= 0, k < mate_c))
        def _():
            collect_core(k)

    @pl.when(outer)
    def _():
        def step(j):
            @pl.when(j < mine_c)
            def _():
                send_c(j).wait_recv()
                share(j)

            collect(j - LAG)

        repeat(0, mine_c + LAG, step)
        repeat(0, mine_c, lambda j: send_a(j).wait_send())

    @pl.when(inner)
    def _():
        def step(j):
            @pl.when(j < mine_c)
            def _():
                send_a(j).wait_recv()
                part[j] = part[j] + land_a[j]
                send_b(j).start()

            k = j - LAG

            @pl.when(jnp.logical_and(k >= 0, k < mine_c))
            def _():
                send_b(k).wait_recv()
                tot[me, k] = part[k] + land_b[k]
                send_c(k).start()
                share(k)

            collect(j - 2 * LAG)

        repeat(0, mine_c + 2 * LAG, step)

        def drain(j):
            send_b(j).wait_send()
            send_c(j).wait_send()

        repeat(0, mine_c, drain)

    repeat(mine_c, mate_c, collect_core)
    repeat(0, mate_c, last)
    st_send.wait_send()
    sty_send.wait_send()
    for s in range(NS):
        p_send[s].wait_send()
        y_send[s].wait_send()
        o_send[s].wait_send()

    def finish(j):
        send_d(j).wait_send()
        send_e(j).wait_send()
        send_f(j).wait_send()

    repeat(0, mine_c, finish)


def solution(mesh):
    vmem = pl.BlockSpec(memory_space=pltpu.VMEM)
    smem = pl.BlockSpec(memory_space=pltpu.SMEM)
    hbm = pl.BlockSpec(memory_space=pltpu.HBM)
    dma = pltpu.SemaphoreType.DMA

    def keep(x):
        return pltpu.with_memory_space_constraint(x, pltpu.VMEM)

    def stay(x):
        return pltpu.with_memory_space_constraint(x, pltpu.HBM)

    def params(mib, collective=None):
        if collective is None:
            return pltpu.CompilerParams(vmem_limit_bytes=mib * 2**20)
        return pltpu.CompilerParams(vmem_limit_bytes=mib * 2**20, collective_id=collective, has_side_effects=True)

    def local_step(hidden, norm_gain, w_query, w_key, w_value, w_out, k_cache, v_cache, positions):
        batch, seq_local, kv_local, hd = k_cache.shape
        d_model, q_cols = w_query.shape
        heads = q_cols // hd
        rows = seq_local * kv_local
        tiles = 2
        tcols = q_cols // 4 // tiles
        cache = (batch, rows, hd)
        acc_type = pltpu.VMEM((heads * batch, hd), F32)
        q, kv, k_in, v_in = pl.pallas_call(
            qkv_kernel,
            out_shape=(acc_type, pltpu.VMEM((2, 2, batch, hd), F32), pltpu.VMEM(cache, BF16), pltpu.VMEM(cache, BF16)),
            in_specs=[hbm] * 8,
            out_specs=(vmem,) * 4,
            scratch_shapes=[
                pltpu.SMEM((batch,), jnp.int32),
                pltpu.VMEM((batch, d_model), BF16),
                pltpu.VMEM((1, d_model), F32),
                pltpu.VMEM((batch, d_model), BF16),
                pltpu.VMEM((tiles, d_model, tcols), BF16),
                pltpu.VMEM((d_model, hd), BF16),
                pltpu.VMEM((4, 5, batch, hd), F32),
                dma((1,)),
                dma((3,)),
                dma((tiles,)),
                dma((2, 4)),
                dma((6, tiles + 1)),
            ],
            compiler_params=params(24, 0),
            name="qkv",
        )(
            stay(positions), stay(hidden), stay(norm_gain.reshape(1, d_model)), stay(w_query), stay(w_key), stay(w_value),
            stay(k_cache.reshape(cache)), stay(v_cache.reshape(cache)),
        )

        k_upd, v_upd, acc, stat, _, _ = pl.pallas_call(
            attention_kernel,
            out_shape=(
                jax.ShapeDtypeStruct(cache, BF16), jax.ShapeDtypeStruct(cache, BF16),
                acc_type, pltpu.VMEM((batch, hd), F32),
                pltpu.VMEM(cache, BF16), pltpu.VMEM(cache, BF16),
            ),
            in_specs=[smem, vmem, vmem, vmem, vmem],
            out_specs=(hbm, hbm, vmem, vmem, vmem, vmem),
            input_output_aliases={3: 4, 4: 5},
            scratch_shapes=[
                pltpu.VMEM((heads * batch, hd), F32),
                pltpu.VMEM((heads * batch, hd), F32),
                dma((2, batch // 8)),
            ],
            compiler_params=params(10),
            name="attention",
        )(positions, keep(q), keep(kv), keep(k_in), keep(v_in))

        mine = heads // 2
        ocols = d_model // 2 // TILES
        buf = pltpu.VMEM((mine, batch, hd), F32)
        st = pltpu.VMEM((batch, hd), F32)
        messages = HALVES * MOST
        block = (batch // HALVES, ocols)
        chunk = pltpu.VMEM((messages,) + block, F32)
        out = pl.pallas_call(
            output_kernel,
            out_shape=pltpu.VMEM((batch, d_model), BF16),
            in_specs=[vmem, vmem, hbm, hbm],
            out_specs=vmem,
            scratch_shapes=[
                pltpu.VMEM((batch, d_model), BF16),
                pltpu.VMEM((MOST, q_cols, ocols), BF16),
                pltpu.VMEM((batch, q_cols), BF16),
                buf, buf, buf, buf, buf, st, st, st, chunk, chunk, chunk,
                pltpu.VMEM((4, messages) + block, F32),
                dma((MOST + 1,)),
                dma((4,)),
                dma((6, NS)),
                dma((12, messages)),
            ],
            compiler_params=params(28, 1),
            name="output",
        )(keep(acc.reshape(heads, batch, hd)), keep(stat), stay(hidden), stay(w_out))
        return out, k_upd.reshape(k_cache.shape), v_upd.reshape(v_cache.shape)

    cache_spec = P("dp", "sp", "tp", None)
    specs_in = (P("dp", None), P(None), P(None, "tp"), P(None, "tp"), P(None, "tp"), P("tp", None), cache_spec, cache_spec, P("dp"))
    specs_out = (P("dp", None), cache_spec, cache_spec)
    return jax.shard_map(local_step, mesh=mesh, in_specs=specs_in, out_specs=specs_out, check_vma=False)
```

```python
import math

import jax
import jax.numpy as jnp
from jax import lax
from jax.experimental import pallas as pl
from jax.experimental.pallas import tpu as pltpu
from jax.sharding import PartitionSpec as P

ROPE_BASE = 1000000.0
EPS = 1e-5
NEG_BIG = float(jnp.finfo(jnp.float32).min)
MESH = pl.DeviceIdType.MESH
F32 = jnp.float32
BF16 = jnp.bfloat16
TILES = 16
FIRST = 8
MOST = max(FIRST, TILES - FIRST)
HALVES = 2
NS = 4
LAG = 4


def remote(src, dst, send, recv, device):
    return pltpu.make_async_remote_copy(
        src_ref=src, dst_ref=dst, send_sem=send, recv_sem=recv, device_id=device, device_id_type=MESH
    )


def round_bf16(x):
    return x.astype(BF16).astype(F32)


def qkv_kernel(
    pos, hid, gain, wq, wk, wv, kc, vc, q_out, kv_out, kc_out, vc_out,
    pos_s, hbuf, gbuf, rbuf, wqb, wkvb, pieces, psem, hsem, wsem, csem, xsem,
):
    me = lax.axis_index("sp")
    core = lax.rem(me, 2)
    mate = me + 1 - 2 * core
    across = lax.rem(me + 2, 4)
    partner = {"sp": mate}
    ynbr = {"sp": across}
    batch, d_model = hid.shape
    tiles, _, cols = wqb.shape
    quarter = tiles * cols
    hcopy = pltpu.make_async_copy(hid, hbuf, hsem.at[0])
    gcopy = pltpu.make_async_copy(gain, gbuf, hsem.at[1])
    pcopy = pltpu.make_async_copy(pos, pos_s, psem.at[0])
    hcopy.start()
    gcopy.start()
    pcopy.start()
    head_cols = pl.ds(pl.multiple_of(core * 128, 128), 128)
    keys = me < 2

    @pl.when(keys)
    def _():
        pltpu.make_async_copy(wk.at[:, head_cols], wkvb, hsem.at[2]).start()

    @pl.when(jnp.logical_not(keys))
    def _():
        pltpu.make_async_copy(wv.at[:, head_cols], wkvb, hsem.at[2]).start()

    def wcopy(t):
        return pltpu.make_async_copy(
            wq.at[:, pl.ds(pl.multiple_of(me * quarter + t * cols, cols), cols)], wqb.at[t], wsem.at[t]
        )

    for t in range(tiles):
        wcopy(t).start()
    barrier = pltpu.get_barrier_semaphore()
    pl.semaphore_signal(barrier, inc=1, device_id=partner, device_id_type=MESH)
    pl.semaphore_signal(barrier, inc=1, device_id=ynbr, device_id_type=MESH)

    def cache_copy(which, g):
        src, dst = ((kc, kc_out), (vc, vc_out))[which]
        rows = pl.ds(g * (batch // 4), batch // 4)
        return pltpu.make_async_copy(src.at[rows], dst.at[rows], csem.at[which, g])

    pcopy.wait()
    lane = lax.broadcasted_iota(jnp.int32, (batch, 128), 1)
    row = lax.broadcasted_iota(jnp.int32, (batch, 128), 0)
    position = jnp.zeros((batch, 128), jnp.int32)
    for b in range(batch):
        position = jnp.where(row == b, pos_s[b], position)
    index = jnp.where(lane < 64, lane, lane - 64).astype(F32)
    angle = position.astype(F32) * jnp.exp(index * (-2.0 / 128 * math.log(ROPE_BASE)))
    cosf = jnp.cos(angle)
    sinf = jnp.where(lane < 64, -1.0, 1.0) * jnp.sin(angle)

    hcopy.wait()
    gcopy.wait()

    def norm_rows(i, carry):
        rows = pl.ds(pl.multiple_of(i * 16, 16), 16)
        x = hbuf[rows, :].astype(F32)
        scale = lax.rsqrt(jnp.sum(x * x, axis=-1, keepdims=True) * (1.0 / d_model) + EPS)
        rbuf[rows, :] = (x * scale * gbuf[...]).astype(BF16)
        return carry

    lax.fori_loop(0, batch // 16, norm_rows, 0)

    def rotate(x):
        return x * cosf + pltpu.roll(x, 64, 1) * sinf

    def span(p):
        return pl.ds(4, 1) if p == 0 else pl.ds(2 * (p - 1), 2)

    def exchange(kind, owner, p, device):
        part = pieces.at[owner, span(p)]
        return remote(part, part, xsem.at[2 * kind, p], xsem.at[2 * kind + 1, p], device)

    def publish(p):
        exchange(0, me, p, ynbr).start()
        exchange(1, me, p, partner).start()

    pltpu.make_async_copy(wk.at[:, head_cols], wkvb, hsem.at[2]).wait()
    kv = jnp.dot(rbuf[...], wkvb[...], preferred_element_type=F32)
    pieces[me, 4] = round_bf16(jnp.where(keys, rotate(kv), kv))
    pl.semaphore_wait(barrier, 2)
    publish(0)
    for t in range(tiles):
        wcopy(t).wait()
        if t == tiles - 1:
            for g in range(4):
                cache_copy(0, g).start()
                cache_copy(1, g).start()
        q = jnp.dot(rbuf[...], wqb[t], preferred_element_type=F32)
        for h in range(2):
            pieces[me, 2 * t + h] = round_bf16(rotate(q[:, h * 128:(h + 1) * 128]))
        publish(t + 1)
    for p in range(tiles + 1):
        exchange(0, me, p, ynbr).wait_recv()
        exchange(2, across, p, partner).start()
    for p in range(tiles + 1):
        exchange(1, me, p, partner).wait_recv()
        exchange(2, across, p, partner).wait_recv()
    for owner in range(4):
        for h in range(4):
            q_out[pl.ds((owner * 4 + h) * batch, batch), :] = pieces[owner, h]
        kv_out[owner % 2, owner // 2] = pieces[owner, 4]
    for p in range(tiles + 1):
        exchange(0, me, p, ynbr).wait_send()
        exchange(1, me, p, partner).wait_send()
        exchange(2, across, p, partner).wait_send()
    for g in range(4):
        cache_copy(0, g).wait()
        cache_copy(1, g).wait()


def attention_kernel(
    pos, q_ref, kv_ref, kc, vc, ko, vo, acc_ref, stat_ref, kbuf, vbuf, mbuf, lbuf, osem,
):
    batch, rows, hd = kbuf.shape
    heads = acc_ref.shape[0] // batch
    groups = batch // 8
    me = lax.axis_index("sp")
    first = me * (rows // 2)

    def seqs(g):
        return pl.ds(pl.multiple_of(g * 8, 8), 8)

    def store(which, g):
        src, dst = ((kbuf, ko), (vbuf, vo))[which]
        return pltpu.make_async_copy(src.at[seqs(g)], dst.at[seqs(g)], osem.at[which, g])

    row_iota = lax.broadcasted_iota(jnp.int32, (16, hd), 0)
    col_iota = lax.broadcasted_iota(jnp.int32, (heads, rows), 1)
    head_iota = lax.broadcasted_iota(jnp.int32, (heads, rows), 0)
    col_head = lax.rem(col_iota, 2)
    col_pos = jnp.where(col_head == head_iota // (heads // 2), first + col_iota // 2, 1 << 20)

    def group(g, carry):
        for i in range(8):
            b = g * 8 + i
            slot = 2 * (pos[b] - first)
            inside = jnp.logical_and(slot >= 0, slot < rows)
            base = pl.multiple_of((jnp.clip(slot, 0, rows - 1) // 16) * 16, 16)
            target = jnp.where(inside, slot - base, -100)
            for buf, which in ((kbuf, 0), (vbuf, 1)):
                old = buf[b, pl.ds(base, 16), :].astype(F32)
                new0 = kv_ref[0, which, pl.ds(b, 1), :]
                new1 = kv_ref[1, which, pl.ds(b, 1), :]
                new = jnp.where(row_iota == target, new0, jnp.where(row_iota == target + 1, new1, old))
                buf[b, pl.ds(base, 16), :] = new.astype(BF16)
        scores = []
        for i in range(8):
            b = g * 8 + i
            q = q_ref[pl.ds(b, heads, stride=batch), :].astype(BF16)
            s = lax.dot_general(q, kbuf[b], (((1,), (1,)), ((), ())), preferred_element_type=F32) * (hd ** -0.5)
            scores.append(jnp.where(col_pos <= pos[b], s, NEG_BIG))
        for i in range(8):
            b = g * 8 + i
            s = scores[i]
            top = jnp.max(s, axis=-1, keepdims=True)
            weights = jnp.where(col_pos <= pos[b], jnp.exp(s - top), 0.0)
            total = jnp.sum(weights, axis=-1, keepdims=True)
            where = pl.ds(b, heads, stride=batch)
            acc_ref[where, :] = jnp.dot(weights.astype(BF16), vbuf[b], preferred_element_type=F32)
            mbuf[where, :] = jnp.broadcast_to(top, (heads, hd))
            lbuf[where, :] = jnp.broadcast_to(total, (heads, hd))
        store(0, g).start()
        store(1, g).start()
        return carry

    lax.fori_loop(0, groups, group, 0)
    lane = lax.broadcasted_iota(jnp.int32, (batch, hd), 1)
    packed = jnp.zeros((batch, hd), F32)
    for h in range(heads):
        packed = jnp.where(lane == h, mbuf[h * batch:(h + 1) * batch, :], packed)
        packed = jnp.where(lane == heads + h, lbuf[h * batch:(h + 1) * batch, :], packed)
    stat_ref[...] = packed
    for g in range(groups):
        store(0, g).wait()
        store(1, g).wait()


def output_kernel(
    acc, stat, hid, wo, out,
    hbuf, wob, obf, acc_p, acc_c, acc_y, o_own, o_land, st_p, st_c, st_y, part, land_a, land_b, tot,
    lsem, stsem, dsem, fsem,
):
    z = lax.axis_index("tp")
    me = lax.axis_index("sp")
    core = lax.rem(me, 2)
    mate = me + 1 - 2 * core
    across = lax.rem(me + 2, 4)
    diagonal = across + 1 - 2 * core
    partner = {"sp": mate}
    ynbr = {"sp": across}
    outer = jnp.logical_or(z == 0, z == 3)
    inner = jnp.logical_not(outer)
    z_in = jnp.where(z == 0, 1, jnp.where(z == 1, 2, jnp.where(z == 2, 1, 2)))
    z_out = jnp.where(z == 1, 0, 3)
    heads, batch, hd = acc.shape
    mine = heads // 2
    tile = wob.shape[2]
    rows_s = batch // NS
    rows_h = batch // HALVES
    mine_n = jnp.where(core == 0, FIRST, TILES - FIRST)
    mate_n = TILES - mine_n

    hcopy = pltpu.make_async_copy(hid, hbuf, lsem.at[MOST])

    def columns(quarter, t):
        first = (quarter // 2) * TILES + lax.rem(quarter, 2) * FIRST
        return pl.ds(pl.multiple_of((first + t) * tile, tile), tile)

    def wcopy(t):
        return pltpu.make_async_copy(wo.at[:, columns(me, t)], wob.at[t], lsem.at[t])

    def repeat(low, high, body):
        def step(i, carry):
            body(i)
            return carry

        lax.fori_loop(low, high, step, 0)

    barrier = pltpu.get_barrier_semaphore()
    pl.semaphore_signal(barrier, inc=1, device_id=partner, device_id_type=MESH)
    pl.semaphore_signal(barrier, inc=1, device_id=ynbr, device_id_type=MESH)

    @pl.when(z > 0)
    def _():
        pl.semaphore_signal(barrier, inc=1, device_id={"tp": z - 1}, device_id_type=MESH)

    @pl.when(z < 3)
    def _():
        pl.semaphore_signal(barrier, inc=1, device_id={"tp": z + 1}, device_id_type=MESH)

    repeat(0, mine_n, lambda t: wcopy(t).start())
    hcopy.start()

    @pl.when(outer)
    def _():
        pl.semaphore_wait(barrier, 3)

    @pl.when(inner)
    def _():
        pl.semaphore_wait(barrier, 4)

    def part_rows(s):
        return pl.ds(s * rows_s, rows_s)

    st_send = remote(stat, st_p, stsem.at[0], stsem.at[1], partner)
    st_send.start()
    p_send = []
    for s in range(NS):
        copy = remote(
            acc.at[pl.ds((1 - core) * mine, mine), part_rows(s)], acc_p.at[:, part_rows(s)],
            dsem.at[0, s], dsem.at[1, s], partner,
        )
        copy.start()
        p_send.append(copy)

    lane = lax.broadcasted_iota(jnp.int32, (batch, hd), 1)

    def merge(a, b):
        top = jnp.maximum(a, b)
        ea = jnp.exp(a - top)
        eb = jnp.exp(b - top)
        la = pltpu.roll(a, hd - heads, 1)
        lb = pltpu.roll(b, hd - heads, 1)
        return top, ea, eb, la * ea + lb * eb

    def own_heads(x):
        return jnp.where(core == 0, x, pltpu.roll(x, hd - mine, 1))

    st_send.wait_recv()
    top, ea, eb, total = merge(own_heads(stat[...]), own_heads(st_p[...]))
    st_c[...] = jnp.where(lane < heads, top, pltpu.roll(total, heads, 1))
    sty_send = remote(st_c, st_y, stsem.at[2], stsem.at[3], ynbr)
    sty_send.start()
    y_send = []
    for s in range(NS):
        p_send[s].wait_recv()
        sl = slice(s * rows_s, (s + 1) * rows_s)
        for h in range(mine):
            acc_c[h, sl, :] = acc[core * mine + h, sl, :] * ea[sl, h:h + 1] + acc_p[h, sl, :] * eb[sl, h:h + 1]
        copy = remote(acc_c.at[:, part_rows(s)], acc_y.at[:, part_rows(s)], dsem.at[2, s], dsem.at[3, s], ynbr)
        copy.start()
        y_send.append(copy)
    sty_send.wait_recv()
    _, ea, eb, total = merge(st_c[...], st_y[...])
    o_send = []

    def send_a(j):
        return remote(part.at[j], land_a.at[j], fsem.at[0, j], fsem.at[1, j], {"tp": z_in})

    def send_b(j):
        return remote(part.at[j], land_b.at[j], fsem.at[2, j], fsem.at[3, j], {"tp": z_in})

    def send_c(j):
        return remote(tot.at[me, j], tot.at[me, j], fsem.at[4, j], fsem.at[5, j], {"tp": z_out})

    def send_d(j):
        return remote(tot.at[me, j], tot.at[me, j], fsem.at[6, j], fsem.at[7, j], ynbr)

    def send_e(j):
        return remote(tot.at[me, j], tot.at[me, j], fsem.at[8, j], fsem.at[9, j], partner)

    def send_f(j):
        return remote(tot.at[across, j], tot.at[across, j], fsem.at[10, j], fsem.at[11, j], partner)

    for half in range(HALVES):
        chunks = range(half * NS // HALVES, (half + 1) * NS // HALVES)
        for s in chunks:
            y_send[s].wait_recv()
            sl = slice(s * rows_s, (s + 1) * rows_s)
            for h in range(mine):
                o = acc_c[h, sl, :] * ea[sl, h:h + 1] + acc_y[h, sl, :] * eb[sl, h:h + 1]
                o = round_bf16(o / total[sl, h:h + 1])
                o_own[h, sl, :] = o
                obf[sl, pl.ds(pl.multiple_of((core * mine + h) * hd, hd), hd)] = o.astype(BF16)
            copy = remote(o_own.at[:, part_rows(s)], o_land.at[:, part_rows(s)], dsem.at[4, s], dsem.at[5, s], partner)
            copy.start()
            o_send.append(copy)
        for s in chunks:
            o_send[s].wait_recv()
            sl = slice(s * rows_s, (s + 1) * rows_s)
            for h in range(mine):
                obf[sl, pl.ds(pl.multiple_of(((1 - core) * mine + h) * hd, hd), hd)] = o_land[h, sl, :].astype(BF16)

        def project(t, half=half):
            if half == 0:
                wcopy(t).wait()
            j = half * mine_n + t
            part[j] = jnp.dot(obf[half * rows_h:(half + 1) * rows_h, :], wob[t], preferred_element_type=F32)

            @pl.when(outer)
            def _():
                send_a(j).start()

        repeat(0, mine_n, project)
    hcopy.wait()

    def emit(quarter, count, j):
        half = j // count
        rows = pl.ds(pl.multiple_of(half * rows_h, rows_h), rows_h)
        where = columns(quarter, j - half * count)
        out[rows, where] = (hbuf[rows, where].astype(F32) + tot[quarter, j]).astype(BF16)

    def share(j):
        send_d(j).start()
        send_e(j).start()
        emit(me, mine_n, j)

    def collect_y(j):
        send_d(j).wait_recv()
        send_f(j).start()
        emit(across, mine_n, j)

    def collect_core(j):
        send_e(j).wait_recv()
        emit(mate, mate_n, j)

    def last(j):
        send_f(j).wait_recv()
        emit(diagonal, mate_n, j)

    mine_c = HALVES * mine_n
    mate_c = HALVES * mate_n

    def collect(k):
        @pl.when(k >= 0)
        def _():
            collect_y(k)

        @pl.when(jnp.logical_and(k >= 0, k < mate_c))
        def _():
            collect_core(k)

    @pl.when(outer)
    def _():
        def step(j):
            @pl.when(j < mine_c)
            def _():
                send_c(j).wait_recv()
                share(j)

            collect(j - LAG)

        repeat(0, mine_c + LAG, step)
        repeat(0, mine_c, lambda j: send_a(j).wait_send())

    @pl.when(inner)
    def _():
        def step(j):
            @pl.when(j < mine_c)
            def _():
                send_a(j).wait_recv()
                part[j] = part[j] + land_a[j]
                send_b(j).start()

            k = j - LAG

            @pl.when(jnp.logical_and(k >= 0, k < mine_c))
            def _():
                send_b(k).wait_recv()
                tot[me, k] = part[k] + land_b[k]
                send_c(k).start()
                share(k)

            collect(j - 2 * LAG)

        repeat(0, mine_c + 2 * LAG, step)

        def drain(j):
            send_b(j).wait_send()
            send_c(j).wait_send()

        repeat(0, mine_c, drain)

    repeat(mine_c, mate_c, collect_core)
    repeat(0, mate_c, last)
    st_send.wait_send()
    sty_send.wait_send()
    for s in range(NS):
        p_send[s].wait_send()
        y_send[s].wait_send()
        o_send[s].wait_send()

    def finish(j):
        send_d(j).wait_send()
        send_e(j).wait_send()
        send_f(j).wait_send()

    repeat(0, mine_c, finish)


def solution(mesh):
    vmem = pl.BlockSpec(memory_space=pltpu.VMEM)
    smem = pl.BlockSpec(memory_space=pltpu.SMEM)
    hbm = pl.BlockSpec(memory_space=pltpu.HBM)
    dma = pltpu.SemaphoreType.DMA

    def keep(x):
        return pltpu.with_memory_space_constraint(x, pltpu.VMEM)

    def stay(x):
        return pltpu.with_memory_space_constraint(x, pltpu.HBM)

    def params(mib, collective=None):
        if collective is None:
            return pltpu.CompilerParams(vmem_limit_bytes=mib * 2**20)
        return pltpu.CompilerParams(vmem_limit_bytes=mib * 2**20, collective_id=collective, has_side_effects=True)

    def local_step(hidden, norm_gain, w_query, w_key, w_value, w_out, k_cache, v_cache, positions):
        batch, seq_local, kv_local, hd = k_cache.shape
        d_model, q_cols = w_query.shape
        heads = q_cols // hd
        rows = seq_local * kv_local
        tiles = 2
        tcols = q_cols // 4 // tiles
        cache = (batch, rows, hd)
        acc_type = pltpu.VMEM((heads * batch, hd), F32)
        q, kv, k_in, v_in = pl.pallas_call(
            qkv_kernel,
            out_shape=(acc_type, pltpu.VMEM((2, 2, batch, hd), F32), pltpu.VMEM(cache, BF16), pltpu.VMEM(cache, BF16)),
            in_specs=[hbm] * 8,
            out_specs=(vmem,) * 4,
            scratch_shapes=[
                pltpu.SMEM((batch,), jnp.int32),
                pltpu.VMEM((batch, d_model), BF16),
                pltpu.VMEM((1, d_model), F32),
                pltpu.VMEM((batch, d_model), BF16),
                pltpu.VMEM((tiles, d_model, tcols), BF16),
                pltpu.VMEM((d_model, hd), BF16),
                pltpu.VMEM((4, 5, batch, hd), F32),
                dma((1,)),
                dma((3,)),
                dma((tiles,)),
                dma((2, 4)),
                dma((6, tiles + 1)),
            ],
            compiler_params=params(24, 0),
            name="qkv",
        )(
            stay(positions), stay(hidden), stay(norm_gain.reshape(1, d_model)), stay(w_query), stay(w_key), stay(w_value),
            stay(k_cache.reshape(cache)), stay(v_cache.reshape(cache)),
        )

        k_upd, v_upd, acc, stat, _, _ = pl.pallas_call(
            attention_kernel,
            out_shape=(
                jax.ShapeDtypeStruct(cache, BF16), jax.ShapeDtypeStruct(cache, BF16),
                acc_type, pltpu.VMEM((batch, hd), F32),
                pltpu.VMEM(cache, BF16), pltpu.VMEM(cache, BF16),
            ),
            in_specs=[smem, vmem, vmem, vmem, vmem],
            out_specs=(hbm, hbm, vmem, vmem, vmem, vmem),
            input_output_aliases={3: 4, 4: 5},
            scratch_shapes=[
                pltpu.VMEM((heads * batch, hd), F32),
                pltpu.VMEM((heads * batch, hd), F32),
                dma((2, batch // 8)),
            ],
            compiler_params=params(10),
            name="attention",
        )(positions, keep(q), keep(kv), keep(k_in), keep(v_in))

        mine = heads // 2
        ocols = d_model // 2 // TILES
        buf = pltpu.VMEM((mine, batch, hd), F32)
        st = pltpu.VMEM((batch, hd), F32)
        messages = HALVES * MOST
        block = (batch // HALVES, ocols)
        chunk = pltpu.VMEM((messages,) + block, F32)
        out = pl.pallas_call(
            output_kernel,
            out_shape=pltpu.VMEM((batch, d_model), BF16),
            in_specs=[vmem, vmem, hbm, hbm],
            out_specs=vmem,
            scratch_shapes=[
                pltpu.VMEM((batch, d_model), BF16),
                pltpu.VMEM((MOST, q_cols, ocols), BF16),
                pltpu.VMEM((batch, q_cols), BF16),
                buf, buf, buf, buf, buf, st, st, st, chunk, chunk, chunk,
                pltpu.VMEM((4, messages) + block, F32),
                dma((MOST + 1,)),
                dma((4,)),
                dma((6, NS)),
                dma((12, messages)),
            ],
            compiler_params=params(28, 1),
            name="output",
        )(keep(acc.reshape(heads, batch, hd)), keep(stat), stay(hidden), stay(w_out))
        return out, k_upd.reshape(k_cache.shape), v_upd.reshape(v_cache.shape)

    cache_spec = P("dp", "sp", "tp", None)
    specs_in = (P("dp", None), P(None), P(None, "tp"), P(None, "tp"), P(None, "tp"), P("tp", None), cache_spec, cache_spec, P("dp"))
    specs_out = (P("dp", None), cache_spec, cache_spec)
    return jax.shard_map(local_step, mesh=mesh, in_specs=specs_in, out_specs=specs_out, check_vma=False)
```

```python
import math

import jax
import jax.numpy as jnp
from jax import lax
from jax.experimental import pallas as pl
from jax.experimental.pallas import tpu as pltpu
from jax.sharding import PartitionSpec as P

ROPE_BASE = 1000000.0
EPS = 1e-5
NEG_BIG = float(jnp.finfo(jnp.float32).min)
MESH = pl.DeviceIdType.MESH
F32 = jnp.float32
BF16 = jnp.bfloat16
TILES = 16
FIRST = 8
MOST = max(FIRST, TILES - FIRST)
HALVES = 2
NS = 4
LAG = 6


def remote(src, dst, send, recv, device):
    return pltpu.make_async_remote_copy(
        src_ref=src, dst_ref=dst, send_sem=send, recv_sem=recv, device_id=device, device_id_type=MESH
    )


def round_bf16(x):
    return x.astype(BF16).astype(F32)


def qkv_kernel(
    pos, hid, gain, wq, wk, wv, kc, vc, q_out, kv_out, kc_out, vc_out,
    pos_s, hbuf, gbuf, rbuf, wqb, wkvb, pieces, psem, hsem, wsem, csem, xsem,
):
    me = lax.axis_index("sp")
    core = lax.rem(me, 2)
    mate = me + 1 - 2 * core
    across = lax.rem(me + 2, 4)
    partner = {"sp": mate}
    ynbr = {"sp": across}
    batch, d_model = hid.shape
    tiles, _, cols = wqb.shape
    quarter = tiles * cols
    hcopy = pltpu.make_async_copy(hid, hbuf, hsem.at[0])
    gcopy = pltpu.make_async_copy(gain, gbuf, hsem.at[1])
    pcopy = pltpu.make_async_copy(pos, pos_s, psem.at[0])
    hcopy.start()
    gcopy.start()
    pcopy.start()
    head_cols = pl.ds(pl.multiple_of(core * 128, 128), 128)
    keys = me < 2

    @pl.when(keys)
    def _():
        pltpu.make_async_copy(wk.at[:, head_cols], wkvb, hsem.at[2]).start()

    @pl.when(jnp.logical_not(keys))
    def _():
        pltpu.make_async_copy(wv.at[:, head_cols], wkvb, hsem.at[2]).start()

    def wcopy(t):
        return pltpu.make_async_copy(
            wq.at[:, pl.ds(pl.multiple_of(me * quarter + t * cols, cols), cols)], wqb.at[t], wsem.at[t]
        )

    for t in range(tiles):
        wcopy(t).start()
    barrier = pltpu.get_barrier_semaphore()
    pl.semaphore_signal(barrier, inc=1, device_id=partner, device_id_type=MESH)
    pl.semaphore_signal(barrier, inc=1, device_id=ynbr, device_id_type=MESH)

    def cache_copy(which, g):
        src, dst = ((kc, kc_out), (vc, vc_out))[which]
        rows = pl.ds(g * (batch // 4), batch // 4)
        return pltpu.make_async_copy(src.at[rows], dst.at[rows], csem.at[which, g])

    pcopy.wait()
    lane = lax.broadcasted_iota(jnp.int32, (batch, 128), 1)
    row = lax.broadcasted_iota(jnp.int32, (batch, 128), 0)
    position = jnp.zeros((batch, 128), jnp.int32)
    for b in range(batch):
        position = jnp.where(row == b, pos_s[b], position)
    index = jnp.where(lane < 64, lane, lane - 64).astype(F32)
    angle = position.astype(F32) * jnp.exp(index * (-2.0 / 128 * math.log(ROPE_BASE)))
    cosf = jnp.cos(angle)
    sinf = jnp.where(lane < 64, -1.0, 1.0) * jnp.sin(angle)

    hcopy.wait()
    gcopy.wait()

    def norm_rows(i, carry):
        rows = pl.ds(pl.multiple_of(i * 16, 16), 16)
        x = hbuf[rows, :].astype(F32)
        scale = lax.rsqrt(jnp.sum(x * x, axis=-1, keepdims=True) * (1.0 / d_model) + EPS)
        rbuf[rows, :] = (x * scale * gbuf[...]).astype(BF16)
        return carry

    lax.fori_loop(0, batch // 16, norm_rows, 0)

    def rotate(x):
        return x * cosf + pltpu.roll(x, 64, 1) * sinf

    def span(p):
        return pl.ds(4, 1) if p == 0 else pl.ds(2 * (p - 1), 2)

    def exchange(kind, owner, p, device):
        part = pieces.at[owner, span(p)]
        return remote(part, part, xsem.at[2 * kind, p], xsem.at[2 * kind + 1, p], device)

    def publish(p):
        exchange(0, me, p, ynbr).start()
        exchange(1, me, p, partner).start()

    pltpu.make_async_copy(wk.at[:, head_cols], wkvb, hsem.at[2]).wait()
    kv = jnp.dot(rbuf[...], wkvb[...], preferred_element_type=F32)
    pieces[me, 4] = round_bf16(jnp.where(keys, rotate(kv), kv))
    pl.semaphore_wait(barrier, 2)
    publish(0)
    for t in range(tiles):
        wcopy(t).wait()
        if t == tiles - 1:
            for g in range(4):
                cache_copy(0, g).start()
                cache_copy(1, g).start()
        q = jnp.dot(rbuf[...], wqb[t], preferred_element_type=F32)
        for h in range(2):
            pieces[me, 2 * t + h] = round_bf16(rotate(q[:, h * 128:(h + 1) * 128]))
        publish(t + 1)
    for p in range(tiles + 1):
        exchange(0, me, p, ynbr).wait_recv()
        exchange(2, across, p, partner).start()
    for p in range(tiles + 1):
        exchange(1, me, p, partner).wait_recv()
        exchange(2, across, p, partner).wait_recv()
    for owner in range(4):
        for h in range(4):
            q_out[pl.ds((owner * 4 + h) * batch, batch), :] = pieces[owner, h]
        kv_out[owner % 2, owner // 2] = pieces[owner, 4]
    for p in range(tiles + 1):
        exchange(0, me, p, ynbr).wait_send()
        exchange(1, me, p, partner).wait_send()
        exchange(2, across, p, partner).wait_send()
    for g in range(4):
        cache_copy(0, g).wait()
        cache_copy(1, g).wait()


def attention_kernel(
    pos, q_ref, kv_ref, kc, vc, ko, vo, acc_ref, stat_ref, kbuf, vbuf, mbuf, lbuf, osem,
):
    batch, rows, hd = kbuf.shape
    heads = acc_ref.shape[0] // batch
    groups = batch // 8
    me = lax.axis_index("sp")
    first = me * (rows // 2)

    def seqs(g):
        return pl.ds(pl.multiple_of(g * 8, 8), 8)

    def store(which, g):
        src, dst = ((kbuf, ko), (vbuf, vo))[which]
        return pltpu.make_async_copy(src.at[seqs(g)], dst.at[seqs(g)], osem.at[which, g])

    row_iota = lax.broadcasted_iota(jnp.int32, (16, hd), 0)
    col_iota = lax.broadcasted_iota(jnp.int32, (heads, rows), 1)
    head_iota = lax.broadcasted_iota(jnp.int32, (heads, rows), 0)
    col_head = lax.rem(col_iota, 2)
    col_pos = jnp.where(col_head == head_iota // (heads // 2), first + col_iota // 2, 1 << 20)

    def group(g, carry):
        for i in range(8):
            b = g * 8 + i
            slot = 2 * (pos[b] - first)
            inside = jnp.logical_and(slot >= 0, slot < rows)
            base = pl.multiple_of((jnp.clip(slot, 0, rows - 1) // 16) * 16, 16)
            target = jnp.where(inside, slot - base, -100)
            for buf, which in ((kbuf, 0), (vbuf, 1)):
                old = buf[b, pl.ds(base, 16), :].astype(F32)
                new0 = kv_ref[0, which, pl.ds(b, 1), :]
                new1 = kv_ref[1, which, pl.ds(b, 1), :]
                new = jnp.where(row_iota == target, new0, jnp.where(row_iota == target + 1, new1, old))
                buf[b, pl.ds(base, 16), :] = new.astype(BF16)
        scores = []
        for i in range(8):
            b = g * 8 + i
            q = q_ref[pl.ds(b, heads, stride=batch), :].astype(BF16)
            s = lax.dot_general(q, kbuf[b], (((1,), (1,)), ((), ())), preferred_element_type=F32) * (hd ** -0.5)
            scores.append(jnp.where(col_pos <= pos[b], s, NEG_BIG))
        for i in range(8):
            b = g * 8 + i
            s = scores[i]
            top = jnp.max(s, axis=-1, keepdims=True)
            weights = jnp.where(col_pos <= pos[b], jnp.exp(s - top), 0.0)
            total = jnp.sum(weights, axis=-1, keepdims=True)
            where = pl.ds(b, heads, stride=batch)
            acc_ref[where, :] = jnp.dot(weights.astype(BF16), vbuf[b], preferred_element_type=F32)
            mbuf[where, :] = jnp.broadcast_to(top, (heads, hd))
            lbuf[where, :] = jnp.broadcast_to(total, (heads, hd))
        store(0, g).start()
        store(1, g).start()
        return carry

    lax.fori_loop(0, groups, group, 0)
    lane = lax.broadcasted_iota(jnp.int32, (batch, hd), 1)
    packed = jnp.zeros((batch, hd), F32)
    for h in range(heads):
        packed = jnp.where(lane == h, mbuf[h * batch:(h + 1) * batch, :], packed)
        packed = jnp.where(lane == heads + h, lbuf[h * batch:(h + 1) * batch, :], packed)
    stat_ref[...] = packed
    for g in range(groups):
        store(0, g).wait()
        store(1, g).wait()


def output_kernel(
    acc, stat, hid, wo, out,
    hbuf, wob, obf, acc_p, acc_c, acc_y, o_own, o_land, st_p, st_c, st_y, part, land_a, land_b, tot,
    lsem, stsem, dsem, fsem,
):
    z = lax.axis_index("tp")
    me = lax.axis_index("sp")
    core = lax.rem(me, 2)
    mate = me + 1 - 2 * core
    across = lax.rem(me + 2, 4)
    diagonal = across + 1 - 2 * core
    partner = {"sp": mate}
    ynbr = {"sp": across}
    outer = jnp.logical_or(z == 0, z == 3)
    inner = jnp.logical_not(outer)
    z_in = jnp.where(z == 0, 1, jnp.where(z == 1, 2, jnp.where(z == 2, 1, 2)))
    z_out = jnp.where(z == 1, 0, 3)
    heads, batch, hd = acc.shape
    mine = heads // 2
    tile = wob.shape[2]
    rows_s = batch // NS
    rows_h = batch // HALVES
    mine_n = jnp.where(core == 0, FIRST, TILES - FIRST)
    mate_n = TILES - mine_n

    hcopy = pltpu.make_async_copy(hid, hbuf, lsem.at[MOST])

    def columns(quarter, t):
        first = (quarter // 2) * TILES + lax.rem(quarter, 2) * FIRST
        return pl.ds(pl.multiple_of((first + t) * tile, tile), tile)

    def wcopy(t):
        return pltpu.make_async_copy(wo.at[:, columns(me, t)], wob.at[t], lsem.at[t])

    def repeat(low, high, body):
        def step(i, carry):
            body(i)
            return carry

        lax.fori_loop(low, high, step, 0)

    barrier = pltpu.get_barrier_semaphore()
    pl.semaphore_signal(barrier, inc=1, device_id=partner, device_id_type=MESH)
    pl.semaphore_signal(barrier, inc=1, device_id=ynbr, device_id_type=MESH)

    @pl.when(z > 0)
    def _():
        pl.semaphore_signal(barrier, inc=1, device_id={"tp": z - 1}, device_id_type=MESH)

    @pl.when(z < 3)
    def _():
        pl.semaphore_signal(barrier, inc=1, device_id={"tp": z + 1}, device_id_type=MESH)

    repeat(0, mine_n, lambda t: wcopy(t).start())
    hcopy.start()

    @pl.when(outer)
    def _():
        pl.semaphore_wait(barrier, 3)

    @pl.when(inner)
    def _():
        pl.semaphore_wait(barrier, 4)

    def part_rows(s):
        return pl.ds(s * rows_s, rows_s)

    st_send = remote(stat, st_p, stsem.at[0], stsem.at[1], partner)
    st_send.start()
    p_send = []
    for s in range(NS):
        copy = remote(
            acc.at[pl.ds((1 - core) * mine, mine), part_rows(s)], acc_p.at[:, part_rows(s)],
            dsem.at[0, s], dsem.at[1, s], partner,
        )
        copy.start()
        p_send.append(copy)

    lane = lax.broadcasted_iota(jnp.int32, (batch, hd), 1)

    def merge(a, b):
        top = jnp.maximum(a, b)
        ea = jnp.exp(a - top)
        eb = jnp.exp(b - top)
        la = pltpu.roll(a, hd - heads, 1)
        lb = pltpu.roll(b, hd - heads, 1)
        return top, ea, eb, la * ea + lb * eb

    def own_heads(x):
        return jnp.where(core == 0, x, pltpu.roll(x, hd - mine, 1))

    st_send.wait_recv()
    top, ea, eb, total = merge(own_heads(stat[...]), own_heads(st_p[...]))
    st_c[...] = jnp.where(lane < heads, top, pltpu.roll(total, heads, 1))
    sty_send = remote(st_c, st_y, stsem.at[2], stsem.at[3], ynbr)
    sty_send.start()
    y_send = []
    for s in range(NS):
        p_send[s].wait_recv()
        sl = slice(s * rows_s, (s + 1) * rows_s)
        for h in range(mine):
            acc_c[h, sl, :] = acc[core * mine + h, sl, :] * ea[sl, h:h + 1] + acc_p[h, sl, :] * eb[sl, h:h + 1]
        copy = remote(acc_c.at[:, part_rows(s)], acc_y.at[:, part_rows(s)], dsem.at[2, s], dsem.at[3, s], ynbr)
        copy.start()
        y_send.append(copy)
    sty_send.wait_recv()
    _, ea, eb, total = merge(st_c[...], st_y[...])
    o_send = []

    def send_a(j):
        return remote(part.at[j], land_a.at[j], fsem.at[0, j], fsem.at[1, j], {"tp": z_in})

    def send_b(j):
        return remote(part.at[j], land_b.at[j], fsem.at[2, j], fsem.at[3, j], {"tp": z_in})

    def send_c(j):
        return remote(tot.at[me, j], tot.at[me, j], fsem.at[4, j], fsem.at[5, j], {"tp": z_out})

    def send_d(j):
        return remote(tot.at[me, j], tot.at[me, j], fsem.at[6, j], fsem.at[7, j], ynbr)

    def send_e(j):
        return remote(tot.at[me, j], tot.at[me, j], fsem.at[8, j], fsem.at[9, j], partner)

    def send_f(j):
        return remote(tot.at[across, j], tot.at[across, j], fsem.at[10, j], fsem.at[11, j], partner)

    for half in range(HALVES):
        chunks = range(half * NS // HALVES, (half + 1) * NS // HALVES)
        for s in chunks:
            y_send[s].wait_recv()
            sl = slice(s * rows_s, (s + 1) * rows_s)
            for h in range(mine):
                o = acc_c[h, sl, :] * ea[sl, h:h + 1] + acc_y[h, sl, :] * eb[sl, h:h + 1]
                o = round_bf16(o / total[sl, h:h + 1])
                o_own[h, sl, :] = o
                obf[sl, pl.ds(pl.multiple_of((core * mine + h) * hd, hd), hd)] = o.astype(BF16)
            copy = remote(o_own.at[:, part_rows(s)], o_land.at[:, part_rows(s)], dsem.at[4, s], dsem.at[5, s], partner)
            copy.start()
            o_send.append(copy)
        for s in chunks:
            o_send[s].wait_recv()
            sl = slice(s * rows_s, (s + 1) * rows_s)
            for h in range(mine):
                obf[sl, pl.ds(pl.multiple_of(((1 - core) * mine + h) * hd, hd), hd)] = o_land[h, sl, :].astype(BF16)

        def project(t, half=half):
            if half == 0:
                wcopy(t).wait()
            j = half * mine_n + t
            part[j] = jnp.dot(obf[half * rows_h:(half + 1) * rows_h, :], wob[t], preferred_element_type=F32)

            @pl.when(outer)
            def _():
                send_a(j).start()

        repeat(0, mine_n, project)
    hcopy.wait()

    def emit(quarter, count, j):
        half = j // count
        rows = pl.ds(pl.multiple_of(half * rows_h, rows_h), rows_h)
        where = columns(quarter, j - half * count)
        out[rows, where] = (hbuf[rows, where].astype(F32) + tot[quarter, j]).astype(BF16)

    def share(j):
        send_d(j).start()
        send_e(j).start()
        emit(me, mine_n, j)

    def collect_y(j):
        send_d(j).wait_recv()
        send_f(j).start()
        emit(across, mine_n, j)

    def collect_core(j):
        send_e(j).wait_recv()
        emit(mate, mate_n, j)

    def last(j):
        send_f(j).wait_recv()
        emit(diagonal, mate_n, j)

    mine_c = HALVES * mine_n
    mate_c = HALVES * mate_n

    def collect(k):
        @pl.when(k >= 0)
        def _():
            collect_y(k)

        @pl.when(jnp.logical_and(k >= 0, k < mate_c))
        def _():
            collect_core(k)

    @pl.when(outer)
    def _():
        def step(j):
            @pl.when(j < mine_c)
            def _():
                send_c(j).wait_recv()
                share(j)

            collect(j - LAG)

        repeat(0, mine_c + LAG, step)
        repeat(0, mine_c, lambda j: send_a(j).wait_send())

    @pl.when(inner)
    def _():
        def step(j):
            @pl.when(j < mine_c)
            def _():
                send_a(j).wait_recv()
                part[j] = part[j] + land_a[j]
                send_b(j).start()

            k = j - LAG

            @pl.when(jnp.logical_and(k >= 0, k < mine_c))
            def _():
                send_b(k).wait_recv()
                tot[me, k] = part[k] + land_b[k]
                send_c(k).start()
                share(k)

            collect(j - 2 * LAG)

        repeat(0, mine_c + 2 * LAG, step)

        def drain(j):
            send_b(j).wait_send()
            send_c(j).wait_send()

        repeat(0, mine_c, drain)

    repeat(mine_c, mate_c, collect_core)
    repeat(0, mate_c, last)
    st_send.wait_send()
    sty_send.wait_send()
    for s in range(NS):
        p_send[s].wait_send()
        y_send[s].wait_send()
        o_send[s].wait_send()

    def finish(j):
        send_d(j).wait_send()
        send_e(j).wait_send()
        send_f(j).wait_send()

    repeat(0, mine_c, finish)


def solution(mesh):
    vmem = pl.BlockSpec(memory_space=pltpu.VMEM)
    smem = pl.BlockSpec(memory_space=pltpu.SMEM)
    hbm = pl.BlockSpec(memory_space=pltpu.HBM)
    dma = pltpu.SemaphoreType.DMA

    def keep(x):
        return pltpu.with_memory_space_constraint(x, pltpu.VMEM)

    def stay(x):
        return pltpu.with_memory_space_constraint(x, pltpu.HBM)

    def params(mib, collective=None):
        if collective is None:
            return pltpu.CompilerParams(vmem_limit_bytes=mib * 2**20)
        return pltpu.CompilerParams(vmem_limit_bytes=mib * 2**20, collective_id=collective, has_side_effects=True)

    def local_step(hidden, norm_gain, w_query, w_key, w_value, w_out, k_cache, v_cache, positions):
        batch, seq_local, kv_local, hd = k_cache.shape
        d_model, q_cols = w_query.shape
        heads = q_cols // hd
        rows = seq_local * kv_local
        tiles = 2
        tcols = q_cols // 4 // tiles
        cache = (batch, rows, hd)
        acc_type = pltpu.VMEM((heads * batch, hd), F32)
        q, kv, k_in, v_in = pl.pallas_call(
            qkv_kernel,
            out_shape=(acc_type, pltpu.VMEM((2, 2, batch, hd), F32), pltpu.VMEM(cache, BF16), pltpu.VMEM(cache, BF16)),
            in_specs=[hbm] * 8,
            out_specs=(vmem,) * 4,
            scratch_shapes=[
                pltpu.SMEM((batch,), jnp.int32),
                pltpu.VMEM((batch, d_model), BF16),
                pltpu.VMEM((1, d_model), F32),
                pltpu.VMEM((batch, d_model), BF16),
                pltpu.VMEM((tiles, d_model, tcols), BF16),
                pltpu.VMEM((d_model, hd), BF16),
                pltpu.VMEM((4, 5, batch, hd), F32),
                dma((1,)),
                dma((3,)),
                dma((tiles,)),
                dma((2, 4)),
                dma((6, tiles + 1)),
            ],
            compiler_params=params(24, 0),
            name="qkv",
        )(
            stay(positions), stay(hidden), stay(norm_gain.reshape(1, d_model)), stay(w_query), stay(w_key), stay(w_value),
            stay(k_cache.reshape(cache)), stay(v_cache.reshape(cache)),
        )

        k_upd, v_upd, acc, stat, _, _ = pl.pallas_call(
            attention_kernel,
            out_shape=(
                jax.ShapeDtypeStruct(cache, BF16), jax.ShapeDtypeStruct(cache, BF16),
                acc_type, pltpu.VMEM((batch, hd), F32),
                pltpu.VMEM(cache, BF16), pltpu.VMEM(cache, BF16),
            ),
            in_specs=[smem, vmem, vmem, vmem, vmem],
            out_specs=(hbm, hbm, vmem, vmem, vmem, vmem),
            input_output_aliases={3: 4, 4: 5},
            scratch_shapes=[
                pltpu.VMEM((heads * batch, hd), F32),
                pltpu.VMEM((heads * batch, hd), F32),
                dma((2, batch // 8)),
            ],
            compiler_params=params(10),
            name="attention",
        )(positions, keep(q), keep(kv), keep(k_in), keep(v_in))

        mine = heads // 2
        ocols = d_model // 2 // TILES
        buf = pltpu.VMEM((mine, batch, hd), F32)
        st = pltpu.VMEM((batch, hd), F32)
        messages = HALVES * MOST
        block = (batch // HALVES, ocols)
        chunk = pltpu.VMEM((messages,) + block, F32)
        out = pl.pallas_call(
            output_kernel,
            out_shape=pltpu.VMEM((batch, d_model), BF16),
            in_specs=[vmem, vmem, hbm, hbm],
            out_specs=vmem,
            scratch_shapes=[
                pltpu.VMEM((batch, d_model), BF16),
                pltpu.VMEM((MOST, q_cols, ocols), BF16),
                pltpu.VMEM((batch, q_cols), BF16),
                buf, buf, buf, buf, buf, st, st, st, chunk, chunk, chunk,
                pltpu.VMEM((4, messages) + block, F32),
                dma((MOST + 1,)),
                dma((4,)),
                dma((6, NS)),
                dma((12, messages)),
            ],
            compiler_params=params(28, 1),
            name="output",
        )(keep(acc.reshape(heads, batch, hd)), keep(stat), stay(hidden), stay(w_out))
        return out, k_upd.reshape(k_cache.shape), v_upd.reshape(v_cache.shape)

    cache_spec = P("dp", "sp", "tp", None)
    specs_in = (P("dp", None), P(None), P(None, "tp"), P(None, "tp"), P(None, "tp"), P("tp", None), cache_spec, cache_spec, P("dp"))
    specs_out = (P("dp", None), cache_spec, cache_spec)
    return jax.shard_map(local_step, mesh=mesh, in_specs=specs_in, out_specs=specs_out, check_vma=False)
```

```python
import math

import jax
import jax.numpy as jnp
from jax import lax
from jax.experimental import pallas as pl
from jax.experimental.pallas import tpu as pltpu
from jax.sharding import PartitionSpec as P

ROPE_BASE = 1000000.0
EPS = 1e-5
NEG_BIG = float(jnp.finfo(jnp.float32).min)
MESH = pl.DeviceIdType.MESH
F32 = jnp.float32
BF16 = jnp.bfloat16
TILES = 8
HALVES = 2
COUNT = TILES * HALVES
NS = 4
LAG_Z = 5
LAG_Y = 5
GROUP = 4


def remote(src, dst, send, recv, device):
    return pltpu.make_async_remote_copy(
        src_ref=src, dst_ref=dst, send_sem=send, recv_sem=recv, device_id=device, device_id_type=MESH
    )


def round_bf16(x):
    return x.astype(BF16).astype(F32)


def qkv_kernel(
    pos, hid, gain, wq, wk, wv, kc, vc, q_out, kv_out, kc_out, vc_out,
    pos_s, hbuf, gbuf, rbuf, wqb, wkvb, pieces, psem, hsem, wsem, csem, xsem,
):
    me = lax.axis_index("sp")
    core = lax.rem(me, 2)
    mate = me + 1 - 2 * core
    across = lax.rem(me + 2, 4)
    partner = {"sp": mate}
    ynbr = {"sp": across}
    batch, d_model = hid.shape
    tiles, _, cols = wqb.shape
    quarter = tiles * cols
    hcopy = pltpu.make_async_copy(hid, hbuf, hsem.at[0])
    gcopy = pltpu.make_async_copy(gain, gbuf, hsem.at[1])
    pcopy = pltpu.make_async_copy(pos, pos_s, psem.at[0])
    hcopy.start()
    gcopy.start()
    pcopy.start()
    head_cols = pl.ds(pl.multiple_of(core * 128, 128), 128)
    keys = me < 2

    @pl.when(keys)
    def _():
        pltpu.make_async_copy(wk.at[:, head_cols], wkvb, hsem.at[2]).start()

    @pl.when(jnp.logical_not(keys))
    def _():
        pltpu.make_async_copy(wv.at[:, head_cols], wkvb, hsem.at[2]).start()

    def wcopy(t):
        return pltpu.make_async_copy(
            wq.at[:, pl.ds(pl.multiple_of(me * quarter + t * cols, cols), cols)], wqb.at[t], wsem.at[t]
        )

    for t in range(tiles):
        wcopy(t).start()
    barrier = pltpu.get_barrier_semaphore()
    pl.semaphore_signal(barrier, inc=1, device_id=partner, device_id_type=MESH)
    pl.semaphore_signal(barrier, inc=1, device_id=ynbr, device_id_type=MESH)

    def cache_copy(which, g):
        src, dst = ((kc, kc_out), (vc, vc_out))[which]
        rows = pl.ds(g * (batch // 4), batch // 4)
        return pltpu.make_async_copy(src.at[rows], dst.at[rows], csem.at[which, g])

    pcopy.wait()
    lane = lax.broadcasted_iota(jnp.int32, (batch, 128), 1)
    row = lax.broadcasted_iota(jnp.int32, (batch, 128), 0)
    position = jnp.zeros((batch, 128), jnp.int32)
    for b in range(batch):
        position = jnp.where(row == b, pos_s[b], position)
    index = jnp.where(lane < 64, lane, lane - 64).astype(F32)
    angle = position.astype(F32) * jnp.exp(index * (-2.0 / 128 * math.log(ROPE_BASE)))
    cosf = jnp.cos(angle)
    sinf = jnp.where(lane < 64, -1.0, 1.0) * jnp.sin(angle)

    hcopy.wait()
    gcopy.wait()

    def norm_rows(i, carry):
        rows = pl.ds(pl.multiple_of(i * 16, 16), 16)
        x = hbuf[rows, :].astype(F32)
        scale = lax.rsqrt(jnp.sum(x * x, axis=-1, keepdims=True) * (1.0 / d_model) + EPS)
        rbuf[rows, :] = (x * scale * gbuf[...]).astype(BF16)
        return carry

    lax.fori_loop(0, batch // 16, norm_rows, 0)

    def rotate(x):
        return x * cosf + pltpu.roll(x, 64, 1) * sinf

    order = (4, 0, 1, 2, 3)

    def exchange(kind, owner, p, device):
        part = pieces.at[owner, p]
        return remote(part, part, xsem.at[2 * kind, p], xsem.at[2 * kind + 1, p], device)

    def publish(p):
        exchange(0, me, p, ynbr).start()
        exchange(1, me, p, partner).start()

    pltpu.make_async_copy(wk.at[:, head_cols], wkvb, hsem.at[2]).wait()
    kv = jnp.dot(rbuf[...], wkvb[...], preferred_element_type=F32)
    pieces[me, 4] = round_bf16(jnp.where(keys, rotate(kv), kv))
    pl.semaphore_wait(barrier, 2)
    publish(4)
    for t in range(tiles):
        wcopy(t).wait()
        if t == tiles - 1:
            for g in range(4):
                cache_copy(0, g).start()
                cache_copy(1, g).start()
        q = jnp.dot(rbuf[...], wqb[t], preferred_element_type=F32)
        for h in range(2):
            pieces[me, 2 * t + h] = round_bf16(rotate(q[:, h * 128:(h + 1) * 128]))
            publish(2 * t + h)
    for p in order:
        exchange(0, me, p, ynbr).wait_recv()
        exchange(2, across, p, partner).start()
    for p in order:
        exchange(1, me, p, partner).wait_recv()
        exchange(2, across, p, partner).wait_recv()
    for owner in range(4):
        for h in range(4):
            q_out[pl.ds((owner * 4 + h) * batch, batch), :] = pieces[owner, h]
        kv_out[owner % 2, owner // 2] = pieces[owner, 4]
    for p in order:
        exchange(0, me, p, ynbr).wait_send()
        exchange(1, me, p, partner).wait_send()
        exchange(2, across, p, partner).wait_send()
    for g in range(4):
        cache_copy(0, g).wait()
        cache_copy(1, g).wait()


def attention_kernel(
    pos, q_ref, kv_ref, kc, vc, ko, vo, acc_ref, stat_ref, kbuf, vbuf, mbuf, lbuf, osem,
):
    batch, rows, hd = kbuf.shape
    heads = acc_ref.shape[0] // batch
    groups = batch // 8
    me = lax.axis_index("sp")
    first = me * (rows // 2)

    def seqs(g):
        return pl.ds(pl.multiple_of(g * 8, 8), 8)

    def store(which, g):
        src, dst = ((kbuf, ko), (vbuf, vo))[which]
        return pltpu.make_async_copy(src.at[seqs(g)], dst.at[seqs(g)], osem.at[which, g])

    row_iota = lax.broadcasted_iota(jnp.int32, (16, hd), 0)
    col_iota = lax.broadcasted_iota(jnp.int32, (heads, rows), 1)
    head_iota = lax.broadcasted_iota(jnp.int32, (heads, rows), 0)
    col_head = lax.rem(col_iota, 2)
    col_pos = jnp.where(col_head == head_iota // (heads // 2), first + col_iota // 2, 1 << 20)

    def group(g, carry):
        for i in range(8):
            b = g * 8 + i
            slot = 2 * (pos[b] - first)
            inside = jnp.logical_and(slot >= 0, slot < rows)
            base = pl.multiple_of((jnp.clip(slot, 0, rows - 1) // 16) * 16, 16)
            target = jnp.where(inside, slot - base, -100)
            for buf, which in ((kbuf, 0), (vbuf, 1)):
                old = buf[b, pl.ds(base, 16), :].astype(F32)
                new0 = kv_ref[0, which, pl.ds(b, 1), :]
                new1 = kv_ref[1, which, pl.ds(b, 1), :]
                new = jnp.where(row_iota == target, new0, jnp.where(row_iota == target + 1, new1, old))
                buf[b, pl.ds(base, 16), :] = new.astype(BF16)
        scores = []
        for i in range(8):
            b = g * 8 + i
            q = q_ref[pl.ds(b, heads, stride=batch), :].astype(BF16)
            s = lax.dot_general(q, kbuf[b], (((1,), (1,)), ((), ())), preferred_element_type=F32) * (hd ** -0.5)
            scores.append(jnp.where(col_pos <= pos[b], s, NEG_BIG))
        for i in range(8):
            b = g * 8 + i
            s = scores[i]
            top = jnp.max(s, axis=-1, keepdims=True)
            weights = jnp.where(col_pos <= pos[b], jnp.exp(s - top), 0.0)
            total = jnp.sum(weights, axis=-1, keepdims=True)
            where = pl.ds(b, heads, stride=batch)
            acc_ref[where, :] = jnp.dot(weights.astype(BF16), vbuf[b], preferred_element_type=F32)
            mbuf[where, :] = jnp.broadcast_to(top, (heads, hd))
            lbuf[where, :] = jnp.broadcast_to(total, (heads, hd))
        store(0, g).start()
        store(1, g).start()
        return carry

    lax.fori_loop(0, groups, group, 0)
    lane = lax.broadcasted_iota(jnp.int32, (batch, hd), 1)
    packed = jnp.zeros((batch, hd), F32)
    for h in range(heads):
        packed = jnp.where(lane == h, mbuf[h * batch:(h + 1) * batch, :], packed)
        packed = jnp.where(lane == heads + h, lbuf[h * batch:(h + 1) * batch, :], packed)
    stat_ref[...] = packed
    for g in range(groups):
        store(0, g).wait()
        store(1, g).wait()


def output_kernel(
    acc, stat, hid, wo, out,
    hbuf, wob, obf, acc_p, acc_c, acc_y, o_own, o_land, st_p, st_c, st_y, part, land_a, land_b, tot,
    lsem, stsem, dsem, fsem, rsem, esem,
):
    z = lax.axis_index("tp")
    me = lax.axis_index("sp")
    core = lax.rem(me, 2)
    mate = me + 1 - 2 * core
    across = lax.rem(me + 2, 4)
    diagonal = across + 1 - 2 * core
    partner = {"sp": mate}
    ynbr = {"sp": across}
    outer = jnp.logical_or(z == 0, z == 3)
    inner = jnp.logical_not(outer)
    z_in = jnp.where(z == 0, 1, jnp.where(z == 1, 2, jnp.where(z == 2, 1, 2)))
    z_out = jnp.where(z == 1, 0, 3)
    heads, batch, hd = acc.shape
    mine = heads // 2
    tile = wob.shape[2]
    rows_s = batch // NS
    rows_h = batch // HALVES

    hcopy = pltpu.make_async_copy(hid, hbuf, lsem.at[TILES])

    def columns(quarter, t):
        return pl.ds(pl.multiple_of((quarter * TILES + t) * tile, tile), tile)

    def wcopy(t):
        return pltpu.make_async_copy(wo.at[:, columns(me, t)], wob.at[t], lsem.at[t])

    def repeat(low, high, body):
        def step(i, carry):
            body(i)
            return carry

        lax.fori_loop(low, high, step, 0)

    barrier = pltpu.get_barrier_semaphore()
    pl.semaphore_signal(barrier, inc=1, device_id=partner, device_id_type=MESH)
    pl.semaphore_signal(barrier, inc=1, device_id=ynbr, device_id_type=MESH)

    @pl.when(z > 0)
    def _():
        pl.semaphore_signal(barrier, inc=1, device_id={"tp": z - 1}, device_id_type=MESH)

    @pl.when(z < 3)
    def _():
        pl.semaphore_signal(barrier, inc=1, device_id={"tp": z + 1}, device_id_type=MESH)

    repeat(0, TILES, lambda t: wcopy(t).start())
    hcopy.start()

    @pl.when(outer)
    def _():
        pl.semaphore_wait(barrier, 3)

    @pl.when(inner)
    def _():
        pl.semaphore_wait(barrier, 4)

    def part_rows(s):
        return pl.ds(s * rows_s, rows_s)

    st_send = remote(stat, st_p, stsem.at[0], stsem.at[1], partner)
    st_send.start()
    p_send = []
    for s in range(NS):
        copy = remote(
            acc.at[pl.ds((1 - core) * mine, mine), part_rows(s)], acc_p.at[:, part_rows(s)],
            dsem.at[0, s], dsem.at[1, s], partner,
        )
        copy.start()
        p_send.append(copy)

    lane = lax.broadcasted_iota(jnp.int32, (batch, hd), 1)

    def merge(a, b):
        top = jnp.maximum(a, b)
        ea = jnp.exp(a - top)
        eb = jnp.exp(b - top)
        la = pltpu.roll(a, hd - heads, 1)
        lb = pltpu.roll(b, hd - heads, 1)
        return top, ea, eb, la * ea + lb * eb

    def own_heads(x):
        return jnp.where(core == 0, x, pltpu.roll(x, hd - mine, 1))

    st_send.wait_recv()
    top, ea, eb, total = merge(own_heads(stat[...]), own_heads(st_p[...]))
    st_c[...] = jnp.where(lane < heads, top, pltpu.roll(total, heads, 1))
    sty_send = remote(st_c, st_y, stsem.at[2], stsem.at[3], ynbr)
    sty_send.start()
    y_send = []
    for s in range(NS):
        p_send[s].wait_recv()
        sl = slice(s * rows_s, (s + 1) * rows_s)
        for h in range(mine):
            acc_c[h, sl, :] = acc[core * mine + h, sl, :] * ea[sl, h:h + 1] + acc_p[h, sl, :] * eb[sl, h:h + 1]
        copy = remote(acc_c.at[:, part_rows(s)], acc_y.at[:, part_rows(s)], dsem.at[2, s], dsem.at[3, s], ynbr)
        copy.start()
        y_send.append(copy)
    sty_send.wait_recv()
    _, ea, eb, total = merge(st_c[...], st_y[...])
    o_send = []

    def send_a(j):
        return remote(part.at[j], land_a.at[j], fsem.at[0], rsem.at[0, j], {"tp": z_in})

    def send_b(j):
        return remote(part.at[j], land_b.at[j], fsem.at[1], rsem.at[1, j], {"tp": z_in})

    def send_c(j):
        return remote(tot.at[me, j], tot.at[me, j], fsem.at[2], rsem.at[2, j], {"tp": z_out})

    def send_d(j):
        return remote(tot.at[me, j], tot.at[me, j], fsem.at[3], rsem.at[3, j], ynbr)

    def send_e(j):
        return remote(tot.at[me, j], tot.at[me, j], fsem.at[4], esem.at[0, j // GROUP], partner)

    def send_f(j):
        return remote(tot.at[across, j], tot.at[across, j], fsem.at[5], esem.at[1, j // GROUP], partner)

    def project(half, t):
        if half == 0:
            wcopy(t).wait()
        j = half * TILES + t
        part[j] = jnp.dot(obf[half * rows_h:(half + 1) * rows_h, :], wob[t], preferred_element_type=F32)

    def project_send(half):
        def step(t):
            project(half, t)

            @pl.when(outer)
            def _():
                send_a(half * TILES + t).start()

        repeat(0, TILES, step)

    for half in range(HALVES):
        chunks = range(half * NS // HALVES, (half + 1) * NS // HALVES)
        for s in chunks:
            y_send[s].wait_recv()
            sl = slice(s * rows_s, (s + 1) * rows_s)
            for h in range(mine):
                o = acc_c[h, sl, :] * ea[sl, h:h + 1] + acc_y[h, sl, :] * eb[sl, h:h + 1]
                o = round_bf16(o / total[sl, h:h + 1])
                o_own[h, sl, :] = o
                obf[sl, pl.ds(pl.multiple_of((core * mine + h) * hd, hd), hd)] = o.astype(BF16)
            copy = remote(o_own.at[:, part_rows(s)], o_land.at[:, part_rows(s)], dsem.at[4, s], dsem.at[5, s], partner)
            copy.start()
            o_send.append(copy)
        for s in chunks:
            o_send[s].wait_recv()
            sl = slice(s * rows_s, (s + 1) * rows_s)
            for h in range(mine):
                obf[sl, pl.ds(pl.multiple_of(((1 - core) * mine + h) * hd, hd), hd)] = o_land[h, sl, :].astype(BF16)

        if half < HALVES - 1:
            project_send(half)
    hcopy.wait()

    def emit(quarter, j):
        half = j // TILES
        rows = pl.ds(pl.multiple_of(half * rows_h, rows_h), rows_h)
        where = columns(quarter, j - half * TILES)
        out[rows, where] = (hbuf[rows, where].astype(F32) + tot[quarter, j]).astype(BF16)

    def share(j):
        send_d(j).start()
        send_e(j).start()
        emit(me, j)

    def collect(j):
        @pl.when(j >= 0)
        def _():
            send_d(j).wait_recv()
            send_f(j).start()
            emit(across, j)

    def gather(kind, owner, g):
        group = tot.at[owner, pl.ds(g * GROUP, GROUP)]
        remote(group, group, fsem.at[4 + kind], esem.at[kind, g], partner).wait_recv()
        repeat(g * GROUP, (g + 1) * GROUP, lambda j: emit(owner, j))

    groups = COUNT // GROUP

    def trickle(j, last):
        for g in range(groups):
            @pl.when(j == last - groups + g)
            def _(g=g):
                gather(0, mate, g)

    @pl.when(outer)
    def _():
        project_send(HALVES - 1)

        def step(j):
            @pl.when(j < COUNT)
            def _():
                send_c(j).wait_recv()
                share(j)

            collect(j - LAG_Y)
            trickle(j, COUNT + LAG_Y)

        repeat(0, COUNT + LAG_Y, step)
        remote(part, land_a, fsem.at[0], rsem.at[0, 0], {"tp": z_in}).wait_send()

    @pl.when(inner)
    def _():
        def step(j):
            @pl.when(j < TILES)
            def _():
                project(HALVES - 1, j)

            @pl.when(j < COUNT)
            def _():
                send_a(j).wait_recv()
                part[j] = part[j] + land_a[j]
                send_b(j).start()

            k = j - LAG_Z

            @pl.when(jnp.logical_and(k >= 0, k < COUNT))
            def _():
                send_b(k).wait_recv()
                tot[me, k] = part[k] + land_b[k]
                send_c(k).start()
                share(k)

            collect(k - LAG_Y)
            trickle(j, COUNT + LAG_Z + LAG_Y)

        repeat(0, COUNT + LAG_Z + LAG_Y, step)
        remote(part, land_b, fsem.at[1], rsem.at[1, 0], {"tp": z_in}).wait_send()
        remote(tot.at[me], tot.at[me], fsem.at[2], rsem.at[2, 0], {"tp": z_out}).wait_send()

    for g in range(groups):
        gather(1, diagonal, g)
    st_send.wait_send()
    sty_send.wait_send()
    for s in range(NS):
        p_send[s].wait_send()
        y_send[s].wait_send()
        o_send[s].wait_send()
    remote(tot.at[me], tot.at[me], fsem.at[3], rsem.at[3, 0], ynbr).wait_send()
    remote(tot.at[me], tot.at[me], fsem.at[4], esem.at[0, 0], partner).wait_send()
    remote(tot.at[across], tot.at[across], fsem.at[5], esem.at[1, 0], partner).wait_send()


def solution(mesh):
    vmem = pl.BlockSpec(memory_space=pltpu.VMEM)
    smem = pl.BlockSpec(memory_space=pltpu.SMEM)
    hbm = pl.BlockSpec(memory_space=pltpu.HBM)
    dma = pltpu.SemaphoreType.DMA

    def keep(x):
        return pltpu.with_memory_space_constraint(x, pltpu.VMEM)

    def stay(x):
        return pltpu.with_memory_space_constraint(x, pltpu.HBM)

    def params(mib, collective=None):
        if collective is None:
            return pltpu.CompilerParams(vmem_limit_bytes=mib * 2**20)
        return pltpu.CompilerParams(vmem_limit_bytes=mib * 2**20, collective_id=collective, has_side_effects=True)

    def local_step(hidden, norm_gain, w_query, w_key, w_value, w_out, k_cache, v_cache, positions):
        batch, seq_local, kv_local, hd = k_cache.shape
        d_model, q_cols = w_query.shape
        heads = q_cols // hd
        rows = seq_local * kv_local
        tiles = 2
        tcols = q_cols // 4 // tiles
        cache = (batch, rows, hd)
        acc_type = pltpu.VMEM((heads * batch, hd), F32)
        q, kv, k_in, v_in = pl.pallas_call(
            qkv_kernel,
            out_shape=(acc_type, pltpu.VMEM((2, 2, batch, hd), F32), pltpu.VMEM(cache, BF16), pltpu.VMEM(cache, BF16)),
            in_specs=[hbm] * 8,
            out_specs=(vmem,) * 4,
            scratch_shapes=[
                pltpu.SMEM((batch,), jnp.int32),
                pltpu.VMEM((batch, d_model), BF16),
                pltpu.VMEM((1, d_model), F32),
                pltpu.VMEM((batch, d_model), BF16),
                pltpu.VMEM((tiles, d_model, tcols), BF16),
                pltpu.VMEM((d_model, hd), BF16),
                pltpu.VMEM((4, 5, batch, hd), F32),
                dma((1,)),
                dma((3,)),
                dma((tiles,)),
                dma((2, 4)),
                dma((6, 5)),
            ],
            compiler_params=params(24, 0),
            name="qkv",
        )(
            stay(positions), stay(hidden), stay(norm_gain.reshape(1, d_model)), stay(w_query), stay(w_key), stay(w_value),
            stay(k_cache.reshape(cache)), stay(v_cache.reshape(cache)),
        )

        k_upd, v_upd, acc, stat, _, _ = pl.pallas_call(
            attention_kernel,
            out_shape=(
                jax.ShapeDtypeStruct(cache, BF16), jax.ShapeDtypeStruct(cache, BF16),
                acc_type, pltpu.VMEM((batch, hd), F32),
                pltpu.VMEM(cache, BF16), pltpu.VMEM(cache, BF16),
            ),
            in_specs=[smem, vmem, vmem, vmem, vmem],
            out_specs=(hbm, hbm, vmem, vmem, vmem, vmem),
            input_output_aliases={3: 4, 4: 5},
            scratch_shapes=[
                pltpu.VMEM((heads * batch, hd), F32),
                pltpu.VMEM((heads * batch, hd), F32),
                dma((2, batch // 8)),
            ],
            compiler_params=params(10),
            name="attention",
        )(positions, keep(q), keep(kv), keep(k_in), keep(v_in))

        mine = heads // 2
        ocols = d_model // 4 // TILES
        buf = pltpu.VMEM((mine, batch, hd), F32)
        st = pltpu.VMEM((batch, hd), F32)
        block = (batch // HALVES, ocols)
        chunk = pltpu.VMEM((COUNT,) + block, F32)
        out = pl.pallas_call(
            output_kernel,
            out_shape=pltpu.VMEM((batch, d_model), BF16),
            in_specs=[vmem, vmem, hbm, hbm],
            out_specs=vmem,
            scratch_shapes=[
                pltpu.VMEM((batch, d_model), BF16),
                pltpu.VMEM((TILES, q_cols, ocols), BF16),
                pltpu.VMEM((batch, q_cols), BF16),
                buf, buf, buf, buf, buf, st, st, st, chunk, chunk, chunk,
                pltpu.VMEM((4, COUNT) + block, F32),
                dma((TILES + 1,)),
                dma((4,)),
                dma((6, NS)),
                dma((6,)),
                dma((4, COUNT)),
                dma((2, COUNT // GROUP)),
            ],
            compiler_params=params(28, 1),
            name="output",
        )(keep(acc.reshape(heads, batch, hd)), keep(stat), stay(hidden), stay(w_out))
        return out, k_upd.reshape(k_cache.shape), v_upd.reshape(v_cache.shape)

    cache_spec = P("dp", "sp", "tp", None)
    specs_in = (P("dp", None), P(None), P(None, "tp"), P(None, "tp"), P(None, "tp"), P("tp", None), cache_spec, cache_spec, P("dp"))
    specs_out = (P("dp", None), cache_spec, cache_spec)
    return jax.shard_map(local_step, mesh=mesh, in_specs=specs_in, out_specs=specs_out, check_vma=False)
```

```python
import math

import jax
import jax.numpy as jnp
from jax import lax
from jax.experimental import pallas as pl
from jax.experimental.pallas import tpu as pltpu
from jax.sharding import PartitionSpec as P

ROPE_BASE = 1000000.0
EPS = 1e-5
NEG_BIG = float(jnp.finfo(jnp.float32).min)
MESH = pl.DeviceIdType.MESH
F32 = jnp.float32
BF16 = jnp.bfloat16
TILES = 4
BLOCKS = 4
COUNT = TILES * BLOCKS
DIRECT = 2
LAG_Z = 5
LAG_Y = 5
GROUP = 4


def remote(src, dst, send, recv, device):
    return pltpu.make_async_remote_copy(
        src_ref=src, dst_ref=dst, send_sem=send, recv_sem=recv, device_id=device, device_id_type=MESH
    )


def round_bf16(x):
    return x.astype(BF16).astype(F32)


def qkv_kernel(
    pos, hid, gain, wq, wk, wv, kc, vc, q_out, kv_out, kc_out, vc_out,
    pos_s, hbuf, gbuf, rbuf, wqb, wkvb, pieces, psem, hsem, wsem, csem, xsem,
):
    me = lax.axis_index("sp")
    core = lax.rem(me, 2)
    mate = me + 1 - 2 * core
    across = lax.rem(me + 2, 4)
    partner = {"sp": mate}
    ynbr = {"sp": across}
    batch, d_model = hid.shape
    tiles, _, cols = wqb.shape
    quarter = tiles * cols
    hcopy = pltpu.make_async_copy(hid, hbuf, hsem.at[0])
    gcopy = pltpu.make_async_copy(gain, gbuf, hsem.at[1])
    pcopy = pltpu.make_async_copy(pos, pos_s, psem.at[0])
    hcopy.start()
    gcopy.start()
    pcopy.start()
    head_cols = pl.ds(pl.multiple_of(core * 128, 128), 128)
    keys = me < 2

    @pl.when(keys)
    def _():
        pltpu.make_async_copy(wk.at[:, head_cols], wkvb, hsem.at[2]).start()

    @pl.when(jnp.logical_not(keys))
    def _():
        pltpu.make_async_copy(wv.at[:, head_cols], wkvb, hsem.at[2]).start()

    def wcopy(t):
        return pltpu.make_async_copy(
            wq.at[:, pl.ds(pl.multiple_of(me * quarter + t * cols, cols), cols)], wqb.at[t], wsem.at[t]
        )

    for t in range(tiles):
        wcopy(t).start()
    barrier = pltpu.get_barrier_semaphore()
    pl.semaphore_signal(barrier, inc=1, device_id=partner, device_id_type=MESH)
    pl.semaphore_signal(barrier, inc=1, device_id=ynbr, device_id_type=MESH)

    def cache_copy(which, g):
        src, dst = ((kc, kc_out), (vc, vc_out))[which]
        rows = pl.ds(g * (batch // 4), batch // 4)
        return pltpu.make_async_copy(src.at[rows], dst.at[rows], csem.at[which, g])

    pcopy.wait()
    lane = lax.broadcasted_iota(jnp.int32, (batch, 128), 1)
    row = lax.broadcasted_iota(jnp.int32, (batch, 128), 0)
    position = jnp.zeros((batch, 128), jnp.int32)
    for b in range(batch):
        position = jnp.where(row == b, pos_s[b], position)
    index = jnp.where(lane < 64, lane, lane - 64).astype(F32)
    angle = position.astype(F32) * jnp.exp(index * (-2.0 / 128 * math.log(ROPE_BASE)))
    cosf = jnp.cos(angle)
    sinf = jnp.where(lane < 64, -1.0, 1.0) * jnp.sin(angle)

    hcopy.wait()
    gcopy.wait()

    def norm_rows(i, carry):
        rows = pl.ds(pl.multiple_of(i * 16, 16), 16)
        x = hbuf[rows, :].astype(F32)
        scale = lax.rsqrt(jnp.sum(x * x, axis=-1, keepdims=True) * (1.0 / d_model) + EPS)
        rbuf[rows, :] = (x * scale * gbuf[...]).astype(BF16)
        return carry

    lax.fori_loop(0, batch // 16, norm_rows, 0)

    def rotate(x):
        return x * cosf + pltpu.roll(x, 64, 1) * sinf

    order = (4, 0, 1, 2, 3)

    def exchange(kind, owner, p, device):
        part = pieces.at[owner, p]
        return remote(part, part, xsem.at[2 * kind, p], xsem.at[2 * kind + 1, p], device)

    def publish(p):
        exchange(0, me, p, ynbr).start()
        exchange(1, me, p, partner).start()

    pltpu.make_async_copy(wk.at[:, head_cols], wkvb, hsem.at[2]).wait()
    kv = jnp.dot(rbuf[...], wkvb[...], preferred_element_type=F32)
    pieces[me, 4] = round_bf16(jnp.where(keys, rotate(kv), kv))
    pl.semaphore_wait(barrier, 2)
    publish(4)
    for t in range(tiles):
        wcopy(t).wait()
        if t == tiles - 1:
            for g in range(4):
                cache_copy(0, g).start()
                cache_copy(1, g).start()
        q = jnp.dot(rbuf[...], wqb[t], preferred_element_type=F32)
        for h in range(2):
            pieces[me, 2 * t + h] = round_bf16(rotate(q[:, h * 128:(h + 1) * 128]))
            publish(2 * t + h)
    for p in order:
        exchange(0, me, p, ynbr).wait_recv()
        exchange(2, across, p, partner).start()
    for p in order:
        exchange(1, me, p, partner).wait_recv()
        exchange(2, across, p, partner).wait_recv()
    for owner in range(4):
        for h in range(4):
            q_out[pl.ds((owner * 4 + h) * batch, batch), :] = pieces[owner, h]
        kv_out[owner % 2, owner // 2] = pieces[owner, 4]
    for p in order:
        exchange(0, me, p, ynbr).wait_send()
        exchange(1, me, p, partner).wait_send()
        exchange(2, across, p, partner).wait_send()
    for g in range(4):
        cache_copy(0, g).wait()
        cache_copy(1, g).wait()


def attention_kernel(
    pos, q_ref, kv_ref, kc, vc, ko, vo, acc_ref, stat_ref, kbuf, vbuf, mbuf, lbuf, osem,
):
    batch, rows, hd = kbuf.shape
    heads = acc_ref.shape[0] // batch
    groups = batch // 8
    me = lax.axis_index("sp")
    first = me * (rows // 2)

    def seqs(g):
        return pl.ds(pl.multiple_of(g * 8, 8), 8)

    def store(which, g):
        src, dst = ((kbuf, ko), (vbuf, vo))[which]
        return pltpu.make_async_copy(src.at[seqs(g)], dst.at[seqs(g)], osem.at[which, g])

    row_iota = lax.broadcasted_iota(jnp.int32, (16, hd), 0)
    col_iota = lax.broadcasted_iota(jnp.int32, (heads, rows), 1)
    head_iota = lax.broadcasted_iota(jnp.int32, (heads, rows), 0)
    col_head = lax.rem(col_iota, 2)
    col_pos = jnp.where(col_head == head_iota // (heads // 2), first + col_iota // 2, 1 << 20)

    def group(g, carry):
        for i in range(8):
            b = g * 8 + i
            slot = 2 * (pos[b] - first)
            inside = jnp.logical_and(slot >= 0, slot < rows)
            base = pl.multiple_of((jnp.clip(slot, 0, rows - 1) // 16) * 16, 16)
            target = jnp.where(inside, slot - base, -100)
            for buf, which in ((kbuf, 0), (vbuf, 1)):
                old = buf[b, pl.ds(base, 16), :].astype(F32)
                new0 = kv_ref[0, which, pl.ds(b, 1), :]
                new1 = kv_ref[1, which, pl.ds(b, 1), :]
                new = jnp.where(row_iota == target, new0, jnp.where(row_iota == target + 1, new1, old))
                buf[b, pl.ds(base, 16), :] = new.astype(BF16)
        scores = []
        for i in range(8):
            b = g * 8 + i
            q = q_ref[pl.ds(b, heads, stride=batch), :].astype(BF16)
            s = lax.dot_general(q, kbuf[b], (((1,), (1,)), ((), ())), preferred_element_type=F32) * (hd ** -0.5)
            scores.append(jnp.where(col_pos <= pos[b], s, NEG_BIG))
        for i in range(8):
            b = g * 8 + i
            s = scores[i]
            top = jnp.max(s, axis=-1, keepdims=True)
            weights = jnp.where(col_pos <= pos[b], jnp.exp(s - top), 0.0)
            total = jnp.sum(weights, axis=-1, keepdims=True)
            where = pl.ds(b, heads, stride=batch)
            acc_ref[where, :] = jnp.dot(weights.astype(BF16), vbuf[b], preferred_element_type=F32)
            mbuf[where, :] = jnp.broadcast_to(top, (heads, hd))
            lbuf[where, :] = jnp.broadcast_to(total, (heads, hd))
        store(0, g).start()
        store(1, g).start()
        return carry

    lax.fori_loop(0, groups, group, 0)
    lane = lax.broadcasted_iota(jnp.int32, (batch, hd), 1)
    packed = jnp.zeros((batch, hd), F32)
    for h in range(heads):
        packed = jnp.where(lane == h, mbuf[h * batch:(h + 1) * batch, :], packed)
        packed = jnp.where(lane == heads + h, lbuf[h * batch:(h + 1) * batch, :], packed)
    stat_ref[...] = packed
    for g in range(groups):
        store(0, g).wait()
        store(1, g).wait()


def output_kernel(
    acc, stat, hid, wo, out,
    hbuf, wob, obf, acc_p, acc_c, acc_y, o_own, o_land, st_p, st_c, st_y, part, land_a, land_b, tot,
    lsem, stsem, dsem, fsem, rsem, esem,
):
    z = lax.axis_index("tp")
    me = lax.axis_index("sp")
    core = lax.rem(me, 2)
    mate = me + 1 - 2 * core
    across = lax.rem(me + 2, 4)
    diagonal = across + 1 - 2 * core
    partner = {"sp": mate}
    ynbr = {"sp": across}
    outer = jnp.logical_or(z == 0, z == 3)
    inner = jnp.logical_not(outer)
    z_in = jnp.where(z == 0, 1, jnp.where(z == 1, 2, jnp.where(z == 2, 1, 2)))
    z_out = jnp.where(z == 1, 0, 3)
    heads, batch, hd = acc.shape
    mine = heads // 2
    tile = wob.shape[2]
    rows_b = batch // BLOCKS

    hcopy = pltpu.make_async_copy(hid, hbuf, lsem.at[TILES])

    def columns(quarter, t):
        return pl.ds(pl.multiple_of((quarter * TILES + t) * tile, tile), tile)

    def wcopy(t):
        return pltpu.make_async_copy(wo.at[:, columns(me, t)], wob.at[t], lsem.at[t])

    def repeat(low, high, body):
        def step(i, carry):
            body(i)
            return carry

        lax.fori_loop(low, high, step, 0)

    barrier = pltpu.get_barrier_semaphore()
    pl.semaphore_signal(barrier, inc=1, device_id=partner, device_id_type=MESH)
    pl.semaphore_signal(barrier, inc=1, device_id=ynbr, device_id_type=MESH)

    @pl.when(z > 0)
    def _():
        pl.semaphore_signal(barrier, inc=1, device_id={"tp": z - 1}, device_id_type=MESH)

    @pl.when(z < 3)
    def _():
        pl.semaphore_signal(barrier, inc=1, device_id={"tp": z + 1}, device_id_type=MESH)

    repeat(0, TILES, lambda t: wcopy(t).start())
    hcopy.start()

    @pl.when(outer)
    def _():
        pl.semaphore_signal(barrier, inc=1, device_id={"sp": across, "tp": z_in}, device_id_type=MESH)
        pl.semaphore_wait(barrier, 4)

    @pl.when(inner)
    def _():
        pl.semaphore_signal(barrier, inc=1, device_id={"sp": across, "tp": z_out}, device_id_type=MESH)
        pl.semaphore_wait(barrier, 5)

    def part_rows(s):
        return pl.ds(s * rows_b, rows_b)

    st_send = remote(stat, st_p, stsem.at[0], stsem.at[1], partner)
    st_send.start()
    p_send = []
    for s in range(BLOCKS):
        copy = remote(
            acc.at[pl.ds((1 - core) * mine, mine), part_rows(s)], acc_p.at[:, part_rows(s)],
            dsem.at[0, s], dsem.at[1, s], partner,
        )
        copy.start()
        p_send.append(copy)

    lane = lax.broadcasted_iota(jnp.int32, (batch, hd), 1)

    def merge(a, b):
        top = jnp.maximum(a, b)
        ea = jnp.exp(a - top)
        eb = jnp.exp(b - top)
        la = pltpu.roll(a, hd - heads, 1)
        lb = pltpu.roll(b, hd - heads, 1)
        return top, ea, eb, la * ea + lb * eb

    def own_heads(x):
        return jnp.where(core == 0, x, pltpu.roll(x, hd - mine, 1))

    st_send.wait_recv()
    top, ea, eb, total = merge(own_heads(stat[...]), own_heads(st_p[...]))
    st_c[...] = jnp.where(lane < heads, top, pltpu.roll(total, heads, 1))
    y_send = []
    sty_send = []
    for s in range(BLOCKS):
        p_send[s].wait_recv()
        sl = slice(s * rows_b, (s + 1) * rows_b)
        for h in range(mine):
            acc_c[h, sl, :] = acc[core * mine + h, sl, :] * ea[sl, h:h + 1] + acc_p[h, sl, :] * eb[sl, h:h + 1]
        copy = remote(st_c.at[part_rows(s)], st_y.at[part_rows(s)], stsem.at[2], stsem.at[3 + s], ynbr)
        copy.start()
        sty_send.append(copy)
        copy = remote(acc_c.at[:, part_rows(s)], acc_y.at[:, part_rows(s)], dsem.at[2, s], dsem.at[3, s], ynbr)
        copy.start()
        y_send.append(copy)
    o_send = []

    def send_a(j):
        return remote(part.at[j], land_a.at[j], fsem.at[0], rsem.at[0, j], {"tp": z_in})

    def send_b(j):
        return remote(part.at[j], land_b.at[j], fsem.at[1], rsem.at[1, j], {"tp": z_in})

    def send_c(j):
        return remote(tot.at[me, j], tot.at[me, j], fsem.at[2], rsem.at[2, j], {"tp": z_out})

    def send_d(j):
        return remote(tot.at[me, j], tot.at[me, j], fsem.at[3], rsem.at[3, j], ynbr)

    def send_e(j):
        return remote(tot.at[me, j], tot.at[me, j], fsem.at[4], esem.at[0, j // GROUP], partner)

    def send_f(j):
        return remote(tot.at[across, j], tot.at[across, j], fsem.at[5], esem.at[1, j // GROUP], partner)

    def project(j):
        rows = pl.ds(pl.multiple_of((j // TILES) * rows_b, rows_b), rows_b)
        part[j] = jnp.dot(obf[rows, :], wob[lax.rem(j, TILES)], preferred_element_type=F32)

    for s in range(BLOCKS):
        sl = slice(s * rows_b, (s + 1) * rows_b)
        sty_send[s].wait_recv()
        _, ea, eb, total = merge(st_c[sl, :], st_y[sl, :])
        y_send[s].wait_recv()
        for h in range(mine):
            o = acc_c[h, sl, :] * ea[:, h:h + 1] + acc_y[h, sl, :] * eb[:, h:h + 1]
            o = round_bf16(o / total[:, h:h + 1])
            o_own[h, sl, :] = o
            obf[sl, pl.ds(pl.multiple_of((core * mine + h) * hd, hd), hd)] = o.astype(BF16)
        copy = remote(o_own.at[:, part_rows(s)], o_land.at[:, part_rows(s)], dsem.at[4, s], dsem.at[5, s], partner)
        copy.start()
        o_send.append(copy)
        copy.wait_recv()
        for h in range(mine):
            obf[sl, pl.ds(pl.multiple_of(((1 - core) * mine + h) * hd, hd), hd)] = o_land[h, sl, :].astype(BF16)
        if s == 0:
            def first_block(t):
                wcopy(t).wait()
                project(t)

                @pl.when(outer)
                def _():
                    send_a(t).start()

            repeat(0, TILES, first_block)
        else:
            @pl.when(outer)
            def _(s=s):
                def next_block(j):
                    project(j)
                    send_a(j).start()

                repeat(s * TILES, (s + 1) * TILES, next_block)
    hcopy.wait()

    def emit(quarter, j):
        rows = pl.ds(pl.multiple_of((j // TILES) * rows_b, rows_b), rows_b)
        where = columns(quarter, lax.rem(j, TILES))
        out[rows, where] = (hbuf[rows, where].astype(F32) + tot[quarter, j]).astype(BF16)

    def send_x(j):
        return remote(tot.at[me, j], tot.at[me, j], fsem.at[6], rsem.at[3, j], {"sp": across, "tp": z_out})

    def share(j):
        send_e(j).start()
        emit(me, j)

    def collect(j):
        @pl.when(j >= 0)
        def _():
            send_d(j).wait_recv()
            send_f(j).start()
            emit(across, j)

    def gather(kind, owner, g):
        group = tot.at[owner, pl.ds(g * GROUP, GROUP)]
        remote(group, group, fsem.at[4 + kind], esem.at[kind, g], partner).wait_recv()
        repeat(g * GROUP, (g + 1) * GROUP, lambda j: emit(owner, j))

    groups = COUNT // GROUP

    def trickle(j, last):
        for g in range(groups):
            @pl.when(j == last - groups + g)
            def _(g=g):
                gather(0, mate, g)

    @pl.when(outer)
    def _():
        def step(j):
            @pl.when(j < COUNT)
            def _():
                send_c(j).wait_recv()

                @pl.when(j < COUNT - DIRECT)
                def _():
                    send_d(j).start()

                share(j)

            collect(j - LAG_Y)
            trickle(j, COUNT + LAG_Y)

        repeat(0, COUNT + LAG_Y, step)
        remote(part, land_a, fsem.at[0], rsem.at[0, 0], {"tp": z_in}).wait_send()
        sent = tot.at[me, pl.ds(0, COUNT - DIRECT)]
        remote(sent, sent, fsem.at[3], rsem.at[3, 0], ynbr).wait_send()

    @pl.when(inner)
    def _():
        def step(j):
            @pl.when(j < COUNT - TILES)
            def _():
                project(TILES + j)

            @pl.when(j < COUNT)
            def _():
                send_a(j).wait_recv()
                part[j] = part[j] + land_a[j]
                send_b(j).start()

            k = j - LAG_Z

            @pl.when(jnp.logical_and(k >= 0, k < COUNT))
            def _():
                send_b(k).wait_recv()
                tot[me, k] = part[k] + land_b[k]
                send_c(k).start()
                send_d(k).start()

                @pl.when(k >= COUNT - DIRECT)
                def _():
                    send_x(k).start()

                share(k)

            collect(k - LAG_Y)
            trickle(j, COUNT + LAG_Z + LAG_Y)

        repeat(0, COUNT + LAG_Z + LAG_Y, step)
        remote(part, land_b, fsem.at[1], rsem.at[1, 0], {"tp": z_in}).wait_send()
        remote(tot.at[me], tot.at[me], fsem.at[2], rsem.at[2, 0], {"tp": z_out}).wait_send()
        remote(tot.at[me], tot.at[me], fsem.at[3], rsem.at[3, 0], ynbr).wait_send()
        sent = tot.at[me, pl.ds(0, DIRECT)]
        remote(sent, sent, fsem.at[6], rsem.at[3, 0], ynbr).wait_send()

    for g in range(groups):
        gather(1, diagonal, g)
    st_send.wait_send()
    remote(st_c, st_y, stsem.at[2], stsem.at[3], ynbr).wait_send()
    for s in range(BLOCKS):
        p_send[s].wait_send()
        y_send[s].wait_send()
        o_send[s].wait_send()
    remote(tot.at[me], tot.at[me], fsem.at[4], esem.at[0, 0], partner).wait_send()
    remote(tot.at[across], tot.at[across], fsem.at[5], esem.at[1, 0], partner).wait_send()


def solution(mesh):
    vmem = pl.BlockSpec(memory_space=pltpu.VMEM)
    smem = pl.BlockSpec(memory_space=pltpu.SMEM)
    hbm = pl.BlockSpec(memory_space=pltpu.HBM)
    dma = pltpu.SemaphoreType.DMA

    def keep(x):
        return pltpu.with_memory_space_constraint(x, pltpu.VMEM)

    def stay(x):
        return pltpu.with_memory_space_constraint(x, pltpu.HBM)

    def params(mib, collective=None):
        if collective is None:
            return pltpu.CompilerParams(vmem_limit_bytes=mib * 2**20)
        return pltpu.CompilerParams(vmem_limit_bytes=mib * 2**20, collective_id=collective, has_side_effects=True)

    def local_step(hidden, norm_gain, w_query, w_key, w_value, w_out, k_cache, v_cache, positions):
        batch, seq_local, kv_local, hd = k_cache.shape
        d_model, q_cols = w_query.shape
        heads = q_cols // hd
        rows = seq_local * kv_local
        tiles = 2
        tcols = q_cols // 4 // tiles
        cache = (batch, rows, hd)
        acc_type = pltpu.VMEM((heads * batch, hd), F32)
        q, kv, k_in, v_in = pl.pallas_call(
            qkv_kernel,
            out_shape=(acc_type, pltpu.VMEM((2, 2, batch, hd), F32), pltpu.VMEM(cache, BF16), pltpu.VMEM(cache, BF16)),
            in_specs=[hbm] * 8,
            out_specs=(vmem,) * 4,
            scratch_shapes=[
                pltpu.SMEM((batch,), jnp.int32),
                pltpu.VMEM((batch, d_model), BF16),
                pltpu.VMEM((1, d_model), F32),
                pltpu.VMEM((batch, d_model), BF16),
                pltpu.VMEM((tiles, d_model, tcols), BF16),
                pltpu.VMEM((d_model, hd), BF16),
                pltpu.VMEM((4, 5, batch, hd), F32),
                dma((1,)),
                dma((3,)),
                dma((tiles,)),
                dma((2, 4)),
                dma((6, 5)),
            ],
            compiler_params=params(24, 0),
            name="qkv",
        )(
            stay(positions), stay(hidden), stay(norm_gain.reshape(1, d_model)), stay(w_query), stay(w_key), stay(w_value),
            stay(k_cache.reshape(cache)), stay(v_cache.reshape(cache)),
        )

        k_upd, v_upd, acc, stat, _, _ = pl.pallas_call(
            attention_kernel,
            out_shape=(
                jax.ShapeDtypeStruct(cache, BF16), jax.ShapeDtypeStruct(cache, BF16),
                acc_type, pltpu.VMEM((batch, hd), F32),
                pltpu.VMEM(cache, BF16), pltpu.VMEM(cache, BF16),
            ),
            in_specs=[smem, vmem, vmem, vmem, vmem],
            out_specs=(hbm, hbm, vmem, vmem, vmem, vmem),
            input_output_aliases={3: 4, 4: 5},
            scratch_shapes=[
                pltpu.VMEM((heads * batch, hd), F32),
                pltpu.VMEM((heads * batch, hd), F32),
                dma((2, batch // 8)),
            ],
            compiler_params=params(10),
            name="attention",
        )(positions, keep(q), keep(kv), keep(k_in), keep(v_in))

        mine = heads // 2
        ocols = d_model // 4 // TILES
        buf = pltpu.VMEM((mine, batch, hd), F32)
        st = pltpu.VMEM((batch, hd), F32)
        block = (batch // BLOCKS, ocols)
        chunk = pltpu.VMEM((COUNT,) + block, F32)
        out = pl.pallas_call(
            output_kernel,
            out_shape=pltpu.VMEM((batch, d_model), BF16),
            in_specs=[vmem, vmem, hbm, hbm],
            out_specs=vmem,
            scratch_shapes=[
                pltpu.VMEM((batch, d_model), BF16),
                pltpu.VMEM((TILES, q_cols, ocols), BF16),
                pltpu.VMEM((batch, q_cols), BF16),
                buf, buf, buf, buf, buf, st, st, st, chunk, chunk, chunk,
                pltpu.VMEM((4, COUNT) + block, F32),
                dma((TILES + 1,)),
                dma((3 + BLOCKS,)),
                dma((6, BLOCKS)),
                dma((7,)),
                dma((4, COUNT)),
                dma((2, COUNT // GROUP)),
            ],
            compiler_params=params(28, 1),
            name="output",
        )(keep(acc.reshape(heads, batch, hd)), keep(stat), stay(hidden), stay(w_out))
        return out, k_upd.reshape(k_cache.shape), v_upd.reshape(v_cache.shape)

    cache_spec = P("dp", "sp", "tp", None)
    specs_in = (P("dp", None), P(None), P(None, "tp"), P(None, "tp"), P(None, "tp"), P("tp", None), cache_spec, cache_spec, P("dp"))
    specs_out = (P("dp", None), cache_spec, cache_spec)
    return jax.shard_map(local_step, mesh=mesh, in_specs=specs_in, out_specs=specs_out, check_vma=False)
```

```python
import math

import jax
import jax.numpy as jnp
from jax import lax
from jax.experimental import pallas as pl
from jax.experimental.pallas import tpu as pltpu
from jax.sharding import PartitionSpec as P

ROPE_BASE = 1000000.0
EPS = 1e-5
NEG_BIG = float(jnp.finfo(jnp.float32).min)
MESH = pl.DeviceIdType.MESH
F32 = jnp.float32
BF16 = jnp.bfloat16
TILES = 4
BLOCKS = 4
COUNT = TILES * BLOCKS
DIRECT = 2
LAG_Z = 5
LAG_Y = 5
GROUP = 4


def remote(src, dst, send, recv, device):
    return pltpu.make_async_remote_copy(
        src_ref=src, dst_ref=dst, send_sem=send, recv_sem=recv, device_id=device, device_id_type=MESH
    )


def round_bf16(x):
    return x.astype(BF16).astype(F32)


def qkv_kernel(
    pos, hid, gain, wq, wk, wv, kc, vc, q_out, kv_out, kc_out, vc_out,
    pos_s, hbuf, gbuf, rbuf, wqb, wkvb, pieces, psem, hsem, wsem, csem, xsem,
):
    me = lax.axis_index("sp")
    core = lax.rem(me, 2)
    mate = me + 1 - 2 * core
    across = lax.rem(me + 2, 4)
    partner = {"sp": mate}
    ynbr = {"sp": across}
    batch, d_model = hid.shape
    tiles, _, cols = wqb.shape
    quarter = tiles * cols
    hcopy = pltpu.make_async_copy(hid, hbuf, hsem.at[0])
    gcopy = pltpu.make_async_copy(gain, gbuf, hsem.at[1])
    pcopy = pltpu.make_async_copy(pos, pos_s, psem.at[0])
    hcopy.start()
    gcopy.start()
    pcopy.start()
    head_cols = pl.ds(pl.multiple_of(core * 128, 128), 128)
    keys = me < 2

    @pl.when(keys)
    def _():
        pltpu.make_async_copy(wk.at[:, head_cols], wkvb, hsem.at[2]).start()

    @pl.when(jnp.logical_not(keys))
    def _():
        pltpu.make_async_copy(wv.at[:, head_cols], wkvb, hsem.at[2]).start()

    def wcopy(t):
        return pltpu.make_async_copy(
            wq.at[:, pl.ds(pl.multiple_of(me * quarter + t * cols, cols), cols)], wqb.at[t], wsem.at[t]
        )

    for t in range(tiles):
        wcopy(t).start()
    barrier = pltpu.get_barrier_semaphore()
    pl.semaphore_signal(barrier, inc=1, device_id=partner, device_id_type=MESH)
    pl.semaphore_signal(barrier, inc=1, device_id=ynbr, device_id_type=MESH)

    def cache_copy(which, g):
        src, dst = ((kc, kc_out), (vc, vc_out))[which]
        rows = pl.ds(g * (batch // 4), batch // 4)
        return pltpu.make_async_copy(src.at[rows], dst.at[rows], csem.at[which, g])

    pcopy.wait()
    lane = lax.broadcasted_iota(jnp.int32, (batch, 128), 1)
    row = lax.broadcasted_iota(jnp.int32, (batch, 128), 0)
    position = jnp.zeros((batch, 128), jnp.int32)
    for b in range(batch):
        position = jnp.where(row == b, pos_s[b], position)
    index = jnp.where(lane < 64, lane, lane - 64).astype(F32)
    angle = position.astype(F32) * jnp.exp(index * (-2.0 / 128 * math.log(ROPE_BASE)))
    cosf = jnp.cos(angle)
    sinf = jnp.where(lane < 64, -1.0, 1.0) * jnp.sin(angle)

    hcopy.wait()
    gcopy.wait()

    def norm_rows(i, carry):
        rows = pl.ds(pl.multiple_of(i * 16, 16), 16)
        x = hbuf[rows, :].astype(F32)
        scale = lax.rsqrt(jnp.sum(x * x, axis=-1, keepdims=True) * (1.0 / d_model) + EPS)
        rbuf[rows, :] = (x * scale * gbuf[...]).astype(BF16)
        return carry

    lax.fori_loop(0, batch // 16, norm_rows, 0)

    def rotate(x):
        return x * cosf + pltpu.roll(x, 64, 1) * sinf

    order = (4, 0, 1, 2, 3)

    def exchange(kind, owner, p, device):
        part = pieces.at[owner, p]
        return remote(part, part, xsem.at[2 * kind, p], xsem.at[2 * kind + 1, p], device)

    def publish(p):
        exchange(0, me, p, ynbr).start()
        exchange(1, me, p, partner).start()

    pltpu.make_async_copy(wk.at[:, head_cols], wkvb, hsem.at[2]).wait()
    kv = jnp.dot(rbuf[...], wkvb[...], preferred_element_type=F32)
    pieces[me, 4] = round_bf16(jnp.where(keys, rotate(kv), kv))
    pl.semaphore_wait(barrier, 2)
    publish(4)
    for t in range(tiles):
        wcopy(t).wait()
        if t == tiles - 1:
            for g in range(4):
                cache_copy(0, g).start()
                cache_copy(1, g).start()
        q = jnp.dot(rbuf[...], wqb[t], preferred_element_type=F32)
        for h in range(2):
            pieces[me, 2 * t + h] = round_bf16(rotate(q[:, h * 128:(h + 1) * 128]))
            publish(2 * t + h)
    for p in order:
        exchange(0, me, p, ynbr).wait_recv()
        exchange(2, across, p, partner).start()
    for p in order:
        exchange(1, me, p, partner).wait_recv()
        exchange(2, across, p, partner).wait_recv()
    for owner in range(4):
        for h in range(4):
            q_out[pl.ds((owner * 4 + h) * batch, batch), :] = pieces[owner, h]
        kv_out[owner % 2, owner // 2] = pieces[owner, 4]
    for p in order:
        exchange(0, me, p, ynbr).wait_send()
        exchange(1, me, p, partner).wait_send()
        exchange(2, across, p, partner).wait_send()
    for g in range(4):
        cache_copy(0, g).wait()
        cache_copy(1, g).wait()


def attention_kernel(
    pos, q_ref, kv_ref, kc, vc, ko, vo, acc_ref, stat_ref, kbuf, vbuf, mbuf, lbuf, osem,
):
    batch, rows, hd = kbuf.shape
    heads = acc_ref.shape[0] // batch
    groups = batch // 8
    me = lax.axis_index("sp")
    first = me * (rows // 2)

    def seqs(g):
        return pl.ds(pl.multiple_of(g * 8, 8), 8)

    def store(which, g):
        src, dst = ((kbuf, ko), (vbuf, vo))[which]
        return pltpu.make_async_copy(src.at[seqs(g)], dst.at[seqs(g)], osem.at[which, g])

    row_iota = lax.broadcasted_iota(jnp.int32, (16, hd), 0)
    col_iota = lax.broadcasted_iota(jnp.int32, (heads, rows), 1)
    head_iota = lax.broadcasted_iota(jnp.int32, (heads, rows), 0)
    col_head = lax.rem(col_iota, 2)
    col_pos = jnp.where(col_head == head_iota // (heads // 2), first + col_iota // 2, 1 << 20)

    def group(g, carry):
        for i in range(8):
            b = g * 8 + i
            slot = 2 * (pos[b] - first)
            inside = jnp.logical_and(slot >= 0, slot < rows)
            base = pl.multiple_of((jnp.clip(slot, 0, rows - 1) // 16) * 16, 16)
            target = jnp.where(inside, slot - base, -100)
            for buf, which in ((kbuf, 0), (vbuf, 1)):
                old = buf[b, pl.ds(base, 16), :].astype(F32)
                new0 = kv_ref[0, which, pl.ds(b, 1), :]
                new1 = kv_ref[1, which, pl.ds(b, 1), :]
                new = jnp.where(row_iota == target, new0, jnp.where(row_iota == target + 1, new1, old))
                buf[b, pl.ds(base, 16), :] = new.astype(BF16)
        scores = []
        for i in range(8):
            b = g * 8 + i
            q = q_ref[pl.ds(b, heads, stride=batch), :].astype(BF16)
            s = lax.dot_general(q, kbuf[b], (((1,), (1,)), ((), ())), preferred_element_type=F32) * (hd ** -0.5)
            scores.append(jnp.where(col_pos <= pos[b], s, NEG_BIG))
        for i in range(8):
            b = g * 8 + i
            s = scores[i]
            top = jnp.max(s, axis=-1, keepdims=True)
            weights = jnp.where(col_pos <= pos[b], jnp.exp(s - top), 0.0)
            total = jnp.sum(weights, axis=-1, keepdims=True)
            where = pl.ds(b, heads, stride=batch)
            acc_ref[where, :] = jnp.dot(weights.astype(BF16), vbuf[b], preferred_element_type=F32)
            mbuf[where, :] = jnp.broadcast_to(top, (heads, hd))
            lbuf[where, :] = jnp.broadcast_to(total, (heads, hd))
        store(0, g).start()
        store(1, g).start()
        return carry

    lax.fori_loop(0, groups, group, 0)
    lane = lax.broadcasted_iota(jnp.int32, (batch, hd), 1)
    packed = jnp.zeros((batch, hd), F32)
    for h in range(heads):
        packed = jnp.where(lane == h, mbuf[h * batch:(h + 1) * batch, :], packed)
        packed = jnp.where(lane == heads + h, lbuf[h * batch:(h + 1) * batch, :], packed)
    stat_ref[...] = packed
    for g in range(groups):
        store(0, g).wait()
        store(1, g).wait()


def output_kernel(
    acc, stat, hid, wo, out,
    hbuf, wob, obf, acc_p, acc_c, acc_y, o_own, o_land, st_p, st_c, st_y, part, land_a, land_b, tot,
    lsem, stsem, dsem, fsem, rsem, esem,
):
    z = lax.axis_index("tp")
    me = lax.axis_index("sp")
    core = lax.rem(me, 2)
    mate = me + 1 - 2 * core
    across = lax.rem(me + 2, 4)
    diagonal = across + 1 - 2 * core
    partner = {"sp": mate}
    ynbr = {"sp": across}
    outer = jnp.logical_or(z == 0, z == 3)
    inner = jnp.logical_not(outer)
    z_in = jnp.where(z == 0, 1, jnp.where(z == 1, 2, jnp.where(z == 2, 1, 2)))
    z_out = jnp.where(z == 1, 0, 3)
    heads, batch, hd = acc.shape
    mine = heads // 2
    tile = wob.shape[2]
    rows_b = batch // BLOCKS

    hcopy = pltpu.make_async_copy(hid, hbuf, lsem.at[TILES])

    def columns(quarter, t):
        return pl.ds(pl.multiple_of((quarter * TILES + t) * tile, tile), tile)

    def wcopy(t):
        return pltpu.make_async_copy(wo.at[:, columns(me, t)], wob.at[t], lsem.at[t])

    def repeat(low, high, body):
        def step(i, carry):
            body(i)
            return carry

        lax.fori_loop(low, high, step, 0)

    barrier = pltpu.get_barrier_semaphore()
    pl.semaphore_signal(barrier, inc=1, device_id=partner, device_id_type=MESH)
    pl.semaphore_signal(barrier, inc=1, device_id=ynbr, device_id_type=MESH)

    @pl.when(z > 0)
    def _():
        pl.semaphore_signal(barrier, inc=1, device_id={"tp": z - 1}, device_id_type=MESH)

    @pl.when(z < 3)
    def _():
        pl.semaphore_signal(barrier, inc=1, device_id={"tp": z + 1}, device_id_type=MESH)

    repeat(0, TILES, lambda t: wcopy(t).start())
    hcopy.start()

    @pl.when(outer)
    def _():
        pl.semaphore_signal(barrier, inc=1, device_id={"sp": across, "tp": z_in}, device_id_type=MESH)
        pl.semaphore_wait(barrier, 4)

    @pl.when(inner)
    def _():
        pl.semaphore_signal(barrier, inc=1, device_id={"sp": across, "tp": z_out}, device_id_type=MESH)
        pl.semaphore_wait(barrier, 5)

    def part_rows(s):
        return pl.ds(s * rows_b, rows_b)

    st_send = remote(stat, st_p, stsem.at[0], stsem.at[1], partner)
    st_send.start()
    p_send = []
    for s in range(BLOCKS):
        copy = remote(
            acc.at[pl.ds((1 - core) * mine, mine), part_rows(s)], acc_p.at[:, part_rows(s)],
            dsem.at[0, s], dsem.at[1, s], partner,
        )
        copy.start()
        p_send.append(copy)

    lane = lax.broadcasted_iota(jnp.int32, (batch, hd), 1)

    def merge(a, b):
        top = jnp.maximum(a, b)
        ea = jnp.exp(a - top)
        eb = jnp.exp(b - top)
        la = pltpu.roll(a, hd - heads, 1)
        lb = pltpu.roll(b, hd - heads, 1)
        return top, ea, eb, la * ea + lb * eb

    def own_heads(x):
        return jnp.where(core == 0, x, pltpu.roll(x, hd - mine, 1))

    st_send.wait_recv()
    top, ea, eb, total = merge(own_heads(stat[...]), own_heads(st_p[...]))
    st_c[...] = jnp.where(lane < heads, top, pltpu.roll(total, heads, 1))
    y_send = []
    sty_send = []
    for s in range(BLOCKS):
        p_send[s].wait_recv()
        sl = slice(s * rows_b, (s + 1) * rows_b)
        for h in range(mine):
            acc_c[h, sl, :] = acc[core * mine + h, sl, :] * ea[sl, h:h + 1] + acc_p[h, sl, :] * eb[sl, h:h + 1]
        copy = remote(st_c.at[part_rows(s)], st_y.at[part_rows(s)], stsem.at[2], stsem.at[3 + s], ynbr)
        copy.start()
        sty_send.append(copy)
        copy = remote(acc_c.at[:, part_rows(s)], acc_y.at[:, part_rows(s)], dsem.at[2, s], dsem.at[3, s], ynbr)
        copy.start()
        y_send.append(copy)
    o_send = []

    def send_a(j):
        return remote(part.at[j], land_a.at[j], fsem.at[0], rsem.at[0, j], {"tp": z_in})

    def send_b(j):
        return remote(part.at[j], land_b.at[j], fsem.at[1], rsem.at[1, j], {"tp": z_in})

    def send_c(j):
        return remote(tot.at[me, j], tot.at[me, j], fsem.at[2], rsem.at[2, j], {"tp": z_out})

    def send_d(j):
        return remote(tot.at[me, j], tot.at[me, j], fsem.at[3], rsem.at[3, j], ynbr)

    def send_e(j):
        return remote(tot.at[me, j], tot.at[me, j], fsem.at[4], esem.at[0, j // GROUP], partner)

    def send_f(j):
        return remote(tot.at[across, j], tot.at[across, j], fsem.at[5], esem.at[1, j // GROUP], partner)

    def project(j):
        rows = pl.ds(pl.multiple_of((j // TILES) * rows_b, rows_b), rows_b)
        part[j] = jnp.dot(obf[rows, :], wob[lax.rem(j, TILES)], preferred_element_type=F32)

    def values_send(s):
        sl = slice(s * rows_b, (s + 1) * rows_b)
        sty_send[s].wait_recv()
        _, ea, eb, total = merge(st_c[sl, :], st_y[sl, :])
        y_send[s].wait_recv()
        for h in range(mine):
            o = acc_c[h, sl, :] * ea[:, h:h + 1] + acc_y[h, sl, :] * eb[:, h:h + 1]
            o = round_bf16(o / total[:, h:h + 1])
            o_own[h, sl, :] = o
            obf[sl, pl.ds(pl.multiple_of((core * mine + h) * hd, hd), hd)] = o.astype(BF16)
        copy = remote(o_own.at[:, part_rows(s)], o_land.at[:, part_rows(s)], dsem.at[4, s], dsem.at[5, s], partner)
        copy.start()
        o_send.append(copy)

    def values_recv(s):
        sl = slice(s * rows_b, (s + 1) * rows_b)
        o_send[s].wait_recv()
        for h in range(mine):
            obf[sl, pl.ds(pl.multiple_of(((1 - core) * mine + h) * hd, hd), hd)] = o_land[h, sl, :].astype(BF16)

    def first_tiles(low, high):
        def tile_step(t):
            wcopy(t).wait()
            project(t)

            @pl.when(outer)
            def _():
                send_a(t).start()

        repeat(low, high, tile_step)

    def outer_tiles(low, high):
        @pl.when(outer)
        def _():
            def tile_step(j):
                project(j)
                send_a(j).start()

            repeat(low, high, tile_step)

    values_send(0)
    values_recv(0)
    for s in range(BLOCKS):
        tiles_of = first_tiles if s == 0 else outer_tiles
        middle = s * TILES + TILES // 2
        tiles_of(s * TILES, middle)
        if s < BLOCKS - 1:
            values_send(s + 1)
        tiles_of(middle, (s + 1) * TILES)
        if s < BLOCKS - 1:
            values_recv(s + 1)
    hcopy.wait()

    def emit(quarter, j):
        rows = pl.ds(pl.multiple_of((j // TILES) * rows_b, rows_b), rows_b)
        where = columns(quarter, lax.rem(j, TILES))
        out[rows, where] = (hbuf[rows, where].astype(F32) + tot[quarter, j]).astype(BF16)

    def send_x(j):
        return remote(tot.at[me, j], tot.at[me, j], fsem.at[6], rsem.at[3, j], {"sp": across, "tp": z_out})

    def share(j):
        send_e(j).start()
        emit(me, j)

    def collect(j):
        @pl.when(j >= 0)
        def _():
            send_d(j).wait_recv()
            send_f(j).start()
            emit(across, j)

    def gather(kind, owner, g):
        group = tot.at[owner, pl.ds(g * GROUP, GROUP)]
        remote(group, group, fsem.at[4 + kind], esem.at[kind, g], partner).wait_recv()
        repeat(g * GROUP, (g + 1) * GROUP, lambda j: emit(owner, j))

    groups = COUNT // GROUP

    def trickle(j, last):
        for g in range(groups):
            @pl.when(j == last - groups + g)
            def _(g=g):
                gather(0, mate, g)

    @pl.when(outer)
    def _():
        def step(j):
            @pl.when(j < COUNT)
            def _():
                send_c(j).wait_recv()

                @pl.when(j < COUNT - DIRECT)
                def _():
                    send_d(j).start()

                share(j)

            collect(j - LAG_Y)
            trickle(j, COUNT + LAG_Y)

        repeat(0, COUNT + LAG_Y, step)
        remote(part, land_a, fsem.at[0], rsem.at[0, 0], {"tp": z_in}).wait_send()
        sent = tot.at[me, pl.ds(0, COUNT - DIRECT)]
        remote(sent, sent, fsem.at[3], rsem.at[3, 0], ynbr).wait_send()

    @pl.when(inner)
    def _():
        def step(j):
            @pl.when(j < COUNT - TILES)
            def _():
                project(TILES + j)

            @pl.when(j < COUNT)
            def _():
                send_a(j).wait_recv()
                part[j] = part[j] + land_a[j]
                send_b(j).start()

            k = j - LAG_Z

            @pl.when(jnp.logical_and(k >= 0, k < COUNT))
            def _():
                send_b(k).wait_recv()
                tot[me, k] = part[k] + land_b[k]
                send_c(k).start()
                send_d(k).start()

                @pl.when(k >= COUNT - DIRECT)
                def _():
                    send_x(k).start()

                share(k)

            collect(k - LAG_Y)
            trickle(j, COUNT + LAG_Z + LAG_Y)

        repeat(0, COUNT + LAG_Z + LAG_Y, step)
        remote(part, land_b, fsem.at[1], rsem.at[1, 0], {"tp": z_in}).wait_send()
        remote(tot.at[me], tot.at[me], fsem.at[2], rsem.at[2, 0], {"tp": z_out}).wait_send()
        remote(tot.at[me], tot.at[me], fsem.at[3], rsem.at[3, 0], ynbr).wait_send()
        sent = tot.at[me, pl.ds(0, DIRECT)]
        remote(sent, sent, fsem.at[6], rsem.at[3, 0], ynbr).wait_send()

    for g in range(groups):
        gather(1, diagonal, g)
    st_send.wait_send()
    remote(st_c, st_y, stsem.at[2], stsem.at[3], ynbr).wait_send()
    for s in range(BLOCKS):
        p_send[s].wait_send()
        y_send[s].wait_send()
        o_send[s].wait_send()
    remote(tot.at[me], tot.at[me], fsem.at[4], esem.at[0, 0], partner).wait_send()
    remote(tot.at[across], tot.at[across], fsem.at[5], esem.at[1, 0], partner).wait_send()


def solution(mesh):
    vmem = pl.BlockSpec(memory_space=pltpu.VMEM)
    smem = pl.BlockSpec(memory_space=pltpu.SMEM)
    hbm = pl.BlockSpec(memory_space=pltpu.HBM)
    dma = pltpu.SemaphoreType.DMA

    def keep(x):
        return pltpu.with_memory_space_constraint(x, pltpu.VMEM)

    def stay(x):
        return pltpu.with_memory_space_constraint(x, pltpu.HBM)

    def params(mib, collective=None):
        if collective is None:
            return pltpu.CompilerParams(vmem_limit_bytes=mib * 2**20)
        return pltpu.CompilerParams(vmem_limit_bytes=mib * 2**20, collective_id=collective, has_side_effects=True)

    def local_step(hidden, norm_gain, w_query, w_key, w_value, w_out, k_cache, v_cache, positions):
        batch, seq_local, kv_local, hd = k_cache.shape
        d_model, q_cols = w_query.shape
        heads = q_cols // hd
        rows = seq_local * kv_local
        tiles = 2
        tcols = q_cols // 4 // tiles
        cache = (batch, rows, hd)
        acc_type = pltpu.VMEM((heads * batch, hd), F32)
        q, kv, k_in, v_in = pl.pallas_call(
            qkv_kernel,
            out_shape=(acc_type, pltpu.VMEM((2, 2, batch, hd), F32), pltpu.VMEM(cache, BF16), pltpu.VMEM(cache, BF16)),
            in_specs=[hbm] * 8,
            out_specs=(vmem,) * 4,
            scratch_shapes=[
                pltpu.SMEM((batch,), jnp.int32),
                pltpu.VMEM((batch, d_model), BF16),
                pltpu.VMEM((1, d_model), F32),
                pltpu.VMEM((batch, d_model), BF16),
                pltpu.VMEM((tiles, d_model, tcols), BF16),
                pltpu.VMEM((d_model, hd), BF16),
                pltpu.VMEM((4, 5, batch, hd), F32),
                dma((1,)),
                dma((3,)),
                dma((tiles,)),
                dma((2, 4)),
                dma((6, 5)),
            ],
            compiler_params=params(24, 0),
            name="qkv",
        )(
            stay(positions), stay(hidden), stay(norm_gain.reshape(1, d_model)), stay(w_query), stay(w_key), stay(w_value),
            stay(k_cache.reshape(cache)), stay(v_cache.reshape(cache)),
        )

        k_upd, v_upd, acc, stat, _, _ = pl.pallas_call(
            attention_kernel,
            out_shape=(
                jax.ShapeDtypeStruct(cache, BF16), jax.ShapeDtypeStruct(cache, BF16),
                acc_type, pltpu.VMEM((batch, hd), F32),
                pltpu.VMEM(cache, BF16), pltpu.VMEM(cache, BF16),
            ),
            in_specs=[smem, vmem, vmem, vmem, vmem],
            out_specs=(hbm, hbm, vmem, vmem, vmem, vmem),
            input_output_aliases={3: 4, 4: 5},
            scratch_shapes=[
                pltpu.VMEM((heads * batch, hd), F32),
                pltpu.VMEM((heads * batch, hd), F32),
                dma((2, batch // 8)),
            ],
            compiler_params=params(10),
            name="attention",
        )(positions, keep(q), keep(kv), keep(k_in), keep(v_in))

        mine = heads // 2
        ocols = d_model // 4 // TILES
        buf = pltpu.VMEM((mine, batch, hd), F32)
        st = pltpu.VMEM((batch, hd), F32)
        block = (batch // BLOCKS, ocols)
        chunk = pltpu.VMEM((COUNT,) + block, F32)
        out = pl.pallas_call(
            output_kernel,
            out_shape=pltpu.VMEM((batch, d_model), BF16),
            in_specs=[vmem, vmem, hbm, hbm],
            out_specs=vmem,
            scratch_shapes=[
                pltpu.VMEM((batch, d_model), BF16),
                pltpu.VMEM((TILES, q_cols, ocols), BF16),
                pltpu.VMEM((batch, q_cols), BF16),
                buf, buf, buf, buf, buf, st, st, st, chunk, chunk, chunk,
                pltpu.VMEM((4, COUNT) + block, F32),
                dma((TILES + 1,)),
                dma((3 + BLOCKS,)),
                dma((6, BLOCKS)),
                dma((7,)),
                dma((4, COUNT)),
                dma((2, COUNT // GROUP)),
            ],
            compiler_params=params(28, 1),
            name="output",
        )(keep(acc.reshape(heads, batch, hd)), keep(stat), stay(hidden), stay(w_out))
        return out, k_upd.reshape(k_cache.shape), v_upd.reshape(v_cache.shape)

    cache_spec = P("dp", "sp", "tp", None)
    specs_in = (P("dp", None), P(None), P(None, "tp"), P(None, "tp"), P(None, "tp"), P("tp", None), cache_spec, cache_spec, P("dp"))
    specs_out = (P("dp", None), cache_spec, cache_spec)
    return jax.shard_map(local_step, mesh=mesh, in_specs=specs_in, out_specs=specs_out, check_vma=False)
```

```python
import math

import jax
import jax.numpy as jnp
from jax import lax
from jax.experimental import pallas as pl
from jax.experimental.pallas import tpu as pltpu
from jax.sharding import PartitionSpec as P

ROPE_BASE = 1000000.0
EPS = 1e-5
NEG_BIG = float(jnp.finfo(jnp.float32).min)
MESH = pl.DeviceIdType.MESH
F32 = jnp.float32
BF16 = jnp.bfloat16
TILES = 8
HALVES = 2
COUNT = TILES * HALVES
NS = 4
LAG_Z = 5
LAG_Y = 5
DIRECT = 2
GROUP = 4


def remote(src, dst, send, recv, device):
    return pltpu.make_async_remote_copy(
        src_ref=src, dst_ref=dst, send_sem=send, recv_sem=recv, device_id=device, device_id_type=MESH
    )


def round_bf16(x):
    return x.astype(BF16).astype(F32)


def qkv_kernel(
    pos, hid, gain, wq, wk, wv, kc, vc, q_out, kv_out, kc_out, vc_out,
    pos_s, hbuf, gbuf, rbuf, wqb, wkvb, pieces, psem, hsem, wsem, csem, xsem,
):
    me = lax.axis_index("sp")
    core = lax.rem(me, 2)
    mate = me + 1 - 2 * core
    across = lax.rem(me + 2, 4)
    partner = {"sp": mate}
    ynbr = {"sp": across}
    batch, d_model = hid.shape
    tiles, _, cols = wqb.shape
    quarter = tiles * cols
    hcopy = pltpu.make_async_copy(hid, hbuf, hsem.at[0])
    gcopy = pltpu.make_async_copy(gain, gbuf, hsem.at[1])
    pcopy = pltpu.make_async_copy(pos, pos_s, psem.at[0])
    hcopy.start()
    gcopy.start()
    pcopy.start()
    head_cols = pl.ds(pl.multiple_of(core * 128, 128), 128)
    keys = me < 2

    @pl.when(keys)
    def _():
        pltpu.make_async_copy(wk.at[:, head_cols], wkvb, hsem.at[2]).start()

    @pl.when(jnp.logical_not(keys))
    def _():
        pltpu.make_async_copy(wv.at[:, head_cols], wkvb, hsem.at[2]).start()

    def wcopy(t):
        return pltpu.make_async_copy(
            wq.at[:, pl.ds(pl.multiple_of(me * quarter + t * cols, cols), cols)], wqb.at[t], wsem.at[t]
        )

    for t in range(tiles):
        wcopy(t).start()
    barrier = pltpu.get_barrier_semaphore()
    pl.semaphore_signal(barrier, inc=1, device_id=partner, device_id_type=MESH)
    pl.semaphore_signal(barrier, inc=1, device_id=ynbr, device_id_type=MESH)

    def cache_copy(which, g):
        src, dst = ((kc, kc_out), (vc, vc_out))[which]
        rows = pl.ds(g * (batch // 4), batch // 4)
        return pltpu.make_async_copy(src.at[rows], dst.at[rows], csem.at[which, g])

    pcopy.wait()
    lane = lax.broadcasted_iota(jnp.int32, (batch, 128), 1)
    row = lax.broadcasted_iota(jnp.int32, (batch, 128), 0)
    position = jnp.zeros((batch, 128), jnp.int32)
    for b in range(batch):
        position = jnp.where(row == b, pos_s[b], position)
    index = jnp.where(lane < 64, lane, lane - 64).astype(F32)
    angle = position.astype(F32) * jnp.exp(index * (-2.0 / 128 * math.log(ROPE_BASE)))
    cosf = jnp.cos(angle)
    sinf = jnp.where(lane < 64, -1.0, 1.0) * jnp.sin(angle)

    hcopy.wait()
    gcopy.wait()

    def norm_rows(i, carry):
        rows = pl.ds(pl.multiple_of(i * 16, 16), 16)
        x = hbuf[rows, :].astype(F32)
        scale = lax.rsqrt(jnp.sum(x * x, axis=-1, keepdims=True) * (1.0 / d_model) + EPS)
        rbuf[rows, :] = (x * scale * gbuf[...]).astype(BF16)
        return carry

    lax.fori_loop(0, batch // 16, norm_rows, 0)

    def rotate(x):
        return x * cosf + pltpu.roll(x, 64, 1) * sinf

    order = (4, 0, 1, 2, 3)

    def exchange(kind, owner, p, device):
        part = pieces.at[owner, p]
        return remote(part, part, xsem.at[2 * kind, p], xsem.at[2 * kind + 1, p], device)

    def publish(p):
        exchange(0, me, p, ynbr).start()
        exchange(1, me, p, partner).start()

    pltpu.make_async_copy(wk.at[:, head_cols], wkvb, hsem.at[2]).wait()
    kv = jnp.dot(rbuf[...], wkvb[...], preferred_element_type=F32)
    pieces[me, 4] = round_bf16(jnp.where(keys, rotate(kv), kv))
    pl.semaphore_wait(barrier, 2)
    publish(4)
    for t in range(tiles):
        wcopy(t).wait()
        if t == tiles - 1:
            for g in range(4):
                cache_copy(0, g).start()
                cache_copy(1, g).start()
        q = jnp.dot(rbuf[...], wqb[t], preferred_element_type=F32)
        for h in range(2):
            pieces[me, 2 * t + h] = round_bf16(rotate(q[:, h * 128:(h + 1) * 128]))
            publish(2 * t + h)
    for p in order:
        exchange(0, me, p, ynbr).wait_recv()
        exchange(2, across, p, partner).start()
    for p in order:
        exchange(1, me, p, partner).wait_recv()
        exchange(2, across, p, partner).wait_recv()
    for owner in range(4):
        for h in range(4):
            q_out[pl.ds((owner * 4 + h) * batch, batch), :] = pieces[owner, h]
        kv_out[owner % 2, owner // 2] = pieces[owner, 4]
    for p in order:
        exchange(0, me, p, ynbr).wait_send()
        exchange(1, me, p, partner).wait_send()
        exchange(2, across, p, partner).wait_send()
    for g in range(4):
        cache_copy(0, g).wait()
        cache_copy(1, g).wait()


def attention_kernel(
    pos, q_ref, kv_ref, kc, vc, ko, vo, acc_ref, stat_ref, kbuf, vbuf, mbuf, lbuf, osem,
):
    batch, rows, hd = kbuf.shape
    heads = acc_ref.shape[0] // batch
    groups = batch // 8
    me = lax.axis_index("sp")
    first = me * (rows // 2)

    def seqs(g):
        return pl.ds(pl.multiple_of(g * 8, 8), 8)

    def store(which, g):
        src, dst = ((kbuf, ko), (vbuf, vo))[which]
        return pltpu.make_async_copy(src.at[seqs(g)], dst.at[seqs(g)], osem.at[which, g])

    row_iota = lax.broadcasted_iota(jnp.int32, (16, hd), 0)
    col_iota = lax.broadcasted_iota(jnp.int32, (heads, rows), 1)
    head_iota = lax.broadcasted_iota(jnp.int32, (heads, rows), 0)
    col_head = lax.rem(col_iota, 2)
    col_pos = jnp.where(col_head == head_iota // (heads // 2), first + col_iota // 2, 1 << 20)

    def group(g, carry):
        for i in range(8):
            b = g * 8 + i
            slot = 2 * (pos[b] - first)
            inside = jnp.logical_and(slot >= 0, slot < rows)
            base = pl.multiple_of((jnp.clip(slot, 0, rows - 1) // 16) * 16, 16)
            target = jnp.where(inside, slot - base, -100)
            for buf, which in ((kbuf, 0), (vbuf, 1)):
                old = buf[b, pl.ds(base, 16), :].astype(F32)
                new0 = kv_ref[0, which, pl.ds(b, 1), :]
                new1 = kv_ref[1, which, pl.ds(b, 1), :]
                new = jnp.where(row_iota == target, new0, jnp.where(row_iota == target + 1, new1, old))
                buf[b, pl.ds(base, 16), :] = new.astype(BF16)
        scores = []
        for i in range(8):
            b = g * 8 + i
            q = q_ref[pl.ds(b, heads, stride=batch), :].astype(BF16)
            s = lax.dot_general(q, kbuf[b], (((1,), (1,)), ((), ())), preferred_element_type=F32) * (hd ** -0.5)
            scores.append(jnp.where(col_pos <= pos[b], s, NEG_BIG))
        for i in range(8):
            b = g * 8 + i
            s = scores[i]
            top = jnp.max(s, axis=-1, keepdims=True)
            weights = jnp.where(col_pos <= pos[b], jnp.exp(s - top), 0.0)
            total = jnp.sum(weights, axis=-1, keepdims=True)
            where = pl.ds(b, heads, stride=batch)
            acc_ref[where, :] = jnp.dot(weights.astype(BF16), vbuf[b], preferred_element_type=F32)
            mbuf[where, :] = jnp.broadcast_to(top, (heads, hd))
            lbuf[where, :] = jnp.broadcast_to(total, (heads, hd))
        store(0, g).start()
        store(1, g).start()
        return carry

    lax.fori_loop(0, groups, group, 0)
    lane = lax.broadcasted_iota(jnp.int32, (batch, hd), 1)
    packed = jnp.zeros((batch, hd), F32)
    for h in range(heads):
        packed = jnp.where(lane == h, mbuf[h * batch:(h + 1) * batch, :], packed)
        packed = jnp.where(lane == heads + h, lbuf[h * batch:(h + 1) * batch, :], packed)
    stat_ref[...] = packed
    for g in range(groups):
        store(0, g).wait()
        store(1, g).wait()


def output_kernel(
    acc, stat, hid, wo, out,
    hbuf, wob, obf, acc_p, acc_c, acc_y, o_own, o_land, st_p, st_c, st_y, part, land_a, land_b, tot,
    lsem, stsem, dsem, fsem, rsem, esem,
):
    z = lax.axis_index("tp")
    me = lax.axis_index("sp")
    core = lax.rem(me, 2)
    mate = me + 1 - 2 * core
    across = lax.rem(me + 2, 4)
    diagonal = across + 1 - 2 * core
    partner = {"sp": mate}
    ynbr = {"sp": across}
    outer = jnp.logical_or(z == 0, z == 3)
    inner = jnp.logical_not(outer)
    z_in = jnp.where(z == 0, 1, jnp.where(z == 1, 2, jnp.where(z == 2, 1, 2)))
    z_out = jnp.where(z == 1, 0, 3)
    heads, batch, hd = acc.shape
    mine = heads // 2
    tile = wob.shape[2]
    rows_s = batch // NS
    rows_h = batch // HALVES

    hcopy = pltpu.make_async_copy(hid, hbuf, lsem.at[TILES])

    def columns(quarter, t):
        return pl.ds(pl.multiple_of((quarter * TILES + t) * tile, tile), tile)

    def wcopy(t):
        return pltpu.make_async_copy(wo.at[:, columns(me, t)], wob.at[t], lsem.at[t])

    def repeat(low, high, body):
        def step(i, carry):
            body(i)
            return carry

        lax.fori_loop(low, high, step, 0)

    barrier = pltpu.get_barrier_semaphore()
    pl.semaphore_signal(barrier, inc=1, device_id=partner, device_id_type=MESH)
    pl.semaphore_signal(barrier, inc=1, device_id=ynbr, device_id_type=MESH)

    @pl.when(z > 0)
    def _():
        pl.semaphore_signal(barrier, inc=1, device_id={"tp": z - 1}, device_id_type=MESH)

    @pl.when(z < 3)
    def _():
        pl.semaphore_signal(barrier, inc=1, device_id={"tp": z + 1}, device_id_type=MESH)

    repeat(0, TILES, lambda t: wcopy(t).start())
    hcopy.start()

    @pl.when(outer)
    def _():
        pl.semaphore_signal(barrier, inc=1, device_id={"sp": across, "tp": z_in}, device_id_type=MESH)
        pl.semaphore_wait(barrier, 4)

    @pl.when(inner)
    def _():
        pl.semaphore_signal(barrier, inc=1, device_id={"sp": across, "tp": z_out}, device_id_type=MESH)
        pl.semaphore_wait(barrier, 5)

    def part_rows(s):
        return pl.ds(s * rows_s, rows_s)

    st_send = remote(stat, st_p, stsem.at[0], stsem.at[1], partner)
    st_send.start()
    p_send = []
    for s in range(NS):
        copy = remote(
            acc.at[pl.ds((1 - core) * mine, mine), part_rows(s)], acc_p.at[:, part_rows(s)],
            dsem.at[0, s], dsem.at[1, s], partner,
        )
        copy.start()
        p_send.append(copy)

    lane = lax.broadcasted_iota(jnp.int32, (batch, hd), 1)

    def merge(a, b):
        top = jnp.maximum(a, b)
        ea = jnp.exp(a - top)
        eb = jnp.exp(b - top)
        la = pltpu.roll(a, hd - heads, 1)
        lb = pltpu.roll(b, hd - heads, 1)
        return top, ea, eb, la * ea + lb * eb

    def own_heads(x):
        return jnp.where(core == 0, x, pltpu.roll(x, hd - mine, 1))

    st_send.wait_recv()
    top, ea, eb, total = merge(own_heads(stat[...]), own_heads(st_p[...]))
    st_c[...] = jnp.where(lane < heads, top, pltpu.roll(total, heads, 1))
    y_send = []
    sty_send = []
    for s in range(NS):
        p_send[s].wait_recv()
        sl = slice(s * rows_s, (s + 1) * rows_s)
        for h in range(mine):
            acc_c[h, sl, :] = acc[core * mine + h, sl, :] * ea[sl, h:h + 1] + acc_p[h, sl, :] * eb[sl, h:h + 1]
        copy = remote(st_c.at[part_rows(s)], st_y.at[part_rows(s)], stsem.at[2], stsem.at[3 + s], ynbr)
        copy.start()
        sty_send.append(copy)
        copy = remote(acc_c.at[:, part_rows(s)], acc_y.at[:, part_rows(s)], dsem.at[2, s], dsem.at[3, s], ynbr)
        copy.start()
        y_send.append(copy)
    o_send = []

    def send_a(j):
        return remote(part.at[j], land_a.at[j], fsem.at[0], rsem.at[0, j], {"tp": z_in})

    def send_b(j):
        return remote(part.at[j], land_b.at[j], fsem.at[1], rsem.at[1, j], {"tp": z_in})

    def send_c(j):
        return remote(tot.at[me, j], tot.at[me, j], fsem.at[2], rsem.at[2, j], {"tp": z_out})

    def send_d(j):
        return remote(tot.at[me, j], tot.at[me, j], fsem.at[3], rsem.at[3, j], ynbr)

    def send_e(j):
        return remote(tot.at[me, j], tot.at[me, j], fsem.at[4], esem.at[0, j // GROUP], partner)

    def send_f(j):
        return remote(tot.at[across, j], tot.at[across, j], fsem.at[5], esem.at[1, j // GROUP], partner)

    def project(j):
        half = j // TILES
        rows = pl.ds(pl.multiple_of(half * rows_h, rows_h), rows_h)
        part[j] = jnp.dot(obf[rows, :], wob[j - half * TILES], preferred_element_type=F32)

    def values_send(s):
        sl = slice(s * rows_s, (s + 1) * rows_s)
        sty_send[s].wait_recv()
        _, ea, eb, total = merge(st_c[sl, :], st_y[sl, :])
        y_send[s].wait_recv()
        for h in range(mine):
            o = acc_c[h, sl, :] * ea[:, h:h + 1] + acc_y[h, sl, :] * eb[:, h:h + 1]
            o = round_bf16(o / total[:, h:h + 1])
            o_own[h, sl, :] = o
            obf[sl, pl.ds(pl.multiple_of((core * mine + h) * hd, hd), hd)] = o.astype(BF16)
        copy = remote(o_own.at[:, part_rows(s)], o_land.at[:, part_rows(s)], dsem.at[4, s], dsem.at[5, s], partner)
        copy.start()
        o_send.append(copy)

    def values_recv(s):
        sl = slice(s * rows_s, (s + 1) * rows_s)
        o_send[s].wait_recv()
        for h in range(mine):
            obf[sl, pl.ds(pl.multiple_of(((1 - core) * mine + h) * hd, hd), hd)] = o_land[h, sl, :].astype(BF16)

    def first_tiles(low, high):
        def tile_step(t):
            wcopy(t).wait()
            project(t)

            @pl.when(outer)
            def _():
                send_a(t).start()

        repeat(low, high, tile_step)

    values_send(0)
    values_send(1)
    values_recv(0)
    values_recv(1)
    first_tiles(0, TILES // 4)
    values_send(2)
    first_tiles(TILES // 4, 3 * TILES // 4)
    values_send(3)
    first_tiles(3 * TILES // 4, TILES)
    values_recv(2)
    values_recv(3)
    hcopy.wait()

    def emit(quarter, j):
        half = j // TILES
        rows = pl.ds(pl.multiple_of(half * rows_h, rows_h), rows_h)
        where = columns(quarter, j - half * TILES)
        out[rows, where] = (hbuf[rows, where].astype(F32) + tot[quarter, j]).astype(BF16)

    def send_x(j):
        return remote(tot.at[me, j], tot.at[me, j], fsem.at[6], rsem.at[3, j], {"sp": across, "tp": z_out})

    def share(j):
        send_e(j).start()
        emit(me, j)

    def collect(j):
        @pl.when(j >= 0)
        def _():
            send_d(j).wait_recv()
            send_f(j).start()
            emit(across, j)

    def gather(kind, owner, g):
        group = tot.at[owner, pl.ds(g * GROUP, GROUP)]
        remote(group, group, fsem.at[4 + kind], esem.at[kind, g], partner).wait_recv()
        repeat(g * GROUP, (g + 1) * GROUP, lambda j: emit(owner, j))

    groups = COUNT // GROUP

    def trickle(j, last):
        for g in range(groups):
            @pl.when(j == last - groups + g)
            def _(g=g):
                gather(0, mate, g)

    @pl.when(outer)
    def _():
        def second_half(j):
            project(j)
            send_a(j).start()

        repeat(TILES, COUNT, second_half)

        def step(j):
            @pl.when(j < COUNT)
            def _():
                send_c(j).wait_recv()

                @pl.when(j < COUNT - DIRECT)
                def _():
                    send_d(j).start()

                share(j)

            collect(j - LAG_Y)
            trickle(j, COUNT + LAG_Y)

        repeat(0, COUNT + LAG_Y, step)
        remote(part, land_a, fsem.at[0], rsem.at[0, 0], {"tp": z_in}).wait_send()
        sent = tot.at[me, pl.ds(0, COUNT - DIRECT)]
        remote(sent, sent, fsem.at[3], rsem.at[3, 0], ynbr).wait_send()

    @pl.when(inner)
    def _():
        def step(j):
            @pl.when(j < TILES)
            def _():
                project(TILES + j)

            @pl.when(j < COUNT)
            def _():
                send_a(j).wait_recv()
                part[j] = part[j] + land_a[j]
                send_b(j).start()

            k = j - LAG_Z

            @pl.when(jnp.logical_and(k >= 0, k < COUNT))
            def _():
                send_b(k).wait_recv()
                tot[me, k] = part[k] + land_b[k]
                send_c(k).start()
                send_d(k).start()

                @pl.when(k >= COUNT - DIRECT)
                def _():
                    send_x(k).start()

                share(k)

            collect(k - LAG_Y)
            trickle(j, COUNT + LAG_Z + LAG_Y)

        repeat(0, COUNT + LAG_Z + LAG_Y, step)
        remote(part, land_b, fsem.at[1], rsem.at[1, 0], {"tp": z_in}).wait_send()
        remote(tot.at[me], tot.at[me], fsem.at[2], rsem.at[2, 0], {"tp": z_out}).wait_send()
        remote(tot.at[me], tot.at[me], fsem.at[3], rsem.at[3, 0], ynbr).wait_send()
        sent = tot.at[me, pl.ds(0, DIRECT)]
        remote(sent, sent, fsem.at[6], rsem.at[3, 0], ynbr).wait_send()

    for g in range(groups):
        gather(1, diagonal, g)
    st_send.wait_send()
    remote(st_c, st_y, stsem.at[2], stsem.at[3], ynbr).wait_send()
    for s in range(NS):
        p_send[s].wait_send()
        y_send[s].wait_send()
        o_send[s].wait_send()
    remote(tot.at[me], tot.at[me], fsem.at[4], esem.at[0, 0], partner).wait_send()
    remote(tot.at[across], tot.at[across], fsem.at[5], esem.at[1, 0], partner).wait_send()


def solution(mesh):
    vmem = pl.BlockSpec(memory_space=pltpu.VMEM)
    smem = pl.BlockSpec(memory_space=pltpu.SMEM)
    hbm = pl.BlockSpec(memory_space=pltpu.HBM)
    dma = pltpu.SemaphoreType.DMA

    def keep(x):
        return pltpu.with_memory_space_constraint(x, pltpu.VMEM)

    def stay(x):
        return pltpu.with_memory_space_constraint(x, pltpu.HBM)

    def params(mib, collective=None):
        if collective is None:
            return pltpu.CompilerParams(vmem_limit_bytes=mib * 2**20)
        return pltpu.CompilerParams(vmem_limit_bytes=mib * 2**20, collective_id=collective, has_side_effects=True)

    def local_step(hidden, norm_gain, w_query, w_key, w_value, w_out, k_cache, v_cache, positions):
        batch, seq_local, kv_local, hd = k_cache.shape
        d_model, q_cols = w_query.shape
        heads = q_cols // hd
        rows = seq_local * kv_local
        tiles = 2
        tcols = q_cols // 4 // tiles
        cache = (batch, rows, hd)
        acc_type = pltpu.VMEM((heads * batch, hd), F32)
        q, kv, k_in, v_in = pl.pallas_call(
            qkv_kernel,
            out_shape=(acc_type, pltpu.VMEM((2, 2, batch, hd), F32), pltpu.VMEM(cache, BF16), pltpu.VMEM(cache, BF16)),
            in_specs=[hbm] * 8,
            out_specs=(vmem,) * 4,
            scratch_shapes=[
                pltpu.SMEM((batch,), jnp.int32),
                pltpu.VMEM((batch, d_model), BF16),
                pltpu.VMEM((1, d_model), F32),
                pltpu.VMEM((batch, d_model), BF16),
                pltpu.VMEM((tiles, d_model, tcols), BF16),
                pltpu.VMEM((d_model, hd), BF16),
                pltpu.VMEM((4, 5, batch, hd), F32),
                dma((1,)),
                dma((3,)),
                dma((tiles,)),
                dma((2, 4)),
                dma((6, 5)),
            ],
            compiler_params=params(24, 0),
            name="qkv",
        )(
            stay(positions), stay(hidden), stay(norm_gain.reshape(1, d_model)), stay(w_query), stay(w_key), stay(w_value),
            stay(k_cache.reshape(cache)), stay(v_cache.reshape(cache)),
        )

        k_upd, v_upd, acc, stat, _, _ = pl.pallas_call(
            attention_kernel,
            out_shape=(
                jax.ShapeDtypeStruct(cache, BF16), jax.ShapeDtypeStruct(cache, BF16),
                acc_type, pltpu.VMEM((batch, hd), F32),
                pltpu.VMEM(cache, BF16), pltpu.VMEM(cache, BF16),
            ),
            in_specs=[smem, vmem, vmem, vmem, vmem],
            out_specs=(hbm, hbm, vmem, vmem, vmem, vmem),
            input_output_aliases={3: 4, 4: 5},
            scratch_shapes=[
                pltpu.VMEM((heads * batch, hd), F32),
                pltpu.VMEM((heads * batch, hd), F32),
                dma((2, batch // 8)),
            ],
            compiler_params=params(10),
            name="attention",
        )(positions, keep(q), keep(kv), keep(k_in), keep(v_in))

        mine = heads // 2
        ocols = d_model // 4 // TILES
        buf = pltpu.VMEM((mine, batch, hd), F32)
        st = pltpu.VMEM((batch, hd), F32)
        block = (batch // HALVES, ocols)
        chunk = pltpu.VMEM((COUNT,) + block, F32)
        out = pl.pallas_call(
            output_kernel,
            out_shape=pltpu.VMEM((batch, d_model), BF16),
            in_specs=[vmem, vmem, hbm, hbm],
            out_specs=vmem,
            scratch_shapes=[
                pltpu.VMEM((batch, d_model), BF16),
                pltpu.VMEM((TILES, q_cols, ocols), BF16),
                pltpu.VMEM((batch, q_cols), BF16),
                buf, buf, buf, buf, buf, st, st, st, chunk, chunk, chunk,
                pltpu.VMEM((4, COUNT) + block, F32),
                dma((TILES + 1,)),
                dma((3 + NS,)),
                dma((6, NS)),
                dma((7,)),
                dma((4, COUNT)),
                dma((2, COUNT // GROUP)),
            ],
            compiler_params=params(28, 1),
            name="output",
        )(keep(acc.reshape(heads, batch, hd)), keep(stat), stay(hidden), stay(w_out))
        return out, k_upd.reshape(k_cache.shape), v_upd.reshape(v_cache.shape)

    cache_spec = P("dp", "sp", "tp", None)
    specs_in = (P("dp", None), P(None), P(None, "tp"), P(None, "tp"), P(None, "tp"), P("tp", None), cache_spec, cache_spec, P("dp"))
    specs_out = (P("dp", None), cache_spec, cache_spec)
    return jax.shard_map(local_step, mesh=mesh, in_specs=specs_in, out_specs=specs_out, check_vma=False)
```

```python
import math

import jax
import jax.numpy as jnp
from jax import lax
from jax.experimental import pallas as pl
from jax.experimental.pallas import tpu as pltpu
from jax.sharding import PartitionSpec as P

ROPE_BASE = 1000000.0
EPS = 1e-5
NEG_BIG = float(jnp.finfo(jnp.float32).min)
MESH = pl.DeviceIdType.MESH
F32 = jnp.float32
BF16 = jnp.bfloat16
TILES = 8
HALVES = 2
COUNT = TILES * HALVES
NS = 4
LAG_Z = 5
LAG_Y = 5
DIRECT = 1
GROUP = 4


def remote(src, dst, send, recv, device):
    return pltpu.make_async_remote_copy(
        src_ref=src, dst_ref=dst, send_sem=send, recv_sem=recv, device_id=device, device_id_type=MESH
    )


def round_bf16(x):
    return x.astype(BF16).astype(F32)


def qkv_kernel(
    pos, hid, gain, wq, wk, wv, kc, vc, q_out, kv_out, kc_out, vc_out,
    pos_s, hbuf, gbuf, rbuf, wqb, wkvb, pieces, psem, hsem, wsem, csem, xsem,
):
    me = lax.axis_index("sp")
    core = lax.rem(me, 2)
    mate = me + 1 - 2 * core
    across = lax.rem(me + 2, 4)
    partner = {"sp": mate}
    ynbr = {"sp": across}
    batch, d_model = hid.shape
    tiles, _, cols = wqb.shape
    quarter = tiles * cols
    hcopy = pltpu.make_async_copy(hid, hbuf, hsem.at[0])
    gcopy = pltpu.make_async_copy(gain, gbuf, hsem.at[1])
    pcopy = pltpu.make_async_copy(pos, pos_s, psem.at[0])
    hcopy.start()
    gcopy.start()
    pcopy.start()
    head_cols = pl.ds(pl.multiple_of(core * 128, 128), 128)
    keys = me < 2

    @pl.when(keys)
    def _():
        pltpu.make_async_copy(wk.at[:, head_cols], wkvb, hsem.at[2]).start()

    @pl.when(jnp.logical_not(keys))
    def _():
        pltpu.make_async_copy(wv.at[:, head_cols], wkvb, hsem.at[2]).start()

    def wcopy(t):
        return pltpu.make_async_copy(
            wq.at[:, pl.ds(pl.multiple_of(me * quarter + t * cols, cols), cols)], wqb.at[t], wsem.at[t]
        )

    for t in range(tiles):
        wcopy(t).start()
    barrier = pltpu.get_barrier_semaphore()
    pl.semaphore_signal(barrier, inc=1, device_id=partner, device_id_type=MESH)
    pl.semaphore_signal(barrier, inc=1, device_id=ynbr, device_id_type=MESH)

    def cache_copy(which, g):
        src, dst = ((kc, kc_out), (vc, vc_out))[which]
        rows = pl.ds(g * (batch // 4), batch // 4)
        return pltpu.make_async_copy(src.at[rows], dst.at[rows], csem.at[which, g])

    pcopy.wait()
    lane = lax.broadcasted_iota(jnp.int32, (batch, 128), 1)
    row = lax.broadcasted_iota(jnp.int32, (batch, 128), 0)
    position = jnp.zeros((batch, 128), jnp.int32)
    for b in range(batch):
        position = jnp.where(row == b, pos_s[b], position)
    index = jnp.where(lane < 64, lane, lane - 64).astype(F32)
    angle = position.astype(F32) * jnp.exp(index * (-2.0 / 128 * math.log(ROPE_BASE)))
    cosf = jnp.cos(angle)
    sinf = jnp.where(lane < 64, -1.0, 1.0) * jnp.sin(angle)

    hcopy.wait()
    gcopy.wait()

    def norm_rows(i, carry):
        rows = pl.ds(pl.multiple_of(i * 16, 16), 16)
        x = hbuf[rows, :].astype(F32)
        scale = lax.rsqrt(jnp.sum(x * x, axis=-1, keepdims=True) * (1.0 / d_model) + EPS)
        rbuf[rows, :] = (x * scale * gbuf[...]).astype(BF16)
        return carry

    lax.fori_loop(0, batch // 16, norm_rows, 0)

    def rotate(x):
        return x * cosf + pltpu.roll(x, 64, 1) * sinf

    order = (4, 0, 1, 2, 3)

    def exchange(kind, owner, p, device):
        part = pieces.at[owner, p]
        return remote(part, part, xsem.at[2 * kind, p], xsem.at[2 * kind + 1, p], device)

    def publish(p):
        exchange(0, me, p, ynbr).start()
        exchange(1, me, p, partner).start()

    pltpu.make_async_copy(wk.at[:, head_cols], wkvb, hsem.at[2]).wait()
    kv = jnp.dot(rbuf[...], wkvb[...], preferred_element_type=F32)
    pieces[me, 4] = round_bf16(jnp.where(keys, rotate(kv), kv))
    pl.semaphore_wait(barrier, 2)
    publish(4)
    for t in range(tiles):
        wcopy(t).wait()
        if t == tiles // 2:
            for g in range(4):
                cache_copy(0, g).start()
                cache_copy(1, g).start()
        q = jnp.dot(rbuf[...], wqb[t], preferred_element_type=F32)
        pieces[me, t] = round_bf16(rotate(q))
        publish(t)
    for p in order:
        exchange(0, me, p, ynbr).wait_recv()
        exchange(2, across, p, partner).start()
    for p in order:
        exchange(1, me, p, partner).wait_recv()
        exchange(2, across, p, partner).wait_recv()
    for owner in range(4):
        for h in range(4):
            q_out[pl.ds((owner * 4 + h) * batch, batch), :] = pieces[owner, h]
        kv_out[owner % 2, owner // 2] = pieces[owner, 4]
    for p in order:
        exchange(0, me, p, ynbr).wait_send()
        exchange(1, me, p, partner).wait_send()
        exchange(2, across, p, partner).wait_send()
    for g in range(4):
        cache_copy(0, g).wait()
        cache_copy(1, g).wait()


def attention_kernel(
    pos, q_ref, kv_ref, kc, vc, ko, vo, acc_ref, stat_ref, kbuf, vbuf, mbuf, lbuf, osem,
):
    batch, rows, hd = kbuf.shape
    heads = acc_ref.shape[0] // batch
    groups = batch // 8
    me = lax.axis_index("sp")
    first = me * (rows // 2)

    def seqs(g):
        return pl.ds(pl.multiple_of(g * 8, 8), 8)

    def store(which, g):
        src, dst = ((kbuf, ko), (vbuf, vo))[which]
        return pltpu.make_async_copy(src.at[seqs(g)], dst.at[seqs(g)], osem.at[which, g])

    row_iota = lax.broadcasted_iota(jnp.int32, (16, hd), 0)
    col_iota = lax.broadcasted_iota(jnp.int32, (heads, rows), 1)
    head_iota = lax.broadcasted_iota(jnp.int32, (heads, rows), 0)
    col_head = lax.rem(col_iota, 2)
    col_pos = jnp.where(col_head == head_iota // (heads // 2), first + col_iota // 2, 1 << 20)

    def group(g, carry):
        for i in range(8):
            b = g * 8 + i
            slot = 2 * (pos[b] - first)
            inside = jnp.logical_and(slot >= 0, slot < rows)
            base = pl.multiple_of((jnp.clip(slot, 0, rows - 1) // 16) * 16, 16)
            target = jnp.where(inside, slot - base, -100)
            for buf, which in ((kbuf, 0), (vbuf, 1)):
                old = buf[b, pl.ds(base, 16), :].astype(F32)
                new0 = kv_ref[0, which, pl.ds(b, 1), :]
                new1 = kv_ref[1, which, pl.ds(b, 1), :]
                new = jnp.where(row_iota == target, new0, jnp.where(row_iota == target + 1, new1, old))
                buf[b, pl.ds(base, 16), :] = new.astype(BF16)
        scores = []
        for i in range(8):
            b = g * 8 + i
            q = q_ref[pl.ds(b, heads, stride=batch), :].astype(BF16)
            s = lax.dot_general(q, kbuf[b], (((1,), (1,)), ((), ())), preferred_element_type=F32) * (hd ** -0.5)
            scores.append(jnp.where(col_pos <= pos[b], s, NEG_BIG))
        for i in range(8):
            b = g * 8 + i
            s = scores[i]
            top = jnp.max(s, axis=-1, keepdims=True)
            weights = jnp.where(col_pos <= pos[b], jnp.exp(s - top), 0.0)
            total = jnp.sum(weights, axis=-1, keepdims=True)
            where = pl.ds(b, heads, stride=batch)
            acc_ref[where, :] = jnp.dot(weights.astype(BF16), vbuf[b], preferred_element_type=F32)
            mbuf[where, :] = jnp.broadcast_to(top, (heads, hd))
            lbuf[where, :] = jnp.broadcast_to(total, (heads, hd))
        store(0, g).start()
        store(1, g).start()
        return carry

    lax.fori_loop(0, groups, group, 0)
    lane = lax.broadcasted_iota(jnp.int32, (batch, hd), 1)
    packed = jnp.zeros((batch, hd), F32)
    for h in range(heads):
        packed = jnp.where(lane == h, mbuf[h * batch:(h + 1) * batch, :], packed)
        packed = jnp.where(lane == heads + h, lbuf[h * batch:(h + 1) * batch, :], packed)
    stat_ref[...] = packed
    for g in range(groups):
        store(0, g).wait()
        store(1, g).wait()


def output_kernel(
    acc, stat, hid, wo, out,
    hbuf, wob, obf, acc_p, acc_c, acc_y, o_own, o_land, st_p, st_c, st_y, part, land_a, land_b, tot,
    lsem, stsem, dsem, fsem, rsem, esem,
):
    z = lax.axis_index("tp")
    me = lax.axis_index("sp")
    core = lax.rem(me, 2)
    mate = me + 1 - 2 * core
    across = lax.rem(me + 2, 4)
    diagonal = across + 1 - 2 * core
    partner = {"sp": mate}
    ynbr = {"sp": across}
    outer = jnp.logical_or(z == 0, z == 3)
    inner = jnp.logical_not(outer)
    z_in = jnp.where(z == 0, 1, jnp.where(z == 1, 2, jnp.where(z == 2, 1, 2)))
    z_out = jnp.where(z == 1, 0, 3)
    heads, batch, hd = acc.shape
    mine = heads // 2
    tile = wob.shape[2]
    rows_s = batch // NS
    rows_h = batch // HALVES

    hcopy = pltpu.make_async_copy(hid, hbuf, lsem.at[TILES])

    def columns(quarter, t):
        return pl.ds(pl.multiple_of((quarter * TILES + t) * tile, tile), tile)

    def wcopy(t):
        return pltpu.make_async_copy(wo.at[:, columns(me, t)], wob.at[t], lsem.at[t])

    def repeat(low, high, body):
        def step(i, carry):
            body(i)
            return carry

        lax.fori_loop(low, high, step, 0)

    barrier = pltpu.get_barrier_semaphore()
    pl.semaphore_signal(barrier, inc=1, device_id=partner, device_id_type=MESH)
    pl.semaphore_signal(barrier, inc=1, device_id=ynbr, device_id_type=MESH)

    @pl.when(z > 0)
    def _():
        pl.semaphore_signal(barrier, inc=1, device_id={"tp": z - 1}, device_id_type=MESH)

    @pl.when(z < 3)
    def _():
        pl.semaphore_signal(barrier, inc=1, device_id={"tp": z + 1}, device_id_type=MESH)

    repeat(0, TILES, lambda t: wcopy(t).start())
    hcopy.start()

    @pl.when(outer)
    def _():
        pl.semaphore_signal(barrier, inc=1, device_id={"sp": across, "tp": z_in}, device_id_type=MESH)
        pl.semaphore_wait(barrier, 4)

    @pl.when(inner)
    def _():
        pl.semaphore_signal(barrier, inc=1, device_id={"sp": across, "tp": z_out}, device_id_type=MESH)
        pl.semaphore_wait(barrier, 5)

    def part_rows(s):
        return pl.ds(s * rows_s, rows_s)

    st_send = remote(stat, st_p, stsem.at[0], stsem.at[1], partner)
    st_send.start()
    p_send = []
    for s in range(NS):
        copy = remote(
            acc.at[pl.ds((1 - core) * mine, mine), part_rows(s)], acc_p.at[:, part_rows(s)],
            dsem.at[0, s], dsem.at[1, s], partner,
        )
        copy.start()
        p_send.append(copy)

    lane = lax.broadcasted_iota(jnp.int32, (batch, hd), 1)

    def merge(a, b):
        top = jnp.maximum(a, b)
        ea = jnp.exp(a - top)
        eb = jnp.exp(b - top)
        la = pltpu.roll(a, hd - heads, 1)
        lb = pltpu.roll(b, hd - heads, 1)
        return top, ea, eb, la * ea + lb * eb

    def own_heads(x):
        return jnp.where(core == 0, x, pltpu.roll(x, hd - mine, 1))

    st_send.wait_recv()
    top, ea, eb, total = merge(own_heads(stat[...]), own_heads(st_p[...]))
    st_c[...] = jnp.where(lane < heads, top, pltpu.roll(total, heads, 1))
    y_send = []
    sty_send = []
    for s in range(NS):
        p_send[s].wait_recv()
        sl = slice(s * rows_s, (s + 1) * rows_s)
        for h in range(mine):
            acc_c[h, sl, :] = acc[core * mine + h, sl, :] * ea[sl, h:h + 1] + acc_p[h, sl, :] * eb[sl, h:h + 1]
        copy = remote(st_c.at[part_rows(s)], st_y.at[part_rows(s)], stsem.at[2], stsem.at[3 + s], ynbr)
        copy.start()
        sty_send.append(copy)
        copy = remote(acc_c.at[:, part_rows(s)], acc_y.at[:, part_rows(s)], dsem.at[2, s], dsem.at[3, s], ynbr)
        copy.start()
        y_send.append(copy)
    o_send = []

    def send_a(j):
        return remote(part.at[j], land_a.at[j], fsem.at[0], rsem.at[0, j], {"tp": z_in})

    def send_b(j):
        return remote(part.at[j], land_b.at[j], fsem.at[1], rsem.at[1, j], {"tp": z_in})

    def send_c(j):
        return remote(tot.at[me, j], tot.at[me, j], fsem.at[2], rsem.at[2, j], {"tp": z_out})

    def send_d(j):
        return remote(tot.at[me, j], tot.at[me, j], fsem.at[3], rsem.at[3, j], ynbr)

    def send_e(j):
        return remote(tot.at[me, j], tot.at[me, j], fsem.at[4], esem.at[0, j // GROUP], partner)

    def send_f(j):
        return remote(tot.at[across, j], tot.at[across, j], fsem.at[5], esem.at[1, j // GROUP], partner)

    def project(j):
        half = j // TILES
        rows = pl.ds(pl.multiple_of(half * rows_h, rows_h), rows_h)
        part[j] = jnp.dot(obf[rows, :], wob[j - half * TILES], preferred_element_type=F32)

    def values_send(s):
        sl = slice(s * rows_s, (s + 1) * rows_s)
        sty_send[s].wait_recv()
        _, ea, eb, total = merge(st_c[sl, :], st_y[sl, :])
        y_send[s].wait_recv()
        for h in range(mine):
            o = acc_c[h, sl, :] * ea[:, h:h + 1] + acc_y[h, sl, :] * eb[:, h:h + 1]
            o = round_bf16(o / total[:, h:h + 1])
            o_own[h, sl, :] = o
            obf[sl, pl.ds(pl.multiple_of((core * mine + h) * hd, hd), hd)] = o.astype(BF16)
        copy = remote(o_own.at[:, part_rows(s)], o_land.at[:, part_rows(s)], dsem.at[4, s], dsem.at[5, s], partner)
        copy.start()
        o_send.append(copy)

    def values_recv(s):
        sl = slice(s * rows_s, (s + 1) * rows_s)
        o_send[s].wait_recv()
        for h in range(mine):
            obf[sl, pl.ds(pl.multiple_of(((1 - core) * mine + h) * hd, hd), hd)] = o_land[h, sl, :].astype(BF16)

    def first_tiles(low, high):
        def tile_step(t):
            wcopy(t).wait()
            project(t)

            @pl.when(outer)
            def _():
                send_a(t).start()

        repeat(low, high, tile_step)

    values_send(0)
    values_send(1)
    values_recv(0)
    values_recv(1)
    first_tiles(0, TILES // 4)
    values_send(2)
    first_tiles(TILES // 4, 3 * TILES // 4)
    values_send(3)
    first_tiles(3 * TILES // 4, TILES)
    values_recv(2)
    values_recv(3)
    hcopy.wait()

    def emit(quarter, j):
        half = j // TILES
        rows = pl.ds(pl.multiple_of(half * rows_h, rows_h), rows_h)
        where = columns(quarter, j - half * TILES)
        out[rows, where] = (hbuf[rows, where].astype(F32) + tot[quarter, j]).astype(BF16)

    def send_x(j):
        return remote(tot.at[me, j], tot.at[me, j], fsem.at[6], rsem.at[3, j], {"sp": across, "tp": z_out})

    def share(j):
        send_e(j).start()
        emit(me, j)

    def collect(j):
        @pl.when(j >= 0)
        def _():
            send_d(j).wait_recv()
            send_f(j).start()
            emit(across, j)

    def gather(kind, owner, g):
        group = tot.at[owner, pl.ds(g * GROUP, GROUP)]
        remote(group, group, fsem.at[4 + kind], esem.at[kind, g], partner).wait_recv()
        repeat(g * GROUP, (g + 1) * GROUP, lambda j: emit(owner, j))

    groups = COUNT // GROUP

    def trickle(j, last):
        for g in range(groups):
            @pl.when(j == last - groups + g)
            def _(g=g):
                gather(0, mate, g)

    @pl.when(outer)
    def _():
        def second_half(j):
            project(j)
            send_a(j).start()

        repeat(TILES, COUNT, second_half)

        def step(j):
            @pl.when(j < COUNT)
            def _():
                send_c(j).wait_recv()

                @pl.when(j < COUNT - DIRECT)
                def _():
                    send_d(j).start()

                share(j)

            collect(j - LAG_Y)
            trickle(j, COUNT + LAG_Y)

        repeat(0, COUNT + LAG_Y, step)
        remote(part, land_a, fsem.at[0], rsem.at[0, 0], {"tp": z_in}).wait_send()
        sent = tot.at[me, pl.ds(0, COUNT - DIRECT)]
        remote(sent, sent, fsem.at[3], rsem.at[3, 0], ynbr).wait_send()

    @pl.when(inner)
    def _():
        def step(j):
            @pl.when(j < TILES)
            def _():
                project(TILES + j)

            @pl.when(j < COUNT)
            def _():
                send_a(j).wait_recv()
                part[j] = part[j] + land_a[j]
                send_b(j).start()

            k = j - LAG_Z

            @pl.when(jnp.logical_and(k >= 0, k < COUNT))
            def _():
                send_b(k).wait_recv()
                tot[me, k] = part[k] + land_b[k]
                send_c(k).start()
                send_d(k).start()

                @pl.when(k >= COUNT - DIRECT)
                def _():
                    send_x(k).start()

                share(k)

            collect(k - LAG_Y)
            trickle(j, COUNT + LAG_Z + LAG_Y)

        repeat(0, COUNT + LAG_Z + LAG_Y, step)
        remote(part, land_b, fsem.at[1], rsem.at[1, 0], {"tp": z_in}).wait_send()
        remote(tot.at[me], tot.at[me], fsem.at[2], rsem.at[2, 0], {"tp": z_out}).wait_send()
        remote(tot.at[me], tot.at[me], fsem.at[3], rsem.at[3, 0], ynbr).wait_send()
        sent = tot.at[me, pl.ds(0, DIRECT)]
        remote(sent, sent, fsem.at[6], rsem.at[3, 0], ynbr).wait_send()

    for g in range(groups):
        gather(1, diagonal, g)
    st_send.wait_send()
    remote(st_c, st_y, stsem.at[2], stsem.at[3], ynbr).wait_send()
    for s in range(NS):
        p_send[s].wait_send()
        y_send[s].wait_send()
        o_send[s].wait_send()
    remote(tot.at[me], tot.at[me], fsem.at[4], esem.at[0, 0], partner).wait_send()
    remote(tot.at[across], tot.at[across], fsem.at[5], esem.at[1, 0], partner).wait_send()


def solution(mesh):
    vmem = pl.BlockSpec(memory_space=pltpu.VMEM)
    smem = pl.BlockSpec(memory_space=pltpu.SMEM)
    hbm = pl.BlockSpec(memory_space=pltpu.HBM)
    dma = pltpu.SemaphoreType.DMA

    def keep(x):
        return pltpu.with_memory_space_constraint(x, pltpu.VMEM)

    def stay(x):
        return pltpu.with_memory_space_constraint(x, pltpu.HBM)

    def params(mib, collective=None):
        if collective is None:
            return pltpu.CompilerParams(vmem_limit_bytes=mib * 2**20)
        return pltpu.CompilerParams(vmem_limit_bytes=mib * 2**20, collective_id=collective, has_side_effects=True)

    def local_step(hidden, norm_gain, w_query, w_key, w_value, w_out, k_cache, v_cache, positions):
        batch, seq_local, kv_local, hd = k_cache.shape
        d_model, q_cols = w_query.shape
        heads = q_cols // hd
        rows = seq_local * kv_local
        tiles = 4
        tcols = q_cols // 4 // tiles
        cache = (batch, rows, hd)
        acc_type = pltpu.VMEM((heads * batch, hd), F32)
        q, kv, k_in, v_in = pl.pallas_call(
            qkv_kernel,
            out_shape=(acc_type, pltpu.VMEM((2, 2, batch, hd), F32), pltpu.VMEM(cache, BF16), pltpu.VMEM(cache, BF16)),
            in_specs=[hbm] * 8,
            out_specs=(vmem,) * 4,
            scratch_shapes=[
                pltpu.SMEM((batch,), jnp.int32),
                pltpu.VMEM((batch, d_model), BF16),
                pltpu.VMEM((1, d_model), F32),
                pltpu.VMEM((batch, d_model), BF16),
                pltpu.VMEM((tiles, d_model, tcols), BF16),
                pltpu.VMEM((d_model, hd), BF16),
                pltpu.VMEM((4, 5, batch, hd), F32),
                dma((1,)),
                dma((3,)),
                dma((tiles,)),
                dma((2, 4)),
                dma((6, 5)),
            ],
            compiler_params=params(24, 0),
            name="qkv",
        )(
            stay(positions), stay(hidden), stay(norm_gain.reshape(1, d_model)), stay(w_query), stay(w_key), stay(w_value),
            stay(k_cache.reshape(cache)), stay(v_cache.reshape(cache)),
        )

        k_upd, v_upd, acc, stat, _, _ = pl.pallas_call(
            attention_kernel,
            out_shape=(
                jax.ShapeDtypeStruct(cache, BF16), jax.ShapeDtypeStruct(cache, BF16),
                acc_type, pltpu.VMEM((batch, hd), F32),
                pltpu.VMEM(cache, BF16), pltpu.VMEM(cache, BF16),
            ),
            in_specs=[smem, vmem, vmem, vmem, vmem],
            out_specs=(hbm, hbm, vmem, vmem, vmem, vmem),
            input_output_aliases={3: 4, 4: 5},
            scratch_shapes=[
                pltpu.VMEM((heads * batch, hd), F32),
                pltpu.VMEM((heads * batch, hd), F32),
                dma((2, batch // 8)),
            ],
            compiler_params=params(10),
            name="attention",
        )(positions, keep(q), keep(kv), keep(k_in), keep(v_in))

        mine = heads // 2
        ocols = d_model // 4 // TILES
        buf = pltpu.VMEM((mine, batch, hd), F32)
        st = pltpu.VMEM((batch, hd), F32)
        block = (batch // HALVES, ocols)
        chunk = pltpu.VMEM((COUNT,) + block, F32)
        out = pl.pallas_call(
            output_kernel,
            out_shape=pltpu.VMEM((batch, d_model), BF16),
            in_specs=[vmem, vmem, hbm, hbm],
            out_specs=vmem,
            scratch_shapes=[
                pltpu.VMEM((batch, d_model), BF16),
                pltpu.VMEM((TILES, q_cols, ocols), BF16),
                pltpu.VMEM((batch, q_cols), BF16),
                buf, buf, buf, buf, buf, st, st, st, chunk, chunk, chunk,
                pltpu.VMEM((4, COUNT) + block, F32),
                dma((TILES + 1,)),
                dma((3 + NS,)),
                dma((6, NS)),
                dma((7,)),
                dma((4, COUNT)),
                dma((2, COUNT // GROUP)),
            ],
            compiler_params=params(28, 1),
            name="output",
        )(keep(acc.reshape(heads, batch, hd)), keep(stat), stay(hidden), stay(w_out))
        return out, k_upd.reshape(k_cache.shape), v_upd.reshape(v_cache.shape)

    cache_spec = P("dp", "sp", "tp", None)
    specs_in = (P("dp", None), P(None), P(None, "tp"), P(None, "tp"), P(None, "tp"), P("tp", None), cache_spec, cache_spec, P("dp"))
    specs_out = (P("dp", None), cache_spec, cache_spec)
    return jax.shard_map(local_step, mesh=mesh, in_specs=specs_in, out_specs=specs_out, check_vma=False)
```

```python
import math

import jax
import jax.numpy as jnp
from jax import lax
from jax.experimental import pallas as pl
from jax.experimental.pallas import tpu as pltpu
from jax.sharding import PartitionSpec as P

ROPE_BASE = 1000000.0
EPS = 1e-5
NEG_BIG = float(jnp.finfo(jnp.float32).min)
MESH = pl.DeviceIdType.MESH
F32 = jnp.float32
BF16 = jnp.bfloat16
TILES = 8
HALVES = 2
COUNT = TILES * HALVES
NS = 4
LAG_Z = 5
LAG_Y = 5
GROUP = 4


def remote(src, dst, send, recv, device):
    return pltpu.make_async_remote_copy(
        src_ref=src, dst_ref=dst, send_sem=send, recv_sem=recv, device_id=device, device_id_type=MESH
    )


def round_bf16(x):
    return x.astype(BF16).astype(F32)


def qkv_kernel(
    pos, hid, gain, wq, wk, wv, kc, vc, q_out, kv_out, kc_out, vc_out,
    pos_s, hbuf, gbuf, rbuf, wqb, wkvb, pieces, psem, hsem, wsem, csem, xsem,
):
    me = lax.axis_index("sp")
    core = lax.rem(me, 2)
    mate = me + 1 - 2 * core
    across = lax.rem(me + 2, 4)
    partner = {"sp": mate}
    ynbr = {"sp": across}
    batch, d_model = hid.shape
    tiles, _, cols = wqb.shape
    quarter = tiles * cols
    hcopy = pltpu.make_async_copy(hid, hbuf, hsem.at[0])
    gcopy = pltpu.make_async_copy(gain, gbuf, hsem.at[1])
    pcopy = pltpu.make_async_copy(pos, pos_s, psem.at[0])
    hcopy.start()
    gcopy.start()
    pcopy.start()
    head_cols = pl.ds(pl.multiple_of(core * 128, 128), 128)
    keys = me < 2

    @pl.when(keys)
    def _():
        pltpu.make_async_copy(wk.at[:, head_cols], wkvb, hsem.at[2]).start()

    @pl.when(jnp.logical_not(keys))
    def _():
        pltpu.make_async_copy(wv.at[:, head_cols], wkvb, hsem.at[2]).start()

    def wcopy(t):
        return pltpu.make_async_copy(
            wq.at[:, pl.ds(pl.multiple_of(me * quarter + t * cols, cols), cols)], wqb.at[t], wsem.at[t]
        )

    for t in range(tiles):
        wcopy(t).start()
    barrier = pltpu.get_barrier_semaphore()
    pl.semaphore_signal(barrier, inc=1, device_id=partner, device_id_type=MESH)
    pl.semaphore_signal(barrier, inc=1, device_id=ynbr, device_id_type=MESH)

    def cache_copy(which, g):
        src, dst = ((kc, kc_out), (vc, vc_out))[which]
        rows = pl.ds(g * (batch // 4), batch // 4)
        return pltpu.make_async_copy(src.at[rows], dst.at[rows], csem.at[which, g])

    pcopy.wait()
    lane = lax.broadcasted_iota(jnp.int32, (batch, 128), 1)
    row = lax.broadcasted_iota(jnp.int32, (batch, 128), 0)
    position = jnp.zeros((batch, 128), jnp.int32)
    for b in range(batch):
        position = jnp.where(row == b, pos_s[b], position)
    index = jnp.where(lane < 64, lane, lane - 64).astype(F32)
    angle = position.astype(F32) * jnp.exp(index * (-2.0 / 128 * math.log(ROPE_BASE)))
    cosf = jnp.cos(angle)
    sinf = jnp.where(lane < 64, -1.0, 1.0) * jnp.sin(angle)

    hcopy.wait()
    gcopy.wait()

    def norm_rows(i, carry):
        rows = pl.ds(pl.multiple_of(i * 16, 16), 16)
        x = hbuf[rows, :].astype(F32)
        scale = lax.rsqrt(jnp.sum(x * x, axis=-1, keepdims=True) * (1.0 / d_model) + EPS)
        rbuf[rows, :] = (x * scale * gbuf[...]).astype(BF16)
        return carry

    lax.fori_loop(0, batch // 16, norm_rows, 0)

    def rotate(x):
        return x * cosf + pltpu.roll(x, 64, 1) * sinf

    order = (4, 0, 1, 2, 3)

    def exchange(kind, owner, p, device):
        part = pieces.at[owner, p]
        return remote(part, part, xsem.at[2 * kind, p], xsem.at[2 * kind + 1, p], device)

    def publish(p):
        exchange(0, me, p, ynbr).start()
        exchange(1, me, p, partner).start()

    pltpu.make_async_copy(wk.at[:, head_cols], wkvb, hsem.at[2]).wait()
    kv = jnp.dot(rbuf[...], wkvb[...], preferred_element_type=F32)
    pieces[me, 4] = round_bf16(jnp.where(keys, rotate(kv), kv))
    pl.semaphore_wait(barrier, 2)
    publish(4)
    for t in range(tiles):
        wcopy(t).wait()
        if t == tiles - 1:
            for g in range(4):
                cache_copy(0, g).start()
                cache_copy(1, g).start()
        q = jnp.dot(rbuf[...], wqb[t], preferred_element_type=F32)
        for h in range(2):
            pieces[me, 2 * t + h] = round_bf16(rotate(q[:, h * 128:(h + 1) * 128]))
            publish(2 * t + h)
    for p in order:
        exchange(0, me, p, ynbr).wait_recv()
        exchange(2, across, p, partner).start()
    for p in order:
        exchange(1, me, p, partner).wait_recv()
        exchange(2, across, p, partner).wait_recv()
    for owner in range(4):
        for h in range(4):
            q_out[pl.ds((owner * 4 + h) * batch, batch), :] = pieces[owner, h]
        kv_out[owner % 2, owner // 2] = pieces[owner, 4]
    for p in order:
        exchange(0, me, p, ynbr).wait_send()
        exchange(1, me, p, partner).wait_send()
        exchange(2, across, p, partner).wait_send()
    for g in range(4):
        cache_copy(0, g).wait()
        cache_copy(1, g).wait()


def attention_kernel(
    pos, q_ref, kv_ref, kc, vc, ko, vo, acc_ref, stat_ref, kbuf, vbuf, mbuf, lbuf, osem,
):
    batch, rows, hd = kbuf.shape
    heads = acc_ref.shape[0] // batch
    groups = batch // 8
    me = lax.axis_index("sp")
    first = me * (rows // 2)

    def seqs(g):
        return pl.ds(pl.multiple_of(g * 8, 8), 8)

    def store(which, g):
        src, dst = ((kbuf, ko), (vbuf, vo))[which]
        return pltpu.make_async_copy(src.at[seqs(g)], dst.at[seqs(g)], osem.at[which, g])

    row_iota = lax.broadcasted_iota(jnp.int32, (16, hd), 0)
    col_iota = lax.broadcasted_iota(jnp.int32, (heads, rows), 1)
    head_iota = lax.broadcasted_iota(jnp.int32, (heads, rows), 0)
    col_head = lax.rem(col_iota, 2)
    col_pos = jnp.where(col_head == head_iota // (heads // 2), first + col_iota // 2, 1 << 20)

    def group(g, carry):
        for i in range(8):
            b = g * 8 + i
            slot = 2 * (pos[b] - first)
            inside = jnp.logical_and(slot >= 0, slot < rows)
            base = pl.multiple_of((jnp.clip(slot, 0, rows - 1) // 16) * 16, 16)
            target = jnp.where(inside, slot - base, -100)
            for buf, which in ((kbuf, 0), (vbuf, 1)):
                old = buf[b, pl.ds(base, 16), :].astype(F32)
                new0 = kv_ref[0, which, pl.ds(b, 1), :]
                new1 = kv_ref[1, which, pl.ds(b, 1), :]
                new = jnp.where(row_iota == target, new0, jnp.where(row_iota == target + 1, new1, old))
                buf[b, pl.ds(base, 16), :] = new.astype(BF16)
        scores = []
        for i in range(8):
            b = g * 8 + i
            q = q_ref[pl.ds(b, heads, stride=batch), :].astype(BF16)
            s = lax.dot_general(q, kbuf[b], (((1,), (1,)), ((), ())), preferred_element_type=F32) * (hd ** -0.5)
            scores.append(jnp.where(col_pos <= pos[b], s, NEG_BIG))
        for i in range(8):
            b = g * 8 + i
            s = scores[i]
            top = jnp.max(s, axis=-1, keepdims=True)
            weights = jnp.where(col_pos <= pos[b], jnp.exp(s - top), 0.0)
            total = jnp.sum(weights, axis=-1, keepdims=True)
            where = pl.ds(b, heads, stride=batch)
            acc_ref[where, :] = jnp.dot(weights.astype(BF16), vbuf[b], preferred_element_type=F32)
            mbuf[where, :] = jnp.broadcast_to(top, (heads, hd))
            lbuf[where, :] = jnp.broadcast_to(total, (heads, hd))
        store(0, g).start()
        store(1, g).start()
        return carry

    lax.fori_loop(0, groups, group, 0)
    lane = lax.broadcasted_iota(jnp.int32, (batch, hd), 1)
    packed = jnp.zeros((batch, hd), F32)
    for h in range(heads):
        packed = jnp.where(lane == h, mbuf[h * batch:(h + 1) * batch, :], packed)
        packed = jnp.where(lane == heads + h, lbuf[h * batch:(h + 1) * batch, :], packed)
    stat_ref[...] = packed
    for g in range(groups):
        store(0, g).wait()
        store(1, g).wait()


def output_kernel(
    acc, stat, hid, wo, out,
    hbuf, wob, obf, acc_p, acc_c, acc_y, o_own, o_land, st_p, st_c, st_y, part, land_a, land_b, tot,
    lsem, stsem, dsem, fsem, rsem, esem,
):
    z = lax.axis_index("tp")
    me = lax.axis_index("sp")
    core = lax.rem(me, 2)
    mate = me + 1 - 2 * core
    across = lax.rem(me + 2, 4)
    diagonal = across + 1 - 2 * core
    partner = {"sp": mate}
    ynbr = {"sp": across}
    outer = jnp.logical_or(z == 0, z == 3)
    inner = jnp.logical_not(outer)
    z_in = jnp.where(z == 0, 1, jnp.where(z == 1, 2, jnp.where(z == 2, 1, 2)))
    z_out = jnp.where(z == 1, 0, 3)
    heads, batch, hd = acc.shape
    mine = heads // 2
    tile = wob.shape[2]
    rows_s = batch // NS
    rows_h = batch // HALVES

    hcopy = pltpu.make_async_copy(hid, hbuf, lsem.at[TILES])

    def columns(quarter, t):
        return pl.ds(pl.multiple_of((quarter * TILES + t) * tile, tile), tile)

    def wcopy(t):
        return pltpu.make_async_copy(wo.at[:, columns(me, t)], wob.at[t], lsem.at[t])

    def repeat(low, high, body):
        def step(i, carry):
            body(i)
            return carry

        lax.fori_loop(low, high, step, 0)

    barrier = pltpu.get_barrier_semaphore()
    pl.semaphore_signal(barrier, inc=1, device_id=partner, device_id_type=MESH)
    pl.semaphore_signal(barrier, inc=1, device_id=ynbr, device_id_type=MESH)

    @pl.when(z > 0)
    def _():
        pl.semaphore_signal(barrier, inc=1, device_id={"tp": z - 1}, device_id_type=MESH)

    @pl.when(z < 3)
    def _():
        pl.semaphore_signal(barrier, inc=1, device_id={"tp": z + 1}, device_id_type=MESH)

    repeat(0, TILES, lambda t: wcopy(t).start())
    hcopy.start()

    @pl.when(outer)
    def _():
        pl.semaphore_wait(barrier, 3)

    @pl.when(inner)
    def _():
        pl.semaphore_wait(barrier, 4)

    def part_rows(s):
        return pl.ds(s * rows_s, rows_s)

    st_send = remote(stat, st_p, stsem.at[0], stsem.at[1], partner)
    st_send.start()
    p_send = []
    for s in range(NS):
        copy = remote(
            acc.at[pl.ds((1 - core) * mine, mine), part_rows(s)], acc_p.at[:, part_rows(s)],
            dsem.at[0, s], dsem.at[1, s], partner,
        )
        copy.start()
        p_send.append(copy)

    lane = lax.broadcasted_iota(jnp.int32, (batch, hd), 1)

    def merge(a, b):
        top = jnp.maximum(a, b)
        ea = jnp.exp(a - top)
        eb = jnp.exp(b - top)
        la = pltpu.roll(a, hd - heads, 1)
        lb = pltpu.roll(b, hd - heads, 1)
        return top, ea, eb, la * ea + lb * eb

    def own_heads(x):
        return jnp.where(core == 0, x, pltpu.roll(x, hd - mine, 1))

    st_send.wait_recv()
    top, ea, eb, total = merge(own_heads(stat[...]), own_heads(st_p[...]))
    st_c[...] = jnp.where(lane < heads, top, pltpu.roll(total, heads, 1))
    y_send = []
    sty_send = []
    for s in range(NS):
        p_send[s].wait_recv()
        sl = slice(s * rows_s, (s + 1) * rows_s)
        for h in range(mine):
            acc_c[h, sl, :] = acc[core * mine + h, sl, :] * ea[sl, h:h + 1] + acc_p[h, sl, :] * eb[sl, h:h + 1]
        copy = remote(st_c.at[part_rows(s)], st_y.at[part_rows(s)], stsem.at[2], stsem.at[3 + s], ynbr)
        copy.start()
        sty_send.append(copy)
        copy = remote(acc_c.at[:, part_rows(s)], acc_y.at[:, part_rows(s)], dsem.at[2, s], dsem.at[3, s], ynbr)
        copy.start()
        y_send.append(copy)
    o_send = []

    def send_a(j):
        return remote(part.at[j], land_a.at[j], fsem.at[0], rsem.at[0, j], {"tp": z_in})

    def send_b(j):
        return remote(part.at[j], land_b.at[j], fsem.at[1], rsem.at[1, j], {"tp": z_in})

    def send_c(j):
        return remote(tot.at[me, j], tot.at[me, j], fsem.at[2], rsem.at[2, j], {"tp": z_out})

    def send_d(j):
        return remote(tot.at[me, j], tot.at[me, j], fsem.at[3], rsem.at[3, j], ynbr)

    def send_e(j):
        return remote(tot.at[me, j], tot.at[me, j], fsem.at[4], esem.at[0, j // GROUP], partner)

    def send_f(j):
        return remote(tot.at[across, j], tot.at[across, j], fsem.at[5], esem.at[1, j // GROUP], partner)

    def project(j):
        half = j // TILES
        rows = pl.ds(pl.multiple_of(half * rows_h, rows_h), rows_h)
        part[j] = jnp.dot(obf[rows, :], wob[j - half * TILES], preferred_element_type=F32)

    def values_send(s):
        sl = slice(s * rows_s, (s + 1) * rows_s)
        sty_send[s].wait_recv()
        _, ea, eb, total = merge(st_c[sl, :], st_y[sl, :])
        y_send[s].wait_recv()
        for h in range(mine):
            o = acc_c[h, sl, :] * ea[:, h:h + 1] + acc_y[h, sl, :] * eb[:, h:h + 1]
            o = round_bf16(o / total[:, h:h + 1])
            o_own[h, sl, :] = o
            obf[sl, pl.ds(pl.multiple_of((core * mine + h) * hd, hd), hd)] = o.astype(BF16)
        copy = remote(o_own.at[:, part_rows(s)], o_land.at[:, part_rows(s)], dsem.at[4, s], dsem.at[5, s], partner)
        copy.start()
        o_send.append(copy)

    def values_recv(s):
        sl = slice(s * rows_s, (s + 1) * rows_s)
        o_send[s].wait_recv()
        for h in range(mine):
            obf[sl, pl.ds(pl.multiple_of(((1 - core) * mine + h) * hd, hd), hd)] = o_land[h, sl, :].astype(BF16)

    def first_tiles(low, high):
        def tile_step(t):
            wcopy(t).wait()
            project(t)

            @pl.when(outer)
            def _():
                send_a(t).start()

        repeat(low, high, tile_step)

    values_send(0)
    values_send(1)
    values_recv(0)
    values_recv(1)
    first_tiles(0, TILES // 4)
    values_send(2)
    first_tiles(TILES // 4, 3 * TILES // 4)
    values_send(3)
    first_tiles(3 * TILES // 4, TILES)
    values_recv(2)
    values_recv(3)
    hcopy.wait()

    def emit(quarter, j):
        half = j // TILES
        rows = pl.ds(pl.multiple_of(half * rows_h, rows_h), rows_h)
        where = columns(quarter, j - half * TILES)
        out[rows, where] = (hbuf[rows, where].astype(F32) + tot[quarter, j]).astype(BF16)

    def share(j):
        send_d(j).start()
        send_e(j).start()
        emit(me, j)

    def collect(j):
        @pl.when(j >= 0)
        def _():
            send_d(j).wait_recv()
            send_f(j).start()
            emit(across, j)

    def gather(kind, owner, g):
        group = tot.at[owner, pl.ds(g * GROUP, GROUP)]
        remote(group, group, fsem.at[4 + kind], esem.at[kind, g], partner).wait_recv()
        repeat(g * GROUP, (g + 1) * GROUP, lambda j: emit(owner, j))

    groups = COUNT // GROUP

    def trickle(j, last):
        for g in range(groups):
            @pl.when(j == last - groups + g)
            def _(g=g):
                gather(0, mate, g)

    @pl.when(outer)
    def _():
        def second_half(j):
            project(j)
            send_a(j).start()

        repeat(TILES, COUNT, second_half)

        def step(j):
            @pl.when(j < COUNT)
            def _():
                send_c(j).wait_recv()
                share(j)

            collect(j - LAG_Y)
            trickle(j, COUNT + LAG_Y)

        repeat(0, COUNT + LAG_Y, step)
        remote(part, land_a, fsem.at[0], rsem.at[0, 0], {"tp": z_in}).wait_send()

    @pl.when(inner)
    def _():
        def step(j):
            @pl.when(j < TILES)
            def _():
                project(TILES + j)

            @pl.when(j < COUNT)
            def _():
                send_a(j).wait_recv()
                part[j] = part[j] + land_a[j]
                send_b(j).start()

            k = j - LAG_Z

            @pl.when(jnp.logical_and(k >= 0, k < COUNT))
            def _():
                send_b(k).wait_recv()
                tot[me, k] = part[k] + land_b[k]
                send_c(k).start()
                share(k)

            collect(k - LAG_Y)
            trickle(j, COUNT + LAG_Z + LAG_Y)

        repeat(0, COUNT + LAG_Z + LAG_Y, step)
        remote(part, land_b, fsem.at[1], rsem.at[1, 0], {"tp": z_in}).wait_send()
        remote(tot.at[me], tot.at[me], fsem.at[2], rsem.at[2, 0], {"tp": z_out}).wait_send()

    for g in range(groups):
        gather(1, diagonal, g)
    st_send.wait_send()
    remote(st_c, st_y, stsem.at[2], stsem.at[3], ynbr).wait_send()
    for s in range(NS):
        p_send[s].wait_send()
        y_send[s].wait_send()
        o_send[s].wait_send()
    remote(tot.at[me], tot.at[me], fsem.at[3], rsem.at[3, 0], ynbr).wait_send()
    remote(tot.at[me], tot.at[me], fsem.at[4], esem.at[0, 0], partner).wait_send()
    remote(tot.at[across], tot.at[across], fsem.at[5], esem.at[1, 0], partner).wait_send()


def solution(mesh):
    vmem = pl.BlockSpec(memory_space=pltpu.VMEM)
    smem = pl.BlockSpec(memory_space=pltpu.SMEM)
    hbm = pl.BlockSpec(memory_space=pltpu.HBM)
    dma = pltpu.SemaphoreType.DMA

    def keep(x):
        return pltpu.with_memory_space_constraint(x, pltpu.VMEM)

    def stay(x):
        return pltpu.with_memory_space_constraint(x, pltpu.HBM)

    def params(mib, collective=None):
        if collective is None:
            return pltpu.CompilerParams(vmem_limit_bytes=mib * 2**20)
        return pltpu.CompilerParams(vmem_limit_bytes=mib * 2**20, collective_id=collective, has_side_effects=True)

    def local_step(hidden, norm_gain, w_query, w_key, w_value, w_out, k_cache, v_cache, positions):
        batch, seq_local, kv_local, hd = k_cache.shape
        d_model, q_cols = w_query.shape
        heads = q_cols // hd
        rows = seq_local * kv_local
        tiles = 2
        tcols = q_cols // 4 // tiles
        cache = (batch, rows, hd)
        acc_type = pltpu.VMEM((heads * batch, hd), F32)
        q, kv, k_in, v_in = pl.pallas_call(
            qkv_kernel,
            out_shape=(acc_type, pltpu.VMEM((2, 2, batch, hd), F32), pltpu.VMEM(cache, BF16), pltpu.VMEM(cache, BF16)),
            in_specs=[hbm] * 8,
            out_specs=(vmem,) * 4,
            scratch_shapes=[
                pltpu.SMEM((batch,), jnp.int32),
                pltpu.VMEM((batch, d_model), BF16),
                pltpu.VMEM((1, d_model), F32),
                pltpu.VMEM((batch, d_model), BF16),
                pltpu.VMEM((tiles, d_model, tcols), BF16),
                pltpu.VMEM((d_model, hd), BF16),
                pltpu.VMEM((4, 5, batch, hd), F32),
                dma((1,)),
                dma((3,)),
                dma((tiles,)),
                dma((2, 4)),
                dma((6, 5)),
            ],
            compiler_params=params(24, 0),
            name="qkv",
        )(
            stay(positions), stay(hidden), stay(norm_gain.reshape(1, d_model)), stay(w_query), stay(w_key), stay(w_value),
            stay(k_cache.reshape(cache)), stay(v_cache.reshape(cache)),
        )

        k_upd, v_upd, acc, stat, _, _ = pl.pallas_call(
            attention_kernel,
            out_shape=(
                jax.ShapeDtypeStruct(cache, BF16), jax.ShapeDtypeStruct(cache, BF16),
                acc_type, pltpu.VMEM((batch, hd), F32),
                pltpu.VMEM(cache, BF16), pltpu.VMEM(cache, BF16),
            ),
            in_specs=[smem, vmem, vmem, vmem, vmem],
            out_specs=(hbm, hbm, vmem, vmem, vmem, vmem),
            input_output_aliases={3: 4, 4: 5},
            scratch_shapes=[
                pltpu.VMEM((heads * batch, hd), F32),
                pltpu.VMEM((heads * batch, hd), F32),
                dma((2, batch // 8)),
            ],
            compiler_params=params(10),
            name="attention",
        )(positions, keep(q), keep(kv), keep(k_in), keep(v_in))

        mine = heads // 2
        ocols = d_model // 4 // TILES
        buf = pltpu.VMEM((mine, batch, hd), F32)
        st = pltpu.VMEM((batch, hd), F32)
        block = (batch // HALVES, ocols)
        chunk = pltpu.VMEM((COUNT,) + block, F32)
        out = pl.pallas_call(
            output_kernel,
            out_shape=pltpu.VMEM((batch, d_model), BF16),
            in_specs=[vmem, vmem, hbm, hbm],
            out_specs=vmem,
            scratch_shapes=[
                pltpu.VMEM((batch, d_model), BF16),
                pltpu.VMEM((TILES, q_cols, ocols), BF16),
                pltpu.VMEM((batch, q_cols), BF16),
                buf, buf, buf, buf, buf, st, st, st, chunk, chunk, chunk,
                pltpu.VMEM((4, COUNT) + block, F32),
                dma((TILES + 1,)),
                dma((3 + NS,)),
                dma((6, NS)),
                dma((6,)),
                dma((4, COUNT)),
                dma((2, COUNT // GROUP)),
            ],
            compiler_params=params(28, 1),
            name="output",
        )(keep(acc.reshape(heads, batch, hd)), keep(stat), stay(hidden), stay(w_out))
        return out, k_upd.reshape(k_cache.shape), v_upd.reshape(v_cache.shape)

    cache_spec = P("dp", "sp", "tp", None)
    specs_in = (P("dp", None), P(None), P(None, "tp"), P(None, "tp"), P(None, "tp"), P("tp", None), cache_spec, cache_spec, P("dp"))
    specs_out = (P("dp", None), cache_spec, cache_spec)
    return jax.shard_map(local_step, mesh=mesh, in_specs=specs_in, out_specs=specs_out, check_vma=False)
```
